256 devices in a mesh: blocks: 64 (over x, z, core), gz: 4 (over y).
Axes of the slice: x: 4, y: 4, z: 8, core: 2. Of those that a mesh axis runs over, the one named last changes fastest.
Arguments:
- coarse_field: float32 [4, 1024, 3, 4096], P('gz', 'blocks'), may hold values from -6 to 6
- coarse_velocity: float32 [4, 1024, 3, 4096], P('gz', 'blocks'), may hold values from -15 to 15
- fine_field: float32 [4, 768, 3, 4096], P('gz', 'blocks'), may hold values from -6 to 6
- fine_velocity: float32 [4, 768, 3, 4096], P('gz', 'blocks'), may hold values from -15 to 15
- pairs: int32 [4, 2048, 6], P('gz', 'blocks'), may hold values from 0 to 63, as said below
Outputs:
- coarse_new: float32 [4, 1024, 3, 4096], P('gz', 'blocks')
- fine_new: float32 [4, 768, 3, 4096], P('gz', 'blocks')
- face_jump: float32 [4, 2048, 256], P('gz', 'blocks')
The draws below stay inside these ranges and needn't reach their ends.
Inputs may be any that keep to these rules, and one draw needn't show every extreme that they name: `pairs`: Columns: fine slot below 12, face axis 0 to 2, owner device below 64, coarse slot below 16, quadrant row and column 0 or 1. No two rows of a device name the same fine slot and face axis, and no two rows of a group name the same coarse block, face axis and quadrant. The rows of one device name one owner device at most 2 times, and exactly 2 times for some owner; rows of one device that name the same owner differ in face axis; some owner is named 2 times by every device of its group. Each face axis stands in 10 to 11 of a device's rows.
All inputs are finite; a program needn't handle non-finite values.
Results may differ from the reference program's by a relative error of at most 0.0003.
Values sent between devices are 32-bit elements; how exact they have to be, the bound alone decides.
No kernel may reach another device: no remote copies, remote signals or barrier semaphores. Data moves between devices by JAX's collectives and lax.ppermute only.
A program may use at most 256 MiB of HBM per device.

```python
import jax
import jax.numpy as jnp
from jax import lax

EDGE = 16
HALF = 8
CB = 16
FB = 12
PAIRS_DEV = 32
COARSE_ALL = 1024
FINE_ALL = 768
N_BLOCKS = 64
N_GZ = 4


def velocity_law(key, count):
    shape = (N_GZ, count * N_BLOCKS, 3, EDGE ** 3)
    group = jnp.arange(N_GZ)[:, None]
    device = jnp.arange(count * N_BLOCKS)[None, :] // count
    position = (device * N_GZ + group).astype(jnp.float32)
    scale = 1.0 + 2.0 * position / max(N_BLOCKS * N_GZ - 1, 1)
    first = jax.random.fold_in(key, 0)
    base = jax.random.truncated_normal(first, -5.0, 5.0, shape, jnp.float32)
    return (base * scale[:, :, None, None]).astype(jnp.float32)


def draw_coarse_velocity(key, part):
    return velocity_law(jax.random.fold_in(key, 3), CB)


def draw_fine_velocity(key, part):
    return velocity_law(jax.random.fold_in(key, 5), FB)


def source_rows(source_key, forced):
    first, second, third, fourth = jax.random.split(source_key, 4)
    order = jax.random.permutation(first, N_BLOCKS)
    spot = jnp.sum(jnp.arange(N_BLOCKS) * (order == forced).astype(jnp.int32))
    swapped = order.at[spot].set(order[0]).at[0].set(forced)
    doubles = jax.random.randint(second, (), 1, PAIRS_DEV // 2 + 1)
    rotate = jax.random.randint(third, (), 0, 3)
    place = jnp.arange(N_BLOCKS)
    counts = jnp.where(place < doubles, 2, jnp.where(place < PAIRS_DEV - doubles, 1, 0))
    starts = jnp.cumsum(counts) - counts
    rank = jnp.arange(PAIRS_DEV)
    link = jnp.sum((starts[None, :] <= rank[:, None]).astype(jnp.int32), axis=1) - 1
    owner = swapped[link]
    face = (rank + rotate) % 3
    within = rank // 3
    slot_tables = jax.vmap(lambda sub: jax.random.permutation(sub, FB))(jax.random.split(fourth, 3))
    fine_slot = slot_tables[face, within]
    return (owner.astype(jnp.int32), face.astype(jnp.int32), fine_slot.astype(jnp.int32))


def one_group(group_key):
    first, second, third, fourth = jax.random.split(group_key, 4)
    forced = jax.random.randint(first, (), 0, N_BLOCKS)
    owner, face, fine_slot = jax.vmap(lambda sub: source_rows(sub, forced))(jax.random.split(second, N_BLOCKS))
    target = owner * 3 + face
    hits = jnp.sum((target[:, :, None] == jnp.arange(N_BLOCKS * 3)[None, None, :]).astype(jnp.int32), axis=1)
    before = jnp.cumsum(hits, axis=0) - hits
    index = jnp.take_along_axis(before, target, axis=1)
    key_tables = jax.vmap(lambda sub: jax.random.permutation(sub, 4 * CB))(jax.random.split(third, N_BLOCKS * 3))
    value = key_tables[target, index]
    columns = jnp.stack([fine_slot, face, owner, value // 4, value // 2 % 2, value % 2], axis=-1)
    orders = jax.vmap(lambda sub: jax.random.permutation(sub, PAIRS_DEV))(jax.random.split(fourth, N_BLOCKS))
    shuffled = jnp.take_along_axis(columns, orders[:, :, None], axis=1)
    return shuffled.reshape(N_BLOCKS * PAIRS_DEV, 6).astype(jnp.int32)


def draw_pairs(key, part):
    base = jax.random.fold_in(key, 11)
    group_keys = jax.vmap(lambda index: jax.random.fold_in(base, index))(jnp.arange(N_GZ))
    return jax.vmap(one_group)(group_keys)


def block_scale(rng, dims, shards, smallest, top_value):
    level, own = 1.0, jax.random.fold_in(rng, 6)
    for dim, parts in shards:
        heights = jnp.exp(jax.random.uniform(jax.random.fold_in(own, dim), (parts,), jnp.float32, smallest / len(shards), top_value / len(shards)))
        level = level * jnp.repeat(heights, dims[dim] // parts).reshape([-1 if axis == dim else 1 for axis in range(len(dims))])
    return level


def gaussian(rng, extent, deviation, reach, shards=(), kind=jnp.bfloat16):
    result = jax.random.normal(rng, extent, jnp.float32) * deviation
    if len(shards) > 0:
        result = block_scale(rng, extent, shards, -0.22, 0.18) * result
    return jnp.clip(result, min=-reach, max=reach).astype(kind)


def setup_inputs(seed: int = 0) -> dict:
    seeds = jax.random.split(jax.random.key(seed), 6)
    coarse_field = gaussian(seeds[0], (N_GZ, COARSE_ALL, 3, EDGE ** 3), 1.0, 6.0, ((0, 4), (1, 64)), jnp.float32)
    coarse_velocity = draw_coarse_velocity(jax.random.fold_in(seeds[5], 71), 0)
    fine_field = gaussian(seeds[2], (N_GZ, FINE_ALL, 3, EDGE ** 3), 1.0, 6.0, ((0, 4), (1, 64)), jnp.float32)
    fine_velocity = draw_fine_velocity(jax.random.fold_in(seeds[5], 71), 0)
    pairs = draw_pairs(jax.random.fold_in(seeds[5], 71), 0)
    return dict(coarse_field=coarse_field, coarse_velocity=coarse_velocity, fine_field=fine_field, fine_velocity=fine_velocity, pairs=pairs)


TANGENT = ((1, 2), (0, 2), (0, 1))

def cube(values):
    return values.reshape(values.shape[:-1] + (EDGE, EDGE, EDGE))

def centred(field):
    return [0.5 * (field[along] + jnp.roll(field[along], -1, axis=along)) for along in range(3)]

def cell_speed(field, velocity):
    centre = centred(field)
    speed_v = jnp.sqrt(velocity[0] * velocity[0] + velocity[1] * velocity[1] + velocity[2] * velocity[2])
    speed_b = jnp.sqrt(centre[0] * centre[0] + centre[1] * centre[1] + centre[2] * centre[2])
    return jnp.max(speed_v + speed_b)

def edge_fields(field, velocity):
    field_x, field_y, field_z = centred(field)
    vel_x, vel_y, vel_z = (velocity[0], velocity[1], velocity[2])
    cell_x = -(vel_y * field_z - vel_z * field_y)
    cell_y = -(vel_z * field_x - vel_x * field_z)
    cell_z = -(vel_x * field_y - vel_y * field_x)

    def corner(values, first, second):
        rolled = jnp.roll(values, 1, axis=first)
        return 0.25 * (values + rolled + jnp.roll(values, 1, axis=second) + jnp.roll(rolled, 1, axis=second))
    return [corner(cell_x, 1, 2), corner(cell_y, 0, 2), corner(cell_z, 0, 1)]

def faraday(field, emf, factor):

    def ahead(values, along):
        return jnp.roll(values, -1, axis=along) - values
    emf_x, emf_y, emf_z = emf
    new_x = field[0] - factor * (ahead(emf_z, 1) - ahead(emf_y, 2))
    new_y = field[1] - factor * (ahead(emf_x, 2) - ahead(emf_z, 0))
    new_z = field[2] - factor * (ahead(emf_y, 0) - ahead(emf_x, 1))
    return jnp.stack([new_x, new_y, new_z])

def put_plane(values, normal, plane_new):
    shape = [1, 1, 1]
    shape[normal] = EDGE
    first = (jnp.arange(EDGE) == 0).reshape(shape)
    return jnp.where(first, jnp.expand_dims(plane_new, normal), values)

def restrict(planes):
    first = 0.5 * (planes[:, 0, 0::2, 0::2] + planes[:, 0, 1::2, 0::2])
    second = 0.5 * (planes[:, 1, 0::2, 0::2] + planes[:, 1, 0::2, 1::2])
    return jnp.stack([first, second], axis=1)

def reference(coarse_field, coarse_velocity, fine_field, fine_velocity, pairs):
    coarse_flat = coarse_field.reshape(-1, 3, EDGE ** 3)
    coarse_vel = coarse_velocity.reshape(-1, 3, EDGE ** 3)
    fine_flat = fine_field.reshape(-1, 3, EDGE ** 3)
    fine_vel = fine_velocity.reshape(-1, 3, EDGE ** 3)
    speeds_c = lax.map(lambda item: cell_speed(cube(item[0]), cube(item[1])), (coarse_flat, coarse_vel))
    speeds_f = lax.map(lambda item: cell_speed(cube(item[0]), cube(item[1])), (fine_flat, fine_vel))
    top_speed = jnp.maximum(jnp.max(speeds_c), jnp.max(speeds_f))
    time_step = 0.2 / top_speed

    def fine_step(item):
        field = cube(item[0])
        emf = edge_fields(field, cube(item[1]))
        updated = faraday(field, emf, time_step / 0.5)
        tangents = jnp.stack([jnp.stack([jnp.take(emf[TANGENT[normal][0]], 0, axis=normal), jnp.take(emf[TANGENT[normal][1]], 0, axis=normal)]) for normal in range(3)])
        normals = jnp.stack([jnp.take(updated[normal], 0, axis=normal) for normal in range(3)])
        return (updated.reshape(3, EDGE ** 3), tangents, normals)
    fine_out, fine_tangents, fine_normals = lax.map(fine_step, (fine_flat, fine_vel))
    pair_rows = pairs.reshape(-1, 6).astype(jnp.int32)
    count = pair_rows.shape[0]
    group = (jnp.arange(count, dtype=jnp.int32) // (PAIRS_DEV * N_BLOCKS)).astype(jnp.int32)
    source = (jnp.arange(count, dtype=jnp.int32) % (PAIRS_DEV * N_BLOCKS) // PAIRS_DEV).astype(jnp.int32)
    fine_block = (group * (FB * N_BLOCKS) + source * FB + pair_rows[:, 0]).astype(jnp.int32)
    face_dir = pair_rows[:, 1]
    coarse_block = (group * (CB * N_BLOCKS) + pair_rows[:, 2] * CB + pair_rows[:, 3]).astype(jnp.int32)
    quad_row = pair_rows[:, 4]
    quad_col = pair_rows[:, 5]
    restricted = restrict(fine_tangents[fine_block, face_dir])
    span = jnp.arange(HALF, dtype=jnp.int32)
    rows_idx = (quad_row[:, None, None, None] * HALF + span[None, None, :, None]).astype(jnp.int32)
    cols_idx = (quad_col[:, None, None, None] * HALF + span[None, None, None, :]).astype(jnp.int32)
    comp_idx = jnp.arange(2, dtype=jnp.int32)[None, :, None, None]
    blocks_all = coarse_flat.shape[0]
    replaced = jnp.zeros((blocks_all, 3, 2, EDGE, EDGE), jnp.float32)
    replaced = replaced.at[coarse_block[:, None, None, None], face_dir[:, None, None, None], comp_idx, rows_idx, cols_idx].set(restricted)
    hit_mask = jnp.zeros((blocks_all, 3, EDGE, EDGE), jnp.float32)
    hit_mask = hit_mask.at[coarse_block[:, None, None], face_dir[:, None, None], rows_idx[:, 0], cols_idx[:, 0]].set(jnp.ones((count, HALF, HALF), jnp.float32))

    def coarse_step(item):
        field = cube(item[0])
        emf = edge_fields(field, cube(item[1]))
        for normal in range(3):
            for which in range(2):
                along = TANGENT[normal][which]
                plane_now = jnp.take(emf[along], 0, axis=normal)
                plane_new = jnp.where(item[3][normal] > 0.5, item[2][normal, which], plane_now)
                emf[along] = put_plane(emf[along], normal, plane_new)
        updated = faraday(field, emf, time_step / 1.0)
        normals = jnp.stack([jnp.take(updated[normal], 0, axis=normal) for normal in range(3)])
        return (updated.reshape(3, EDGE ** 3), normals)
    coarse_out, coarse_normals = lax.map(coarse_step, (coarse_flat, coarse_vel, replaced, hit_mask))
    quadrant = coarse_normals[coarse_block[:, None, None], face_dir[:, None, None], rows_idx[:, 0], cols_idx[:, 0]]
    prolonged = jnp.repeat(jnp.repeat(quadrant, 2, axis=1), 2, axis=2)
    face_jump = fine_normals[fine_block, face_dir] - prolonged
    return (coarse_out.reshape(coarse_field.shape), fine_out.reshape(fine_field.shape), face_jump.reshape(N_GZ, PAIRS_DEV * N_BLOCKS, EDGE * EDGE))
```

```python
import jax
import jax.numpy as jnp
import numpy as np
from jax import lax
from jax.experimental import pallas as pl
from jax.experimental.pallas import tpu as pltpu
from jax.sharding import Mesh
from jax.sharding import PartitionSpec as P

EDGE = 16
HALF = 8
CB = 16
FB = 12
PAIRS = 32
PEERS = 64
WIDE = EDGE * EDGE
CELLS = EDGE**3
PITCH = 104
BLOCKS = ("blocks_0", "blocks_1", "blocks_2")
F32 = jnp.float32
BF16 = jnp.bfloat16
TANGENT = ((1, 2), (0, 2), (0, 1))


def _face_lane(row, col, flip):
    return col * EDGE + row if flip else row * EDGE + col


def _restrict_matrix(flip):
    out = np.zeros((2, WIDE, 128), np.float32)
    for m in range(HALF):
        for n in range(HALF):
            o = m * HALF + n
            out[0, _face_lane(2 * m, 2 * n, flip), o] = 0.5
            out[0, _face_lane(2 * m + 1, 2 * n, flip), o] = 0.5
            out[1, _face_lane(2 * m, 2 * n, flip), 64 + o] = 0.5
            out[1, _face_lane(2 * m, 2 * n + 1, flip), 64 + o] = 0.5
    return out.reshape(2 * WIDE, 128)


def _expand_matrix(flip):
    out = np.zeros((128, 256), np.float32)
    for m in range(HALF):
        for n in range(HALF):
            o = m * HALF + n
            out[o, _face_lane(m, n, flip)] = 1.0
            out[64 + o, 128 + _face_lane(m, n, flip)] = 1.0
    return out


def _quadrant_matrix(flip):
    out = np.zeros((WIDE, WIDE), np.float32)
    for row in range(EDGE):
        for col in range(EDGE):
            quad = (row // HALF) * 2 + col // HALF
            out[_face_lane(row, col, flip), quad * 64 + (row % HALF) * HALF + col % HALF] = 1.0
    return out


def _flip_matrix():
    out = np.zeros((WIDE, WIDE), np.float32)
    for row in range(EDGE):
        for col in range(EDGE):
            out[_face_lane(row, col, True), _face_lane(row, col, False)] = 1.0
    return out


def _prolong_matrix():
    out = np.zeros((128, WIDE), np.float32)
    for row in range(EDGE):
        for col in range(EDGE):
            o = (row // 2) * HALF + col // 2
            out[o, _face_lane(row, col, False)] = 1.0
            out[64 + o, _face_lane(row, col, False)] = 1.0
    return out


RESTRICT = np.stack([_restrict_matrix(False), _restrict_matrix(True)])
EXPAND = np.stack([_expand_matrix(False), _expand_matrix(True)])
QUADRANT = np.stack([_quadrant_matrix(False), _quadrant_matrix(True)])
FLIP = _flip_matrix()
PROLONG = _prolong_matrix()


def halves(value):
    high = value.astype(BF16)
    return high, (value - high.astype(F32)).astype(BF16)


def mm(a, b, dims=((1,), (0,))):
    return lax.dot_general(a, b, (dims, ((), ())), preferred_element_type=F32)


def mm_left(value, matrix, dims=((1,), (0,))):
    high, low = halves(value)
    return mm(high, matrix, dims) + mm(low, matrix, dims)


def mm_right(matrix, value, dims=((1,), (0,))):
    high, low = halves(value)
    return mm(matrix, high, dims) + mm(matrix, low, dims)


def lanes_of(value):
    return lax.broadcasted_iota(jnp.int32, value.shape, 1)


def y_prev(p):
    a, b = pltpu.roll(p[0], 16, 1), pltpu.roll(p[1], 16, 1)
    edge = lanes_of(a) < 16
    return jnp.where(edge, b, a), jnp.where(edge, a, b)


def y_next(p):
    a, b = pltpu.roll(p[0], 112, 1), pltpu.roll(p[1], 112, 1)
    edge = lanes_of(a) >= 112
    return jnp.where(edge, b, a), jnp.where(edge, a, b)


def z_prev(p):
    edge = (lanes_of(p[0]) & 15) == 0
    return tuple(jnp.where(edge, pltpu.roll(x, 113, 1), pltpu.roll(x, 1, 1)) for x in p)


def z_next(p):
    edge = (lanes_of(p[0]) & 15) == 15
    return tuple(jnp.where(edge, pltpu.roll(x, 15, 1), pltpu.roll(x, 127, 1)) for x in p)


def each(fn, *pairs):
    return tuple(fn(*(p[h] for p in pairs)) for h in range(2))


def slab(ref, comp, i, first, count):
    base = pl.multiple_of(i * WIDE, 128)
    return (
        ref[comp, first : first + count, pl.ds(base, 128)],
        ref[comp, first : first + count, pl.ds(pl.multiple_of(base + 128, 128), 128)],
    )


def put_slab(ref, comp, i, first, count, value):
    base = pl.multiple_of(i * WIDE, 128)
    ref[comp, first : first + count, pl.ds(base, 128)] = value[0]
    ref[comp, first : first + count, pl.ds(pl.multiple_of(base + 128, 128), 128)] = value[1]


def fine_slab(ref, comp, i):
    def one(half):
        start = comp * 32 + 2 * i + half
        return jnp.concatenate(
            [
                ref[pl.ds(start, 8, stride=PITCH), :],
                ref[pl.ds(start + 8 * PITCH, 8, stride=PITCH), :],
            ],
            axis=0,
        )

    return one(0), one(1)


def put_fine_slab(ref, comp, i, value):
    for half in range(2):
        start = comp * 32 + 2 * i + half
        ref[pl.ds(start, 8, stride=PITCH), :] = value[half][0:8]
        ref[pl.ds(start + 8 * PITCH, 8, stride=PITCH), :] = value[half][8:16]


def fetch_fine(source, target, sem):
    return [
        pltpu.make_async_copy(source.at[b], target.at[pl.ds(b * PITCH, 96)], sem)
        for b in range(FB)
    ]


def face_row_wise(load):
    def step(i, held):
        turned = pltpu.roll(load(i), (i % 8) * 16, 1)
        place = (lanes_of(turned) // 16) == i % 8
        upper = jnp.broadcast_to(i >= 8, turned.shape)
        return (
            jnp.where(place & ~upper, turned, held[0]),
            jnp.where(place & upper, turned, held[1]),
        )

    zero = jnp.zeros((CB, 128), F32)
    return lax.fori_loop(0, EDGE, step, (zero, zero))


def face_column_wise(load):
    def step(i, held):
        both = load(i)
        place = (lanes_of(both[0]) & 15) == i
        return each(lambda x, h: jnp.where(place, pltpu.roll(x, i, 1), h), both, held)

    zero = jnp.zeros((CB, 128), F32)
    return lax.fori_loop(0, EDGE, step, (zero, zero))


def routes(pairs_ref):
    slot, face, owner = pairs_ref[0], pairs_ref[1], pairs_ref[2]
    peer = lax.broadcasted_iota(jnp.int32, (PEERS, PAIRS), 0)
    named = (owner == peer).astype(F32)
    before = (
        lax.broadcasted_iota(jnp.int32, (PAIRS, PAIRS), 0)
        < lax.broadcasted_iota(jnp.int32, (PAIRS, PAIRS), 1)
    ).astype(F32)
    earlier = mm(named.astype(BF16), before.astype(BF16))
    rank = jnp.sum(named * earlier, axis=0, keepdims=True)
    first = jnp.where(rank < 0.5, named, 0.0)
    second = jnp.where(rank < 0.5, 0.0, named)
    at_row = lax.broadcasted_iota(jnp.int32, (3 * CB, PAIRS), 0)
    source = (face * CB + slot == at_row).astype(F32)
    return first, second, source


def first_kernel(
    cb, cv, fb, fv, pairs, restrict, send, speed, emf, scb, scv, sfb, sfv, cell, sems
):
    fine_copies = fetch_fine(fb, sfb, sems.at[0]) + fetch_fine(fv, sfv, sems.at[1])
    for copy in fine_copies:
        copy.start()
    coarse_copies = [
        pltpu.make_async_copy(cb, scb, sems.at[2]),
        pltpu.make_async_copy(cv, scv, sems.at[3]),
    ]
    for copy in coarse_copies:
        copy.start()
    idle = pl.ds(FB * PITCH, (CB - FB) * PITCH)
    sfb[idle, :] = jnp.zeros(((CB - FB) * PITCH, 128), F32)
    sfv[idle, :] = jnp.zeros(((CB - FB) * PITCH, 128), F32)

    def cells(load_b, load_v, first):
        def step(i, top):
            following = lax.rem(i + 1, EDGE)
            bx, by, bz = load_b(0, i), load_b(1, i), load_b(2, i)
            vx, vy, vz = load_v(0, i), load_v(1, i), load_v(2, i)
            mean = lambda a, b: 0.5 * (a + b)
            cx = each(mean, bx, load_b(0, following))
            cy = each(mean, by, y_next(by))
            cz = each(mean, bz, z_next(bz))
            put_slab(cell, 0, i, first, CB, each(lambda a, b, c, d: a * b - c * d, vz, cy, vy, cz))
            put_slab(cell, 1, i, first, CB, each(lambda a, b, c, d: a * b - c * d, vx, cz, vz, cx))
            put_slab(cell, 2, i, first, CB, each(lambda a, b, c, d: a * b - c * d, vy, cx, vx, cy))
            size = lambda a, b, c: jnp.sqrt(a * a + b * b + c * c)
            fast = each(lambda a, b: a + b, each(size, vx, vy, vz), each(size, cx, cy, cz))
            return jnp.maximum(top, jnp.maximum(fast[0], fast[1]))

        return lax.fori_loop(0, EDGE, step, jnp.zeros((CB, 128), F32))

    def edges(first):
        def step(i, carry):
            prior = lax.rem(i + EDGE - 1, EDGE)
            add = lambda a, b: a + b
            quarter = lambda a, b: 0.25 * (a + b)
            ex = slab(cell, 0, i, first, CB)
            sum_x = each(add, ex, y_prev(ex))
            put_slab(emf, 0, i, first, CB, each(quarter, sum_x, z_prev(sum_x)))
            sum_y = each(add, slab(cell, 1, i, first, CB), slab(cell, 1, prior, first, CB))
            put_slab(emf, 1, i, first, CB, each(quarter, sum_y, z_prev(sum_y)))
            sum_z = each(add, slab(cell, 2, i, first, CB), slab(cell, 2, prior, first, CB))
            put_slab(emf, 2, i, first, CB, each(quarter, sum_z, y_prev(sum_z)))
            return carry

        lax.fori_loop(0, EDGE, step, 0)

    for copy in fine_copies:
        copy.wait()
    top_fine = cells(lambda c, i: fine_slab(sfb, c, i), lambda c, i: fine_slab(sfv, c, i), CB)
    edges(CB)

    first, second, source = routes(pairs)
    rows = []
    for d in range(3):
        planes = []
        for along in TANGENT[d]:
            if d == 0:
                planes.append(slab(emf, along, 0, CB, CB))
            elif d == 1:
                planes.append(face_row_wise(lambda i: slab(emf, along, i, CB, CB)[0]))
            else:
                planes.append(face_column_wise(lambda i: slab(emf, along, i, CB, CB)))
        both = jnp.concatenate([*planes[0], *planes[1]], axis=1)
        rows.append(mm_left(both, restrict[1 if d == 2 else 0]))
    rows = jnp.concatenate(rows, axis=0)
    nt = ((1,), (1,))
    key = (pairs[1] * 64 + (pairs[4] * 2 + pairs[5]) * CB + pairs[3] + 1).astype(F32)
    lane = lax.broadcasted_iota(jnp.int32, (PEERS, 128), 1)
    meta = jnp.zeros((PEERS, 128), F32)
    for k, chosen in enumerate((first, second)):
        pick = mm(chosen.astype(BF16), source.astype(BF16), nt)
        send[:, 0, k * 128 : (k + 1) * 128] = mm_right(pick.astype(BF16), rows)
        meta = jnp.where(lane == k, jnp.sum(chosen * key, axis=1, keepdims=True), meta)
    send[:, 0, 256:384] = meta

    for copy in coarse_copies:
        copy.wait()
    top_coarse = cells(lambda c, i: slab(scb, c, i, 0, CB), lambda c, i: slab(scv, c, i, 0, CB), 0)
    edges(0)
    top = jnp.max(jnp.maximum(top_fine, top_coarse), axis=0, keepdims=True)
    speed[...] = jnp.broadcast_to(jnp.max(top, axis=1, keepdims=True), (1, 128))


def second_kernel(
    got, cb, fb, emf_in, expand, quadrant, new_c, new_f, back, normals, sfb, emf, out_f, sems
):
    copies = fetch_fine(fb, sfb, sems.at[0])
    for copy in copies:
        copy.start()
    load_emf = pltpu.make_async_copy(emf_in, emf, sems.at[1])
    load_emf.start()
    idle = pl.ds(FB * PITCH, (CB - FB) * PITCH)
    sfb[idle, :] = jnp.zeros(((CB - FB) * PITCH, 128), F32)

    meta = got[:, 0, 256:384]
    top = jnp.max(jnp.max(meta[:, 2:3], axis=0, keepdims=True), axis=1, keepdims=True)
    time_step = 0.2 / top
    keys = [meta[:, k : k + 1].astype(jnp.int32) - 1 for k in range(2)]
    target = lax.broadcasted_iota(jnp.int32, (PEERS, 256), 1)
    hit = jnp.concatenate([(k == target).astype(F32) for k in keys], axis=0).astype(BF16)
    rows = jnp.concatenate([got[:, 0, 0:128], got[:, 0, 128:256]], axis=0)
    tn = ((0,), (0,))
    replaced = mm_right(hit, rows, tn)[0:192]
    counted = mm(hit, jnp.ones((2 * PEERS, 128), BF16), tn)[0:192]
    spread = jnp.concatenate(
        [mm_left(replaced[0:128], expand[0]), mm_left(replaced[128:192], expand[1])], axis=0
    )
    lane = lax.broadcasted_iota(jnp.int32, (CB, 128), 1)

    def faces(d):
        def at(quad):
            return slice(d * 64 + quad * CB, d * 64 + (quad + 1) * CB)

        planes, masks = ([], []), []
        for h in range(2):
            near, far = (h, h + 2) if d == 2 else (2 * h, 2 * h + 1)
            for t in range(2):
                part = slice(t * 128, (t + 1) * 128)
                planes[t].append(spread[at(near), part] + pltpu.roll(spread[at(far), part], 8, 1))
            masks.append(jnp.where((lane & 15) < 8, counted[at(near)], counted[at(far)]))
        return planes, masks

    load_emf.wait()
    for t, along in enumerate(TANGENT[0]):
        planes, masks = faces(0)
        now = slab(emf, along, 0, 0, CB)
        put_slab(emf, along, 0, 0, CB, each(lambda m, p, e: jnp.where(m > 0.5, p, e), masks, planes[t], now))
    planes_1, masks_1 = faces(1)
    planes_2, masks_2 = faces(2)

    def correct(i, carry):
        turn = lax.rem(8 - i % 8, 8) * 16
        upper = jnp.broadcast_to(i >= 8, (CB, 128))
        there = pltpu.roll(jnp.where(upper, masks_1[1], masks_1[0]), turn, 1)
        for t, along in enumerate(TANGENT[1]):
            value = pltpu.roll(jnp.where(upper, planes_1[t][1], planes_1[t][0]), turn, 1)
            base = pl.multiple_of(i * WIDE, 128)
            now = emf[along, 0:CB, pl.ds(base, 128)]
            emf[along, 0:CB, pl.ds(base, 128)] = jnp.where((lane < 16) & (there > 0.5), value, now)
        turn = lax.rem(128 - i, 128)
        column = (lane & 15) == 0
        there = [column & (pltpu.roll(m, turn, 1) > 0.5) for m in masks_2]
        for t, along in enumerate(TANGENT[2]):
            value = [pltpu.roll(p, turn, 1) for p in planes_2[t]]
            now = slab(emf, along, i, 0, CB)
            put_slab(emf, along, i, 0, CB, each(jnp.where, there, value, now))
        return carry

    lax.fori_loop(0, EDGE, correct, 0)
    for copy in copies:
        copy.wait()

    def update(first, factor, load_b, store):
        def step(i, carry):
            following = lax.rem(i + 1, EDGE)
            ex, ey, ez = (slab(emf, c, i, first, CB) for c in range(3))
            ey_far, ez_far = (slab(emf, c, following, first, CB) for c in (1, 2))
            curl = lambda b, p, q, r, s: b - factor * ((p - q) - (r - s))
            store(0, i, each(curl, load_b(0, i), y_next(ez), ez, z_next(ey), ey))
            store(1, i, each(curl, load_b(1, i), z_next(ex), ex, ez_far, ez))
            store(2, i, each(curl, load_b(2, i), ey_far, ey, y_next(ex), ex))
            return carry

        lax.fori_loop(0, EDGE, step, 0)

    update(
        0,
        time_step,
        lambda c, i: slab(cb, c, i, 0, CB),
        lambda c, i, value: put_slab(new_c, c, i, 0, CB, value),
    )
    update(
        CB,
        time_step / 0.5,
        lambda c, i: fine_slab(sfb, c, i),
        lambda c, i, value: put_fine_slab(out_f, c, i, value),
    )
    results = [
        pltpu.make_async_copy(out_f.at[pl.ds(b * PITCH, 96)], new_f.at[b], sems.at[2])
        for b in range(FB)
    ]
    for copy in results:
        copy.start()
    quads = []
    faces_c = (
        slab(new_c, 0, 0, 0, CB),
        face_row_wise(lambda i: slab(new_c, 1, i, 0, CB)[0]),
        face_column_wise(lambda i: slab(new_c, 2, i, 0, CB)),
    )
    for d in range(3):
        quads.append(mm_left(jnp.concatenate(faces_c[d], axis=1), quadrant[1 if d == 2 else 0]))
    quads = jnp.concatenate([*quads, jnp.zeros((CB, WIDE), F32)], axis=0)
    wide_lane = lax.broadcasted_iota(jnp.int32, (PEERS, 64), 1)
    out_lane = lax.broadcasted_iota(jnp.int32, (PEERS, 128), 1)
    answers = []
    for k in range(2):
        key = keys[k]
        row = jnp.where(key >= 0, (key >> 6) * CB + (key & 15), -1)
        pick = (row == wide_lane).astype(F32).astype(BF16)
        both = mm_right(pick, quads)
        quad = (key >> 4) & 3
        value = jnp.where(quad >= 2, both[:, 128:256], both[:, 0:128])
        answers.append(jnp.where((quad & 1) == k, value, pltpu.roll(value, 64, 1)))
    back[:, 0, :] = jnp.where(out_lane < 64, answers[0], answers[1])

    faces_f = (
        fine_slab(out_f, 0, 0),
        face_row_wise(lambda i: fine_slab(out_f, 1, i)[0]),
        face_column_wise(lambda i: fine_slab(out_f, 2, i)),
    )
    for d in range(3):
        normals[d * CB : (d + 1) * CB, 0:128] = faces_f[d][0]
        normals[d * CB : (d + 1) * CB, 128:256] = faces_f[d][1]
    for copy in results:
        copy.wait()


def third_kernel(got, normals, pairs, flip, prolong, jump):
    first, second, source = routes(pairs)
    tn = ((0,), (0,))
    rows = got[:, 0, :]
    lane = lax.broadcasted_iota(jnp.int32, (PAIRS, 128), 1)
    own = jnp.where(
        lane < 64,
        mm_right(first.astype(BF16), rows, tn),
        mm_right(second.astype(BF16), rows, tn),
    )
    coarse = mm_left(own, prolong[...])
    source = source.astype(BF16)
    straight = mm_right(source[0 : 2 * CB], normals[0 : 2 * CB], tn)
    flipped = mm_left(mm_right(source[2 * CB :], normals[2 * CB :], tn), flip[...])
    jump[...] = straight + flipped - coarse


VMEM = pl.BlockSpec(memory_space=pltpu.VMEM)
ANY = pl.BlockSpec(memory_space=pl.ANY)


def on_device(coarse_field, coarse_velocity, fine_field, fine_velocity, pairs):
    cb = coarse_field[0].transpose(1, 0, 2)
    cv = coarse_velocity[0].transpose(1, 0, 2)
    fb = fine_field[0].reshape(FB, 96, 128)
    fv = fine_velocity[0].reshape(FB, 96, 128)
    rows = pairs[0].T.reshape(6, 1, PAIRS)
    field = pltpu.VMEM((3, CB, CELLS), F32)
    pitched = pltpu.VMEM((CB * PITCH, 128), F32)
    limit = pltpu.CompilerParams(vmem_limit_bytes=32 * 1024 * 1024)
    send, speed, emf = pl.pallas_call(
        first_kernel,
        out_shape=(
            jax.ShapeDtypeStruct((PEERS, 1, 384), F32),
            jax.ShapeDtypeStruct((1, 128), F32),
            jax.ShapeDtypeStruct((3, 2 * CB, CELLS), F32),
        ),
        in_specs=[ANY, ANY, ANY, ANY, VMEM, VMEM],
        out_specs=(VMEM, VMEM, VMEM),
        scratch_shapes=[
            field,
            field,
            pitched,
            pitched,
            pltpu.VMEM((3, 2 * CB, CELLS), F32),
            pltpu.SemaphoreType.DMA((4,)),
        ],
        compiler_params=limit,
        name="edges_and_rows",
    )(cb, cv, fb, fv, rows, jnp.asarray(RESTRICT, BF16))
    count = lax.axis_size("gz")
    others = [
        lax.ppermute(speed, "gz", [(i, (i + k) % count) for i in range(count)])
        for k in range(1, count)
    ]
    for other in others:
        speed = jnp.maximum(speed, other)
    lane = lax.broadcasted_iota(jnp.int32, send.shape, 2)
    send = jnp.where(lane == 258, speed[0, 0], send)
    got = lax.all_to_all(send, BLOCKS, 0, 0, tiled=True)
    new_c, new_f, back, normals = pl.pallas_call(
        second_kernel,
        out_shape=(
            jax.ShapeDtypeStruct((3, CB, CELLS), F32),
            jax.ShapeDtypeStruct((FB, 96, 128), F32),
            jax.ShapeDtypeStruct((PEERS, 1, 128), F32),
            jax.ShapeDtypeStruct((3 * CB, WIDE), F32),
        ),
        in_specs=[VMEM, VMEM, ANY, ANY, VMEM, VMEM],
        out_specs=(VMEM, ANY, VMEM, VMEM),
        scratch_shapes=[
            pitched,
            pltpu.VMEM((3, 2 * CB, CELLS), F32),
            pitched,
            pltpu.SemaphoreType.DMA((3,)),
        ],
        compiler_params=limit,
        name="corrected_updates",
    )(got, cb, fb, emf, jnp.asarray(EXPAND, BF16), jnp.asarray(QUADRANT, BF16))
    returned = lax.all_to_all(back, BLOCKS, 0, 0, tiled=True)
    jump = pl.pallas_call(
        third_kernel,
        out_shape=jax.ShapeDtypeStruct((PAIRS, WIDE), F32),
        in_specs=[VMEM] * 5,
        out_specs=VMEM,
        compiler_params=limit,
        name="face_jumps",
    )(returned, normals, rows, jnp.asarray(FLIP, BF16), jnp.asarray(PROLONG, BF16))
    return (
        new_c.transpose(1, 0, 2)[None],
        new_f.reshape(1, FB, 3, CELLS),
        jump[None],
    )


def solution(mesh):
    split = Mesh(
        mesh.devices.reshape(4, 8, 2, mesh.shape["gz"]), ("blocks_0", "blocks_1", "blocks_2", "gz")
    )
    in_specs = (
        P("gz", BLOCKS, None, None),
        P("gz", BLOCKS, None, None),
        P("gz", BLOCKS, None, None),
        P("gz", BLOCKS, None, None),
        P("gz", BLOCKS, None),
    )
    out_specs = (P("gz", BLOCKS, None, None), P("gz", BLOCKS, None, None), P("gz", BLOCKS, None))
    return jax.shard_map(
        on_device, mesh=split, in_specs=in_specs, out_specs=out_specs, check_vma=False
    )
```

```python
import jax
import jax.numpy as jnp
import numpy as np
from jax import lax
from jax.experimental import pallas as pl
from jax.experimental.pallas import tpu as pltpu
from jax.sharding import Mesh
from jax.sharding import PartitionSpec as P

EDGE = 16
HALF = 8
CB = 16
FB = 12
PAIRS = 32
PEERS = 64
WIDE = EDGE * EDGE
CELLS = EDGE**3
PITCH = 104
BLOCKS = ("blocks_0", "blocks_1", "blocks_2")
F32 = jnp.float32
BF16 = jnp.bfloat16
TANGENT = ((1, 2), (0, 2), (0, 1))
UNROLL = 16


def _face_lane(row, col, flip):
    return col * EDGE + row if flip else row * EDGE + col


def _restrict_matrix(flip):
    out = np.zeros((2, WIDE, 128), np.float32)
    for m in range(HALF):
        for n in range(HALF):
            o = m * HALF + n
            out[0, _face_lane(2 * m, 2 * n, flip), o] = 0.5
            out[0, _face_lane(2 * m + 1, 2 * n, flip), o] = 0.5
            out[1, _face_lane(2 * m, 2 * n, flip), 64 + o] = 0.5
            out[1, _face_lane(2 * m, 2 * n + 1, flip), 64 + o] = 0.5
    return out.reshape(2 * WIDE, 128)


def _expand_matrix(flip):
    out = np.zeros((128, 256), np.float32)
    for m in range(HALF):
        for n in range(HALF):
            o = m * HALF + n
            out[o, _face_lane(m, n, flip)] = 1.0
            out[64 + o, 128 + _face_lane(m, n, flip)] = 1.0
    return out


def _quadrant_matrix(flip):
    out = np.zeros((WIDE, WIDE), np.float32)
    for row in range(EDGE):
        for col in range(EDGE):
            quad = (row // HALF) * 2 + col // HALF
            out[_face_lane(row, col, flip), quad * 64 + (row % HALF) * HALF + col % HALF] = 1.0
    return out


def _flip_matrix():
    out = np.zeros((WIDE, WIDE), np.float32)
    for row in range(EDGE):
        for col in range(EDGE):
            out[_face_lane(row, col, True), _face_lane(row, col, False)] = 1.0
    return out


def _prolong_matrix():
    out = np.zeros((128, WIDE), np.float32)
    for row in range(EDGE):
        for col in range(EDGE):
            o = (row // 2) * HALF + col // 2
            out[o, _face_lane(row, col, False)] = 1.0
            out[64 + o, _face_lane(row, col, False)] = 1.0
    return out


RESTRICT = np.stack([_restrict_matrix(False), _restrict_matrix(True)])
EXPAND = np.stack([_expand_matrix(False), _expand_matrix(True)])
QUADRANT = np.stack([_quadrant_matrix(False), _quadrant_matrix(True)])
FLIP = _flip_matrix()
PROLONG = _prolong_matrix()


def halves(value):
    high = value.astype(BF16)
    return high, (value - high.astype(F32)).astype(BF16)


def mm(a, b, dims=((1,), (0,))):
    return lax.dot_general(a, b, (dims, ((), ())), preferred_element_type=F32)


def mm_left(value, matrix, dims=((1,), (0,))):
    high, low = halves(value)
    return mm(high, matrix, dims) + mm(low, matrix, dims)


def mm_right(matrix, value, dims=((1,), (0,))):
    high, low = halves(value)
    return mm(matrix, high, dims) + mm(matrix, low, dims)


def lanes_of(value):
    return lax.broadcasted_iota(jnp.int32, value.shape, 1)


def y_prev(p):
    a, b = pltpu.roll(p[0], 16, 1), pltpu.roll(p[1], 16, 1)
    edge = lanes_of(a) < 16
    return jnp.where(edge, b, a), jnp.where(edge, a, b)


def y_next(p):
    a, b = pltpu.roll(p[0], 112, 1), pltpu.roll(p[1], 112, 1)
    edge = lanes_of(a) >= 112
    return jnp.where(edge, b, a), jnp.where(edge, a, b)


def z_prev(p):
    edge = (lanes_of(p[0]) & 15) == 0
    return tuple(jnp.where(edge, pltpu.roll(x, 113, 1), pltpu.roll(x, 1, 1)) for x in p)


def z_next(p):
    edge = (lanes_of(p[0]) & 15) == 15
    return tuple(jnp.where(edge, pltpu.roll(x, 15, 1), pltpu.roll(x, 127, 1)) for x in p)


def each(fn, *pairs):
    return tuple(fn(*(p[h] for p in pairs)) for h in range(2))


def span(i, half):
    start = i * WIDE + half * 128
    return pl.ds(start if isinstance(start, int) else pl.multiple_of(start, 128), 128)


def slab(ref, comp, i, first, count):
    return tuple(ref[comp, first : first + count, span(i, half)] for half in range(2))


def put_slab(ref, comp, i, first, count, value):
    for half in range(2):
        ref[comp, first : first + count, span(i, half)] = value[half]


def fine_slab(ref, comp, i):
    def one(half):
        start = comp * 32 + 2 * i + half
        return jnp.concatenate(
            [
                ref[pl.ds(start, 8, stride=PITCH), :],
                ref[pl.ds(start + 8 * PITCH, 8, stride=PITCH), :],
            ],
            axis=0,
        )

    return one(0), one(1)


def put_fine_slab(ref, comp, i, value):
    for half in range(2):
        start = comp * 32 + 2 * i + half
        ref[pl.ds(start, 8, stride=PITCH), :] = value[half][0:8]
        ref[pl.ds(start + 8 * PITCH, 8, stride=PITCH), :] = value[half][8:16]


def fetch_fine(source, target, sem):
    return [
        pltpu.make_async_copy(source.at[b], target.at[pl.ds(b * PITCH, 96)], sem)
        for b in range(FB)
    ]


def face_row_wise(load):
    out = [jnp.zeros((CB, 128), F32)] * 2
    group = lax.broadcasted_iota(jnp.int32, (CB, 128), 1) // 16
    for i in range(EDGE):
        turned = pltpu.roll(load(i), i % 8 * 16, 1)
        out[i // 8] = jnp.where(group == i % 8, turned, out[i // 8])
    return tuple(out)


def face_column_wise(load):
    out = (jnp.zeros((CB, 128), F32),) * 2
    column = lax.broadcasted_iota(jnp.int32, (CB, 128), 1) & 15
    for i in range(EDGE):
        out = each(lambda x, h: jnp.where(column == i, pltpu.roll(x, i, 1), h), load(i), out)
    return out


def routes(pairs_ref):
    slot, face, owner = pairs_ref[0], pairs_ref[1], pairs_ref[2]
    peer = lax.broadcasted_iota(jnp.int32, (PEERS, PAIRS), 0)
    named = (owner == peer).astype(F32)
    before = (
        lax.broadcasted_iota(jnp.int32, (PAIRS, PAIRS), 0)
        < lax.broadcasted_iota(jnp.int32, (PAIRS, PAIRS), 1)
    ).astype(F32)
    earlier = mm(named.astype(BF16), before.astype(BF16))
    rank = jnp.sum(named * earlier, axis=0, keepdims=True)
    first = jnp.where(rank < 0.5, named, 0.0)
    second = jnp.where(rank < 0.5, 0.0, named)
    at_row = lax.broadcasted_iota(jnp.int32, (3 * CB, PAIRS), 0)
    source = (face * CB + slot == at_row).astype(F32)
    return first, second, source


def cells_kernel(cb, cv, fb, fv, cell_c, cell_f, b_c, b_f, speed, v_c, v_f, sems):
    fine_copies = fetch_fine(fb, b_f, sems.at[0]) + fetch_fine(fv, v_f, sems.at[1])
    coarse_copies = [
        pltpu.make_async_copy(cb, b_c, sems.at[2]),
        pltpu.make_async_copy(cv, v_c, sems.at[3]),
    ]
    for copy in fine_copies + coarse_copies:
        copy.start()
    idle = pl.ds(FB * PITCH, (CB - FB) * PITCH)
    b_f[idle, :] = jnp.zeros(((CB - FB) * PITCH, 128), F32)
    v_f[idle, :] = jnp.zeros(((CB - FB) * PITCH, 128), F32)

    def cells(load_b, load_v, cell):
        def step(i, top):
            following = lax.rem(i + 1, EDGE)
            bx, by, bz = load_b(0, i), load_b(1, i), load_b(2, i)
            vx, vy, vz = load_v(0, i), load_v(1, i), load_v(2, i)
            mean = lambda a, b: 0.5 * (a + b)
            cx = each(mean, bx, load_b(0, following))
            cy = each(mean, by, y_next(by))
            cz = each(mean, bz, z_next(bz))
            cross = lambda a, b, c, d: a * b - c * d
            put_slab(cell, 0, i, 0, CB, each(cross, vz, cy, vy, cz))
            put_slab(cell, 1, i, 0, CB, each(cross, vx, cz, vz, cx))
            put_slab(cell, 2, i, 0, CB, each(cross, vy, cx, vx, cy))
            size = lambda a, b, c: jnp.sqrt(a * a + b * b + c * c)
            fast = each(lambda a, b: a + b, each(size, vx, vy, vz), each(size, cx, cy, cz))
            return jnp.maximum(top, jnp.maximum(fast[0], fast[1]))

        return lax.fori_loop(0, EDGE, step, jnp.zeros((CB, 128), F32), unroll=UNROLL)

    for copy in fine_copies:
        copy.wait()
    top_fine = cells(lambda c, i: fine_slab(b_f, c, i), lambda c, i: fine_slab(v_f, c, i), cell_f)
    for copy in coarse_copies:
        copy.wait()
    top_coarse = cells(
        lambda c, i: slab(b_c, c, i, 0, CB), lambda c, i: slab(v_c, c, i, 0, CB), cell_c
    )
    top = jnp.max(jnp.maximum(top_fine, top_coarse), axis=0, keepdims=True)
    speed[...] = jnp.broadcast_to(jnp.max(top, axis=1, keepdims=True), (1, 128))


def edges(cell, emf):
    def step(i, carry):
        prior = lax.rem(i + EDGE - 1, EDGE)
        add = lambda a, b: a + b
        quarter = lambda a, b: 0.25 * (a + b)
        ex = slab(cell, 0, i, 0, CB)
        sum_x = each(add, ex, y_prev(ex))
        put_slab(emf, 0, i, 0, CB, each(quarter, sum_x, z_prev(sum_x)))
        sum_y = each(add, slab(cell, 1, i, 0, CB), slab(cell, 1, prior, 0, CB))
        put_slab(emf, 1, i, 0, CB, each(quarter, sum_y, z_prev(sum_y)))
        sum_z = each(add, slab(cell, 2, i, 0, CB), slab(cell, 2, prior, 0, CB))
        put_slab(emf, 2, i, 0, CB, each(quarter, sum_z, y_prev(sum_z)))
        return carry

    lax.fori_loop(0, EDGE, step, 0, unroll=UNROLL)


def face_of(ref, along, d):
    if d == 0:
        return slab(ref, along, 0, 0, CB)
    if d == 1:
        return face_row_wise(lambda i: slab(ref, along, i, 0, CB)[0])
    return face_column_wise(lambda i: slab(ref, along, i, 0, CB))


def rows_kernel(cell, pairs, restrict, send, emf):
    edges(cell, emf)
    first, second, source = routes(pairs)
    rows = []
    for d in range(3):
        planes = [face_of(emf, along, d) for along in TANGENT[d]]
        both = jnp.concatenate([*planes[0], *planes[1]], axis=1)
        rows.append(mm_left(both, restrict[1 if d == 2 else 0]))
    rows = jnp.concatenate(rows, axis=0)
    nt = ((1,), (1,))
    key = (pairs[1] * 64 + (pairs[4] * 2 + pairs[5]) * CB + pairs[3] + 1).astype(F32)
    lane = lax.broadcasted_iota(jnp.int32, (PEERS, 128), 1)
    meta = jnp.zeros((PEERS, 128), F32)
    for k, chosen in enumerate((first, second)):
        pick = mm(chosen.astype(BF16), source.astype(BF16), nt)
        send[:, 0, k * 128 : (k + 1) * 128] = mm_right(pick.astype(BF16), rows)
        meta = jnp.where(lane == k, jnp.sum(chosen * key, axis=1, keepdims=True), meta)
    send[:, 0, 256:384] = meta


def coarse_kernel(cell, b_c, quadrant, emf, planes, quads):
    edges(cell, emf)
    for d in range(3):
        for t in range(2):
            at = (d * 2 + t) * CB
            face = face_of(emf, TANGENT[d][t], d)
            planes[at : at + CB, 0:128] = face[0]
            planes[at : at + CB, 128:256] = face[1]
        normal = jnp.concatenate(face_of(b_c, d, d), axis=1)
        quads[d * CB : (d + 1) * CB, :] = mm_left(normal, quadrant[1 if d == 2 else 0])


def answer_kernel(got, planes, quads_b, expand, quadrant, rows_b, rows_c, patch, masks):
    meta = got[:, 0, 256:384]
    keys = [meta[:, k : k + 1].astype(jnp.int32) - 1 for k in range(2)]
    target = lax.broadcasted_iota(jnp.int32, (PEERS, 256), 1)
    hit = jnp.concatenate([(k == target).astype(F32) for k in keys], axis=0).astype(BF16)
    rows = jnp.concatenate([got[:, 0, 0:128], got[:, 0, 128:256]], axis=0)
    tn = ((0,), (0,))
    replaced = mm_right(hit, rows, tn)[0:192]
    counted = mm(hit, jnp.ones((2 * PEERS, 128), BF16), tn)[0:192]
    spread = (mm_left(replaced, expand[0]), mm_left(replaced, expand[1]))
    lane = lax.broadcasted_iota(jnp.int32, (CB, 128), 1)

    def at(d, quad):
        return slice(d * 64 + quad * CB, d * 64 + (quad + 1) * CB)

    def value(d, t, flip):
        part = slice(t * 128, (t + 1) * 128)
        out = []
        for h in range(2):
            near, far = (h, h + 2) if flip else (2 * h, 2 * h + 1)
            x = spread[flip]
            out.append(x[at(d, near), part] + pltpu.roll(x[at(d, far), part], 8, 1))
        return tuple(out)

    def mask(d, flip):
        out = []
        for h in range(2):
            near, far = (h, h + 2) if flip else (2 * h, 2 * h + 1)
            out.append(jnp.where((lane & 15) < 8, counted[at(d, near)], counted[at(d, far)]) > 0.5)
        return tuple(out)

    value = {
        (d, t): value(d, t, int(d == 2)) for d in range(3) for t in range(2)
    } | {"1x": value(1, 0, 1), "2x": value(2, 0, 0)}
    hits = {d: mask(d, int(d == 2)) for d in range(3)} | {"1x": mask(1, 1), "2x": mask(2, 0)}
    for d in range(3):
        for h in range(2):
            side = slice(h * 128, (h + 1) * 128)
            masks[d * CB : (d + 1) * CB, side] = hits[d][h].astype(F32)
            for t in range(2):
                first = (d * 2 + t) * CB
                patch[first : first + CB, side] = value[d, t][h]

    def face(d, t):
        first = (d * 2 + t) * CB
        return planes[first : first + CB, 0:128], planes[first : first + CB, 128:256]

    both = lambda a, b: a & b
    column = ((lane & 15) == 0,) * 2
    row = (lane < 16, lane < 0)
    put = lambda m, new, old: each(jnp.where, m, new, old)
    ey_0 = put(hits[0], value[0, 0], face(0, 0))
    ez_0 = put(hits[0], value[0, 1], face(0, 1))
    ez_1 = put(each(both, row, hits[0]), value[0, 1], face(1, 1))
    ey_2 = put(each(both, column, hits[0]), value[0, 0], face(2, 1))
    ex_1 = put(hits[1], value[1, 0], face(1, 0))
    ez_1 = put(hits[1], value[1, 1], ez_1)
    ez_0 = put(each(both, row, hits[1]), value[1, 1], ez_0)
    ex_2 = put(each(both, row, hits["1x"]), value["1x"], face(2, 0))
    ex_2 = put(hits[2], value[2, 0], ex_2)
    ey_2 = put(hits[2], value[2, 1], ey_2)
    ex_1 = put(each(both, column, hits["2x"]), value["2x"], ex_1)
    ey_0 = put(each(both, column, hits[2]), value[2, 1], ey_0)
    curl = lambda p, q, r, s: (p - q) - (r - s)
    curls = (
        each(curl, y_next(ez_0), ez_0, z_next(ey_0), ey_0),
        each(curl, z_next(ex_1), ex_1, y_next(ez_1), ez_1),
        each(curl, z_next(ey_2), ey_2, y_next(ex_2), ex_2),
    )
    straight = jnp.concatenate(
        [jnp.concatenate(curls[0], axis=1), jnp.concatenate(curls[1], axis=1)], axis=0
    )
    quads_c = jnp.concatenate(
        [
            mm_left(straight, quadrant[0]),
            mm_left(jnp.concatenate(curls[2], axis=1), quadrant[1]),
        ],
        axis=0,
    )
    wide_lane = lax.broadcasted_iota(jnp.int32, (PEERS, 3 * CB), 1)
    out_lane = lax.broadcasted_iota(jnp.int32, (PEERS, 128), 1)
    for out, quads in ((rows_b, quads_b[...]), (rows_c, quads_c)):
        answers = []
        for k in range(2):
            key = keys[k]
            place = jnp.where(key >= 0, (key >> 6) * CB + (key & 15), -1)
            pick = (place == wide_lane).astype(F32).astype(BF16)
            found = mm_right(pick, quads)
            quad = (key >> 4) & 3
            side = jnp.where(quad >= 2, found[:, 128:256], found[:, 0:128])
            answers.append(jnp.where((quad & 1) == k, side, pltpu.roll(side, 64, 1)))
        out[:, 0, :] = jnp.where(out_lane < 64, answers[0], answers[1])


def update_kernel(
    top, emf_c, patch, masks, emf_f, b_c, b_f, new_c, new_f, normals, emf, out_c, out_f, sems
):
    time_step = 0.2 / top[0:1, 2:3]
    lane = lax.broadcasted_iota(jnp.int32, (CB, 128), 1)

    def pair(ref, first):
        return ref[first : first + CB, 0:128], ref[first : first + CB, 128:256]

    def update(emf, factor, load_b, store, done):
        for i in range(EDGE):
            following = (i + 1) % EDGE
            ex, ey, ez = (slab(emf, c, i, 0, CB) for c in range(3))
            ey_far, ez_far = (slab(emf, c, following, 0, CB) for c in (1, 2))
            curl = lambda b, p, q, r, s: b - factor * ((p - q) - (r - s))
            store(0, i, each(curl, load_b(0, i), y_next(ez), ez, z_next(ey), ey))
            store(1, i, each(curl, load_b(1, i), z_next(ex), ex, ez_far, ez))
            store(2, i, each(curl, load_b(2, i), ey_far, ey, y_next(ex), ex))
            done(i)

    update(
        emf_f,
        time_step / 0.5,
        lambda c, i: fine_slab(b_f, c, i),
        lambda c, i, value: put_fine_slab(out_f, c, i, value),
        lambda i: None,
    )
    results = [
        pltpu.make_async_copy(out_f.at[pl.ds(b * PITCH, 96)], new_f.at[b], sems.at[0])
        for b in range(FB)
    ]
    for copy in results:
        copy.start()

    planes = {(d, t): pair(patch, (d * 2 + t) * CB) for d in range(3) for t in range(2)}
    hits = [pair(masks, d * CB) for d in range(3)]
    for i in range(EDGE):
        now = {c: slab(emf_c, c, i, 0, CB) for c in range(3)}
        if i == 0:
            for t, c in enumerate(TANGENT[0]):
                now[c] = each(lambda m, p, e: jnp.where(m > 0.5, p, e), hits[0], planes[0, t], now[c])
        turn, h = (8 - i % 8) % 8 * 16, i // 8
        there = (lane < 16) & (pltpu.roll(hits[1][h], turn, 1) > 0.5)
        for t, c in enumerate(TANGENT[1]):
            now[c] = (jnp.where(there, pltpu.roll(planes[1, t][h], turn, 1), now[c][0]), now[c][1])
        turn = (128 - i) % 128
        there = [((lane & 15) == 0) & (pltpu.roll(m, turn, 1) > 0.5) for m in hits[2]]
        for t, c in enumerate(TANGENT[2]):
            value = [pltpu.roll(p, turn, 1) for p in planes[2, t]]
            now[c] = each(jnp.where, there, value, now[c])
        for c in range(3):
            put_slab(emf, c, i, 0, CB, now[c])

    def send_chunk(i):
        if i % 4 == 3:
            part = pl.ds((i - 3) * WIDE, 4 * WIDE)
            copy = pltpu.make_async_copy(out_c.at[:, :, part], new_c.at[:, :, part], sems.at[1])
            copy.start()
            results.append(copy)

    update(
        emf,
        time_step,
        lambda c, i: slab(b_c, c, i, 0, CB),
        lambda c, i, value: put_slab(out_c, c, i, 0, CB, value),
        send_chunk,
    )
    faces = (
        fine_slab(out_f, 0, 0),
        face_row_wise(lambda i: fine_slab(out_f, 1, i)[0]),
        face_column_wise(lambda i: fine_slab(out_f, 2, i)),
    )
    for d in range(3):
        normals[d * CB : (d + 1) * CB, 0:128] = faces[d][0]
        normals[d * CB : (d + 1) * CB, 128:256] = faces[d][1]
    for copy in results:
        copy.wait()


def third_kernel(got, normals, pairs, flip, prolong, jump):
    first, second, source = routes(pairs)
    tn = ((0,), (0,))
    rows = got[:, 0, :]
    lane = lax.broadcasted_iota(jnp.int32, (PAIRS, 128), 1)
    own = jnp.where(
        lane < 64,
        mm_right(first.astype(BF16), rows, tn),
        mm_right(second.astype(BF16), rows, tn),
    )
    coarse = mm_left(own, prolong[...])
    source = source.astype(BF16)
    straight = mm_right(source[0 : 2 * CB], normals[0 : 2 * CB], tn)
    flipped = mm_left(mm_right(source[2 * CB :], normals[2 * CB :], tn), flip[...])
    jump[...] = straight + flipped - coarse


VMEM = pl.BlockSpec(memory_space=pltpu.VMEM)
HBM = pl.BlockSpec(memory_space=pltpu.HBM)
FIELD = (3, CB, CELLS)
PITCHED = (CB * PITCH, 128)


def call(kernel, name, outs, args, scratch=()):
    far = [isinstance(out, tuple) and out[0] == "hbm" for out in outs]
    return pl.pallas_call(
        kernel,
        out_shape=[
            pltpu.HBM(out[1], F32) if is_far else pltpu.VMEM(out, F32)
            for out, is_far in zip(outs, far)
        ],
        in_specs=[HBM if is_far else VMEM for _, is_far in args],
        out_specs=[HBM if is_far else VMEM for is_far in far],
        scratch_shapes=list(scratch),
        compiler_params=pltpu.CompilerParams(vmem_limit_bytes=24 * 1024 * 1024),
        name=name,
    )(
        *(
            pltpu.with_memory_space_constraint(a, pltpu.HBM if is_far else pltpu.VMEM)
            for a, is_far in args
        )
    )


def on_device(coarse_field, coarse_velocity, fine_field, fine_velocity, pairs):
    cb = coarse_field[0].transpose(1, 0, 2)
    cv = coarse_velocity[0].transpose(1, 0, 2)
    fb = fine_field[0].reshape(FB, 96, 128)
    fv = fine_velocity[0].reshape(FB, 96, 128)
    rows = pairs.transpose(2, 0, 1)
    restrict, expand, quadrant, flip, prolong = (
        jnp.asarray(x, BF16) for x in (RESTRICT, EXPAND, QUADRANT, FLIP, PROLONG)
    )
    near = lambda *arrays: [(a, False) for a in arrays]
    far = lambda *arrays: [(a, True) for a in arrays]
    count = lax.axis_size("gz")

    cell_c, cell_f, b_c, b_f, speed = call(
        cells_kernel,
        "cells",
        [FIELD, FIELD, FIELD, PITCHED, (1, 128)],
        far(cb, cv, fb, fv),
        [pltpu.VMEM(FIELD, F32), pltpu.VMEM(PITCHED, F32), pltpu.SemaphoreType.DMA((4,))],
    )
    other = lax.ppermute(speed, "gz", [(i, i ^ 1) for i in range(count)])
    send, emf_f = call(
        rows_kernel, "rows", [(PEERS, 1, 384), FIELD], near(cell_f, rows, restrict)
    )
    speed = jnp.maximum(speed, other)
    lane = lax.broadcasted_iota(jnp.int32, send.shape, 2)
    send = jnp.where(lane == 258, speed[0, 0], send)
    got = lax.all_to_all(send, BLOCKS, 0, 0, tiled=True)
    emf_c, planes, quads = call(
        coarse_kernel,
        "coarse_edges",
        [FIELD, (6 * CB, WIDE), (3 * CB, WIDE)],
        near(cell_c, b_c, quadrant),
    )
    top = jnp.max(got[:, :, 256:384], axis=0)
    other = lax.ppermute(top, "gz", [(i, i ^ 2) for i in range(count)])
    rows_b, rows_c, patch, masks = call(
        answer_kernel,
        "answers",
        [(PEERS, 1, 128), (PEERS, 1, 128), (6 * CB, WIDE), (3 * CB, WIDE)],
        near(got, planes, quads, expand, quadrant),
    )
    top = jnp.maximum(top, other)
    back = rows_b - (0.2 / top[0, 2]) * rows_c
    returned = lax.all_to_all(back, BLOCKS, 0, 0, tiled=True)
    new_c, new_f, normals = call(
        update_kernel,
        "updates",
        [("hbm", FIELD), ("hbm", (FB, 96, 128)), (3 * CB, WIDE)],
        near(top, emf_c, patch, masks, emf_f, b_c, b_f),
        [
            pltpu.VMEM(FIELD, F32),
            pltpu.VMEM(FIELD, F32),
            pltpu.VMEM(PITCHED, F32),
            pltpu.SemaphoreType.DMA((2,)),
        ],
    )
    (jump,) = call(
        third_kernel,
        "face_jumps",
        [(PAIRS, WIDE)],
        near(returned, normals, rows, flip, prolong),
    )
    return (
        new_c.transpose(1, 0, 2)[None],
        new_f.reshape(1, FB, 3, CELLS),
        jump[None],
    )


def solution(mesh):
    split = Mesh(
        mesh.devices.reshape(4, 8, 2, mesh.shape["gz"]), ("blocks_0", "blocks_1", "blocks_2", "gz")
    )
    in_specs = (
        P("gz", BLOCKS, None, None),
        P("gz", BLOCKS, None, None),
        P("gz", BLOCKS, None, None),
        P("gz", BLOCKS, None, None),
        P("gz", BLOCKS, None),
    )
    out_specs = (P("gz", BLOCKS, None, None), P("gz", BLOCKS, None, None), P("gz", BLOCKS, None))
    return jax.shard_map(
        on_device, mesh=split, in_specs=in_specs, out_specs=out_specs, check_vma=False
    )
```

```python
import jax
import jax.numpy as jnp
from jax import lax
from jax.experimental import pallas as pl
from jax.experimental.pallas import tpu as pltpu
from jax.sharding import Mesh
from jax.sharding import PartitionSpec as P

EDGE = 16
HALF = 8
CB = 16
FB = 12
PAIRS = 32
PEERS = 64
WIDE = EDGE * EDGE
CELLS = EDGE**3
PITCH = 104
BLOCKS = ("blocks_0", "blocks_1", "blocks_2")
F32 = jnp.float32
BF16 = jnp.bfloat16
TANGENT = ((1, 2), (0, 2), (0, 1))
UNROLL = 16


def grid_of(rows, cols):
    return (
        lax.broadcasted_iota(jnp.int32, (rows, cols), 0),
        lax.broadcasted_iota(jnp.int32, (1, cols), 1),
    )


def face_lane(row, col, flip):
    return col * EDGE + row if flip else row * EDGE + col


def as_matrix(where, value=1.0):
    return jnp.where(where, value, 0.0).astype(BF16)


def restrict_matrix(flip):
    at, to = grid_of(WIDE, 128)
    m, n = (to >> 3) & 7, to & 7
    base = face_lane(2 * m, 2 * n, flip)
    firsts = (to < 64) & ((at == base) | (at == base + face_lane(1, 0, flip)))
    seconds = (to >= 64) & ((at == base) | (at == base + face_lane(0, 1, flip)))
    return jnp.concatenate([as_matrix(firsts, 0.5), as_matrix(seconds, 0.5)], axis=0)


def expand_matrix(flip):
    at, _ = grid_of(128, 256)
    to = lax.broadcasted_iota(jnp.int32, (128, 256), 1)
    place = face_lane((at >> 3) & 7, at & 7, flip)
    return as_matrix(((at >> 6) == (to >> 7)) & (place == (to & 127)))


def quadrant_matrix(flip):
    at, to = grid_of(WIDE, WIDE)
    row, col = (to >> 7) * HALF + ((to >> 3) & 7), ((to >> 6) & 1) * HALF + (to & 7)
    return as_matrix(at == face_lane(row, col, flip))


def flip_matrix():
    at, to = grid_of(WIDE, WIDE)
    return as_matrix(at == (to & 15) * EDGE + (to >> 4))


def prolong_matrix():
    at, to = grid_of(128, WIDE)
    return as_matrix((at & 63) == (to >> 5) * HALF + ((to & 15) >> 1))


def halves(value):
    high = value.astype(BF16)
    return high, (value - high.astype(F32)).astype(BF16)


def mm(a, b, dims=((1,), (0,))):
    return lax.dot_general(a, b, (dims, ((), ())), preferred_element_type=F32)


def mm_left(value, matrix, dims=((1,), (0,))):
    high, low = halves(value)
    return mm(high, matrix, dims) + mm(low, matrix, dims)


def mm_right(matrix, value, dims=((1,), (0,))):
    high, low = halves(value)
    return mm(matrix, high, dims) + mm(matrix, low, dims)


def lanes_of(value):
    return lax.broadcasted_iota(jnp.int32, value.shape, 1)


def y_prev(p):
    a, b = pltpu.roll(p[0], 16, 1), pltpu.roll(p[1], 16, 1)
    edge = lanes_of(a) < 16
    return jnp.where(edge, b, a), jnp.where(edge, a, b)


def y_next(p):
    a, b = pltpu.roll(p[0], 112, 1), pltpu.roll(p[1], 112, 1)
    edge = lanes_of(a) >= 112
    return jnp.where(edge, b, a), jnp.where(edge, a, b)


def z_prev(p):
    edge = (lanes_of(p[0]) & 15) == 0
    return tuple(jnp.where(edge, pltpu.roll(x, 113, 1), pltpu.roll(x, 1, 1)) for x in p)


def z_next(p):
    edge = (lanes_of(p[0]) & 15) == 15
    return tuple(jnp.where(edge, pltpu.roll(x, 15, 1), pltpu.roll(x, 127, 1)) for x in p)


def each(fn, *pairs):
    return tuple(fn(*(p[h] for p in pairs)) for h in range(2))


def span(i, half):
    start = i * WIDE + half * 128
    return pl.ds(start if isinstance(start, int) else pl.multiple_of(start, 128), 128)


def slab(ref, comp, i, first, count):
    return tuple(ref[comp, first : first + count, span(i, half)] for half in range(2))


def put_slab(ref, comp, i, first, count, value):
    for half in range(2):
        ref[comp, first : first + count, span(i, half)] = value[half]


def fine_slab(ref, comp, i):
    def one(half):
        start = comp * 32 + 2 * i + half
        return jnp.concatenate(
            [
                ref[pl.ds(start, 8, stride=PITCH), :],
                ref[pl.ds(start + 8 * PITCH, 8, stride=PITCH), :],
            ],
            axis=0,
        )

    return one(0), one(1)


def put_fine_slab(ref, comp, i, value):
    for half in range(2):
        start = comp * 32 + 2 * i + half
        ref[pl.ds(start, 8, stride=PITCH), :] = value[half][0:8]
        ref[pl.ds(start + 8 * PITCH, 8, stride=PITCH), :] = value[half][8:16]


def fetch_fine(source, target, sem):
    return [
        pltpu.make_async_copy(source.at[b], target.at[pl.ds(b * PITCH, 96)], sem)
        for b in range(FB)
    ]


def face_row_wise(load):
    out = [jnp.zeros((CB, 128), F32)] * 2
    group = lax.broadcasted_iota(jnp.int32, (CB, 128), 1) // 16
    for i in range(EDGE):
        turned = pltpu.roll(load(i), i % 8 * 16, 1)
        out[i // 8] = jnp.where(group == i % 8, turned, out[i // 8])
    return tuple(out)


def face_column_wise(load):
    out = (jnp.zeros((CB, 128), F32),) * 2
    column = lax.broadcasted_iota(jnp.int32, (CB, 128), 1) & 15
    for i in range(EDGE):
        out = each(lambda x, h: jnp.where(column == i, pltpu.roll(x, i, 1), h), load(i), out)
    return out


def routes(pairs_ref):
    slot, face, owner = pairs_ref[0], pairs_ref[1], pairs_ref[2]
    peer = lax.broadcasted_iota(jnp.int32, (PEERS, PAIRS), 0)
    named = (owner == peer).astype(F32)
    before = (
        lax.broadcasted_iota(jnp.int32, (PAIRS, PAIRS), 0)
        < lax.broadcasted_iota(jnp.int32, (PAIRS, PAIRS), 1)
    ).astype(F32)
    earlier = mm(named.astype(BF16), before.astype(BF16))
    rank = jnp.sum(named * earlier, axis=0, keepdims=True)
    first = jnp.where(rank < 0.5, named, 0.0)
    second = jnp.where(rank < 0.5, 0.0, named)
    at_row = lax.broadcasted_iota(jnp.int32, (3 * CB, PAIRS), 0)
    source = (face * CB + slot == at_row).astype(F32)
    return first, second, source


def edges(cell, emf):
    last = [slab(cell, c, EDGE - 1, 0, CB) for c in range(3)]
    now = last
    add = lambda a, b: a + b
    quarter = lambda a, b: 0.25 * (a + b)
    for i in reversed(range(EDGE)):
        prior = [slab(cell, c, i - 1, 0, CB) for c in range(3)] if i else last
        sum_x = each(add, now[0], y_prev(now[0]))
        sum_y = each(add, now[1], prior[1])
        sum_z = each(add, now[2], prior[2])
        put_slab(emf, 0, i, 0, CB, each(quarter, sum_x, z_prev(sum_x)))
        put_slab(emf, 1, i, 0, CB, each(quarter, sum_y, z_prev(sum_y)))
        put_slab(emf, 2, i, 0, CB, each(quarter, sum_z, y_prev(sum_z)))
        now = prior


def face_of(ref, along, d):
    if d == 0:
        return slab(ref, along, 0, 0, CB)
    if d == 1:
        return face_row_wise(lambda i: slab(ref, along, i, 0, CB)[0])
    return face_column_wise(lambda i: slab(ref, along, i, 0, CB))


def first_kernel(
    cb, cv, fb, fv, far_pairs,
    send, cell_c, emf_f, b_f,
    b_c, v_c, pitched_b, v_f, pairs, out, sems,
):
    fine_copies = fetch_fine(fb, pitched_b, sems.at[0]) + fetch_fine(fv, v_f, sems.at[1])
    coarse_copies = [
        [
            pltpu.make_async_copy(far.at[:, :, part], near.at[:, :, part], sems.at[2 + q])
            for far, near in ((cb, b_c), (cv, v_c))
        ]
        for q, part in enumerate(pl.ds(q * 4 * WIDE, 4 * WIDE) for q in range(4))
    ]
    pairs_copy = pltpu.make_async_copy(far_pairs, pairs, sems.at[6])
    for copy in [pairs_copy, *fine_copies, *sum(coarse_copies, [])]:
        copy.start()
    idle = pl.ds(FB * PITCH, (CB - FB) * PITCH)
    pitched_b[idle, :] = jnp.zeros(((CB - FB) * PITCH, 128), F32)
    v_f[idle, :] = jnp.zeros(((CB - FB) * PITCH, 128), F32)
    pairs_copy.wait()
    first, second, source = routes(pairs)
    nt = ((1,), (1,))
    key = (pairs[1] * 64 + (pairs[4] * 2 + pairs[5]) * CB + pairs[3] + 1).astype(F32)
    lane = lax.broadcasted_iota(jnp.int32, (PEERS, 128), 1)
    meta = jnp.zeros((PEERS, 128), F32)
    picks = []
    for k, chosen in enumerate((first, second)):
        picks.append(mm(chosen.astype(BF16), source.astype(BF16), nt).astype(BF16))
        meta = jnp.where(lane == k, jnp.sum(chosen * key, axis=1, keepdims=True), meta)

    def cells(load_b, load_v, cell, ready):
        top = jnp.zeros((CB, 128), F32)
        for i in range(EDGE):
            ready(i)
            bx, by, bz = load_b(0, i), load_b(1, i), load_b(2, i)
            vx, vy, vz = load_v(0, i), load_v(1, i), load_v(2, i)
            mean = lambda a, b: 0.5 * (a + b)
            cx = each(mean, bx, load_b(0, (i + 1) % EDGE))
            cy = each(mean, by, y_next(by))
            cz = each(mean, bz, z_next(bz))
            cross = lambda a, b, c, d: a * b - c * d
            put_slab(cell, 0, i, 0, CB, each(cross, vz, cy, vy, cz))
            put_slab(cell, 1, i, 0, CB, each(cross, vx, cz, vz, cx))
            put_slab(cell, 2, i, 0, CB, each(cross, vy, cx, vx, cy))
            size = lambda a, b, c: jnp.sqrt(a * a + b * b + c * c)
            fast = each(lambda a, b: a + b, each(size, vx, vy, vz), each(size, cx, cy, cz))
            top = jnp.maximum(top, jnp.maximum(fast[0], fast[1]))
        return top

    for copy in fine_copies:
        copy.wait()
    held = {}

    def fine_b(c, i):
        if (c, i) not in held:
            held[c, i] = fine_slab(pitched_b, c, i)
            put_slab(b_f, c, i, 0, CB, held[c, i])
        return held[c, i]

    top_fine = cells(fine_b, lambda c, i: fine_slab(v_f, c, i), emf_f, lambda i: None)
    edges(emf_f, emf_f)
    restrict = [restrict_matrix(False), restrict_matrix(True)]
    rows = []
    for d in range(3):
        planes = [face_of(emf_f, along, d) for along in TANGENT[d]]
        both = jnp.concatenate([*planes[0], *planes[1]], axis=1)
        rows.append(mm_left(both, restrict[1 if d == 2 else 0]))
    rows = jnp.concatenate(rows, axis=0)
    for k in range(2):
        out[:, 0, k * 128 : (k + 1) * 128] = mm_right(picks[k], rows)
    rows_copy = pltpu.make_async_copy(
        out.at[:, :, pl.ds(0, 256)], send.at[:, :, pl.ds(0, 256)], sems.at[7]
    )
    rows_copy.start()

    def coarse_ready(i):
        for q in range(4):
            if i == max(4 * q - 1, 0):
                for copy in coarse_copies[q]:
                    copy.wait()

    top_coarse = cells(
        lambda c, i: slab(b_c, c, i, 0, CB),
        lambda c, i: slab(v_c, c, i, 0, CB),
        cell_c,
        coarse_ready,
    )
    top = jnp.max(jnp.maximum(top_fine, top_coarse), axis=0, keepdims=True)
    top = jnp.broadcast_to(jnp.max(top, axis=1, keepdims=True), (PEERS, 128))
    out[:, 0, 256:384] = jnp.where(lane < 2, meta, top)
    meta_copy = pltpu.make_async_copy(
        out.at[:, :, pl.ds(256, 128)], send.at[:, :, pl.ds(256, 128)], sems.at[8]
    )
    meta_copy.start()
    rows_copy.wait()
    meta_copy.wait()


def coarse_kernel(cell, cb, emf, far_planes, quads, b_c, planes, sems):
    load = pltpu.make_async_copy(cb, b_c, sems.at[0])
    load.start()
    edges(cell, emf)
    for d in range(3):
        for t in range(2):
            at = (d * 2 + t) * CB
            face = face_of(emf, TANGENT[d][t], d)
            planes[at : at + CB, 0:128] = face[0]
            planes[at : at + CB, 128:256] = face[1]
    store = pltpu.make_async_copy(planes, far_planes, sems.at[1])
    store.start()
    quadrant = [quadrant_matrix(False), quadrant_matrix(True)]
    load.wait()
    for d in range(3):
        normal = jnp.concatenate(face_of(b_c, d, d), axis=1)
        quads[d * CB : (d + 1) * CB, :] = mm_left(normal, quadrant[1 if d == 2 else 0])
    store.wait()


def answer_kernel(
    got, far_planes, quads_b, cb, back, far_patch, masks, b_c, planes, patch, out, sems
):
    load = pltpu.make_async_copy(cb, b_c, sems.at[0])
    load_planes = pltpu.make_async_copy(far_planes, planes, sems.at[1])
    load_planes.start()
    load.start()
    expand = [expand_matrix(False), expand_matrix(True)]
    quadrant = [quadrant_matrix(False), quadrant_matrix(True)]
    meta = got[:, 0, 256:384]
    keys = [meta[:, k : k + 1].astype(jnp.int32) - 1 for k in range(2)]
    target = lax.broadcasted_iota(jnp.int32, (PEERS, 256), 1)
    hit = jnp.concatenate([(k == target).astype(F32) for k in keys], axis=0).astype(BF16)
    rows = jnp.concatenate([got[:, 0, 0:128], got[:, 0, 128:256]], axis=0)
    tn = ((0,), (0,))
    replaced = mm_right(hit, rows, tn)[0:192]
    counted = mm(hit, jnp.ones((2 * PEERS, 128), BF16), tn)[0:192]
    spread = (mm_left(replaced, expand[0]), mm_left(replaced, expand[1]))
    lane = lax.broadcasted_iota(jnp.int32, (CB, 128), 1)

    def at(d, quad):
        return slice(d * 64 + quad * CB, d * 64 + (quad + 1) * CB)

    def value(d, t, flip):
        part = slice(t * 128, (t + 1) * 128)
        out = []
        for h in range(2):
            near, far = (h, h + 2) if flip else (2 * h, 2 * h + 1)
            x = spread[flip]
            out.append(x[at(d, near), part] + pltpu.roll(x[at(d, far), part], 8, 1))
        return tuple(out)

    def mask(d, flip):
        out = []
        for h in range(2):
            near, far = (h, h + 2) if flip else (2 * h, 2 * h + 1)
            out.append(jnp.where((lane & 15) < 8, counted[at(d, near)], counted[at(d, far)]) > 0.5)
        return tuple(out)

    value = {
        (d, t): value(d, t, int(d == 2)) for d in range(3) for t in range(2)
    } | {"1x": value(1, 0, 1), "2x": value(2, 0, 0)}
    hits = {d: mask(d, int(d == 2)) for d in range(3)} | {"1x": mask(1, 1), "2x": mask(2, 0)}
    for h in range(2):
        side = slice(h * 128, (h + 1) * 128)
        masks[:, side] = sum(hits[d][h].astype(F32) * 2.0**d for d in range(3))
        for d in range(3):
            for t in range(2):
                first = (d * 2 + t) * CB
                patch[first : first + CB, side] = value[d, t][h]

    store = pltpu.make_async_copy(patch, far_patch, sems.at[2])
    store.start()
    load_planes.wait()

    def face(d, t):
        first = (d * 2 + t) * CB
        return planes[first : first + CB, 0:128], planes[first : first + CB, 128:256]

    both = lambda a, b: a & b
    column = ((lane & 15) == 0,) * 2
    row = (lane < 16, lane < 0)
    put = lambda m, new, old: each(jnp.where, m, new, old)
    ey_0 = put(hits[0], value[0, 0], face(0, 0))
    ez_0 = put(hits[0], value[0, 1], face(0, 1))
    ez_1 = put(each(both, row, hits[0]), value[0, 1], face(1, 1))
    ey_2 = put(each(both, column, hits[0]), value[0, 0], face(2, 1))
    ex_1 = put(hits[1], value[1, 0], face(1, 0))
    ez_1 = put(hits[1], value[1, 1], ez_1)
    ez_0 = put(each(both, row, hits[1]), value[1, 1], ez_0)
    ex_2 = put(each(both, row, hits["1x"]), value["1x"], face(2, 0))
    ex_2 = put(hits[2], value[2, 0], ex_2)
    ey_2 = put(hits[2], value[2, 1], ey_2)
    ex_1 = put(each(both, column, hits["2x"]), value["2x"], ex_1)
    ey_0 = put(each(both, column, hits[2]), value[2, 1], ey_0)
    curl = lambda p, q, r, s: (p - q) - (r - s)
    curls = (
        each(curl, y_next(ez_0), ez_0, z_next(ey_0), ey_0),
        each(curl, z_next(ex_1), ex_1, y_next(ez_1), ez_1),
        each(curl, z_next(ey_2), ey_2, y_next(ex_2), ex_2),
    )
    straight = jnp.concatenate(
        [jnp.concatenate(curls[0], axis=1), jnp.concatenate(curls[1], axis=1)], axis=0
    )
    quads_c = jnp.concatenate(
        [
            mm_left(straight, quadrant[0]),
            mm_left(jnp.concatenate(curls[2], axis=1), quadrant[1]),
        ],
        axis=0,
    )
    wide_lane = lax.broadcasted_iota(jnp.int32, (PEERS, 3 * CB), 1)
    out_lane = lax.broadcasted_iota(jnp.int32, (PEERS, 128), 1)
    for part, quads in enumerate((quads_b[...], quads_c)):
        answers = []
        for k in range(2):
            key = keys[k]
            place = jnp.where(key >= 0, (key >> 6) * CB + (key & 15), -1)
            pick = (place == wide_lane).astype(F32).astype(BF16)
            found = mm_right(pick, quads)
            quad = (key >> 4) & 3
            side = jnp.where(quad >= 2, found[:, 128:256], found[:, 0:128])
            answers.append(jnp.where((quad & 1) == k, side, pltpu.roll(side, 64, 1)))
        side = slice(part * 128, (part + 1) * 128)
        out[:, 0, side] = jnp.where(out_lane < 64, answers[0], answers[1])
    send = pltpu.make_async_copy(out, back, sems.at[3])
    send.start()
    for copy in (load, store, send):
        copy.wait()


def update_kernel(
    top, emf_c, far_patch, masks, emf_f, b_c, b_f, far_pairs,
    new_c, new_f, picked, chosen,
    emf, out_c, out_f, pairs, patch, sems,
):
    load = pltpu.make_async_copy(far_pairs, pairs, sems.at[2])
    load_patch = pltpu.make_async_copy(far_patch, patch, sems.at[3])
    load_patch.start()
    load.start()
    time_step = 0.2 / top[0:1, 2:3]
    lane = lax.broadcasted_iota(jnp.int32, (CB, 128), 1)

    def pair(ref, first):
        return ref[first : first + CB, 0:128], ref[first : first + CB, 128:256]

    def update(emf, factor, load_b, store, done):
        for i in range(EDGE):
            following = (i + 1) % EDGE
            ex, ey, ez = (slab(emf, c, i, 0, CB) for c in range(3))
            ey_far, ez_far = (slab(emf, c, following, 0, CB) for c in (1, 2))
            curl = lambda b, p, q, r, s: b - factor * ((p - q) - (r - s))
            store(0, i, each(curl, load_b(0, i), y_next(ez), ez, z_next(ey), ey))
            store(1, i, each(curl, load_b(1, i), z_next(ex), ex, ez_far, ez))
            store(2, i, each(curl, load_b(2, i), ey_far, ey, y_next(ex), ex))
            done(i)

    update(
        emf_f,
        time_step / 0.5,
        lambda c, i: slab(b_f, c, i, 0, CB),
        lambda c, i, value: put_fine_slab(out_f, c, i, value),
        lambda i: None,
    )
    results = [
        pltpu.make_async_copy(out_f.at[pl.ds(b * PITCH, 96)], new_f.at[b], sems.at[0])
        for b in range(FB)
    ]
    for copy in results:
        copy.start()

    load_patch.wait()
    planes = {(d, t): pair(patch, (d * 2 + t) * CB) for d in range(3) for t in range(2)}
    bits = [m.astype(jnp.int32) for m in pair(masks, 0)]
    hits = [[((m >> d) & 1).astype(F32) for m in bits] for d in range(3)]
    for i in range(EDGE):
        now = {c: slab(emf_c, c, i, 0, CB) for c in range(3)}
        if i == 0:
            for t, c in enumerate(TANGENT[0]):
                now[c] = each(lambda m, p, e: jnp.where(m > 0.5, p, e), hits[0], planes[0, t], now[c])
        turn, h = (8 - i % 8) % 8 * 16, i // 8
        there = (lane < 16) & (pltpu.roll(hits[1][h], turn, 1) > 0.5)
        for t, c in enumerate(TANGENT[1]):
            now[c] = (jnp.where(there, pltpu.roll(planes[1, t][h], turn, 1), now[c][0]), now[c][1])
        turn = (128 - i) % 128
        there = [((lane & 15) == 0) & (pltpu.roll(m, turn, 1) > 0.5) for m in hits[2]]
        for t, c in enumerate(TANGENT[2]):
            value = [pltpu.roll(p, turn, 1) for p in planes[2, t]]
            now[c] = each(jnp.where, there, value, now[c])
        for c in range(3):
            put_slab(emf, c, i, 0, CB, now[c])

    def send_chunk(i):
        if i % 4 == 3:
            part = pl.ds((i - 3) * WIDE, 4 * WIDE)
            copy = pltpu.make_async_copy(out_c.at[:, :, part], new_c.at[:, :, part], sems.at[1])
            copy.start()
            results.append(copy)

    update(
        emf,
        time_step,
        lambda c, i: slab(b_c, c, i, 0, CB),
        lambda c, i, value: put_slab(out_c, c, i, 0, CB, value),
        send_chunk,
    )
    faces = (
        fine_slab(out_f, 0, 0),
        face_row_wise(lambda i: fine_slab(out_f, 1, i)[0]),
        face_column_wise(lambda i: fine_slab(out_f, 2, i)),
    )
    load.wait()
    first, second, source = routes(pairs)
    tn = ((0,), (0,))
    same = (
        lax.broadcasted_iota(jnp.int32, (PEERS, PEERS), 0)
        == lax.broadcasted_iota(jnp.int32, (PEERS, PEERS), 1)
    ).astype(F32).astype(BF16)
    chosen[...] = jnp.concatenate(
        [mm(first.astype(BF16), same, tn), mm(second.astype(BF16), same, tn)], axis=1
    )
    source = source.astype(BF16)
    flip = flip_matrix()
    normals = [jnp.concatenate(face, axis=1) for face in faces]
    straight = mm_right(source[0 : 2 * CB], jnp.concatenate(normals[0:2], axis=0), tn)
    flipped = mm_left(mm_right(source[2 * CB :], normals[2], tn), flip)
    picked[...] = straight + flipped
    for copy in results:
        copy.wait()


def third_kernel(got, top, picked, chosen, jump, held, sems):
    rows = got[:, 0, 0:128] - (0.2 / top[0:1, 2:3]) * got[:, 0, 128:256]
    lane = lax.broadcasted_iota(jnp.int32, (PAIRS, 128), 1)
    picks = chosen[...].astype(BF16)
    sides = [mm_right(picks[:, k * PEERS : (k + 1) * PEERS], rows) for k in range(2)]
    own = jnp.where(lane < 64, sides[0], sides[1])
    held[...] = picked[...] - mm_left(own, prolong_matrix())
    copy = pltpu.make_async_copy(held, jump, sems.at[0])
    copy.start()
    copy.wait()


VMEM = pl.BlockSpec(memory_space=pltpu.VMEM)
HBM = pl.BlockSpec(memory_space=pltpu.HBM)
FIELD = (3, CB, CELLS)
PITCHED = (CB * PITCH, 128)
FACES = (6 * CB, WIDE)


def call(kernel, name, outs, args, scratch=(), aliases=None):
    far = [isinstance(out, tuple) and out[0] == "hbm" for out in outs]
    return pl.pallas_call(
        kernel,
        out_shape=[
            pltpu.HBM(out[1], F32) if is_far else pltpu.VMEM(out, F32)
            for out, is_far in zip(outs, far)
        ],
        in_specs=[HBM if is_far else VMEM for _, is_far in args],
        out_specs=[HBM if is_far else VMEM for is_far in far],
        scratch_shapes=list(scratch),
        input_output_aliases=aliases or {},
        compiler_params=pltpu.CompilerParams(vmem_limit_bytes=24 * 1024 * 1024),
        name=name,
    )(
        *(
            pltpu.with_memory_space_constraint(a, pltpu.HBM if is_far else pltpu.VMEM)
            for a, is_far in args
        )
    )


def on_device(coarse_field, coarse_velocity, fine_field, fine_velocity, pairs):
    cb = coarse_field[0].transpose(1, 0, 2)
    cv = coarse_velocity[0].transpose(1, 0, 2)
    fb = fine_field[0].reshape(FB, 96, 128)
    fv = fine_velocity[0].reshape(FB, 96, 128)
    rows = pairs.transpose(2, 0, 1)
    near = lambda *arrays: [(a, False) for a in arrays]
    far = lambda *arrays: [(a, True) for a in arrays]
    count = lax.axis_size("gz")

    field = pltpu.VMEM(FIELD, F32)
    pitched = pltpu.VMEM(PITCHED, F32)
    small = pltpu.VMEM((6, 1, PAIRS), jnp.int32)
    sems = pltpu.SemaphoreType.DMA
    send, cell_c, emf_f, b_f = call(
        first_kernel,
        "speeds_and_rows",
        [("hbm", (PEERS, 1, 384)), FIELD, FIELD, FIELD],
        far(cb, cv, fb, fv, rows),
        [field, field, pitched, pitched, small, pltpu.VMEM((PEERS, 1, 384), F32), sems((9,))],
    )
    got = lax.all_to_all(send, BLOCKS, 0, 0, tiled=True)
    emf_c, planes, quads = call(
        coarse_kernel,
        "coarse_edges",
        [FIELD, ("hbm", FACES), (3 * CB, WIDE)],
        near(cell_c) + far(cb),
        [field, pltpu.VMEM(FACES, F32), sems((2,))],
        {0: 0},
    )
    got, emf_c, planes, quads = lax.optimization_barrier((got, emf_c, planes, quads))
    top = jnp.max(got[:, :, 256:384], axis=0)
    top = jnp.maximum(top, lax.ppermute(top, "gz", [(i, i ^ 1) for i in range(count)]))
    back, patch, masks, b_c = call(
        answer_kernel,
        "answers",
        [("hbm", (PEERS, 1, 256)), ("hbm", FACES), (CB, WIDE), FIELD],
        near(got) + far(planes) + near(quads) + far(cb),
        [
            pltpu.VMEM(FACES, F32),
            pltpu.VMEM(FACES, F32),
            pltpu.VMEM((PEERS, 1, 256), F32),
            sems((4,)),
        ],
    )
    back, top = lax.optimization_barrier((back, top))
    top = jnp.maximum(top, lax.ppermute(top, "gz", [(i, i ^ 2) for i in range(count)]))
    returned = lax.all_to_all(back, BLOCKS, 0, 0, tiled=True)
    new_c, new_f, picked, chosen = call(
        update_kernel,
        "updates",
        [("hbm", FIELD), ("hbm", (FB, 96, 128)), (PAIRS, WIDE), (PAIRS, 128)],
        near(top, emf_c) + far(patch) + near(masks, emf_f, b_c, b_f) + far(rows),
        [field, field, pitched, small, pltpu.VMEM(FACES, F32), sems((4,))],
    )
    (jump,) = call(
        third_kernel,
        "face_jumps",
        [("hbm", (PAIRS, WIDE))],
        near(returned, top, picked, chosen),
        [pltpu.VMEM((PAIRS, WIDE), F32), sems((1,))],
    )
    return (
        new_c.transpose(1, 0, 2)[None],
        new_f.reshape(1, FB, 3, CELLS),
        jump[None],
    )


def solution(mesh):
    split = Mesh(
        mesh.devices.reshape(4, 8, 2, mesh.shape["gz"]), ("blocks_0", "blocks_1", "blocks_2", "gz")
    )
    in_specs = (
        P("gz", BLOCKS, None, None),
        P("gz", BLOCKS, None, None),
        P("gz", BLOCKS, None, None),
        P("gz", BLOCKS, None, None),
        P("gz", BLOCKS, None),
    )
    out_specs = (P("gz", BLOCKS, None, None), P("gz", BLOCKS, None, None), P("gz", BLOCKS, None))
    return jax.shard_map(
        on_device, mesh=split, in_specs=in_specs, out_specs=out_specs, check_vma=False
    )
```

```python
import jax
import jax.numpy as jnp
from jax import lax
from jax.experimental import pallas as pl
from jax.experimental.pallas import tpu as pltpu
from jax.sharding import Mesh
from jax.sharding import PartitionSpec as P

EDGE = 16
HALF = 8
CB = 16
FB = 12
PAIRS = 32
PEERS = 64
WIDE = EDGE * EDGE
CELLS = EDGE**3
PITCH = 104
BLOCKS = ("blocks_0", "blocks_1", "blocks_2")
F32 = jnp.float32
BF16 = jnp.bfloat16
TANGENT = ((1, 2), (0, 2), (0, 1))


def grid_of(rows, cols):
    return (
        lax.broadcasted_iota(jnp.int32, (rows, cols), 0),
        lax.broadcasted_iota(jnp.int32, (1, cols), 1),
    )


def face_lane(row, col, flip):
    return col * EDGE + row if flip else row * EDGE + col


def as_matrix(where, value=1.0):
    return jnp.where(where, value, 0.0).astype(BF16)


def restrict_matrix(flip):
    at, to = grid_of(WIDE, 128)
    m, n = (to >> 3) & 7, to & 7
    base = face_lane(2 * m, 2 * n, flip)
    firsts = (to < 64) & ((at == base) | (at == base + face_lane(1, 0, flip)))
    seconds = (to >= 64) & ((at == base) | (at == base + face_lane(0, 1, flip)))
    return jnp.concatenate([as_matrix(firsts, 0.5), as_matrix(seconds, 0.5)], axis=0)


def expand_matrix(flip):
    at, _ = grid_of(128, 256)
    to = lax.broadcasted_iota(jnp.int32, (128, 256), 1)
    place = face_lane((at >> 3) & 7, at & 7, flip)
    return as_matrix(((at >> 6) == (to >> 7)) & (place == (to & 127)))


def quadrant_matrix(flip):
    at, to = grid_of(WIDE, WIDE)
    row, col = (to >> 7) * HALF + ((to >> 3) & 7), ((to >> 6) & 1) * HALF + (to & 7)
    return as_matrix(at == face_lane(row, col, flip))


def flip_matrix():
    at, to = grid_of(WIDE, WIDE)
    return as_matrix(at == (to & 15) * EDGE + (to >> 4))


def prolong_matrix():
    at, to = grid_of(128, WIDE)
    return as_matrix((at & 63) == (to >> 5) * HALF + ((to & 15) >> 1))


def halves(value):
    high = value.astype(BF16)
    return high, (value - high.astype(F32)).astype(BF16)


def mm(a, b, dims=((1,), (0,))):
    return lax.dot_general(a, b, (dims, ((), ())), preferred_element_type=F32)


def mm_left(value, matrix, dims=((1,), (0,))):
    high, low = halves(value)
    return mm(high, matrix, dims) + mm(low, matrix, dims)


def mm_right(matrix, value, dims=((1,), (0,))):
    high, low = halves(value)
    return mm(matrix, high, dims) + mm(matrix, low, dims)


def lanes_of(value):
    return lax.broadcasted_iota(jnp.int32, value.shape, 1)


def y_prev(p):
    a, b = pltpu.roll(p[0], 16, 1), pltpu.roll(p[1], 16, 1)
    edge = lanes_of(a) < 16
    return jnp.where(edge, b, a), jnp.where(edge, a, b)


def y_next(p):
    a, b = pltpu.roll(p[0], 112, 1), pltpu.roll(p[1], 112, 1)
    edge = lanes_of(a) >= 112
    return jnp.where(edge, b, a), jnp.where(edge, a, b)


def z_prev(p):
    edge = (lanes_of(p[0]) & 15) == 0
    return tuple(jnp.where(edge, pltpu.roll(x, 113, 1), pltpu.roll(x, 1, 1)) for x in p)


def z_next(p):
    edge = (lanes_of(p[0]) & 15) == 15
    return tuple(jnp.where(edge, pltpu.roll(x, 15, 1), pltpu.roll(x, 127, 1)) for x in p)


def each(fn, *pairs):
    return tuple(fn(*(p[h] for p in pairs)) for h in range(2))


def span(i, half):
    start = i * WIDE + half * 128
    return pl.ds(start if isinstance(start, int) else pl.multiple_of(start, 128), 128)


def slab(ref, comp, i, first, count):
    return tuple(ref[comp, first : first + count, span(i, half)] for half in range(2))


def put_slab(ref, comp, i, first, count, value):
    for half in range(2):
        ref[comp, first : first + count, span(i, half)] = value[half]


def fine_slab(ref, comp, i):
    def one(half):
        start = comp * 32 + 2 * i + half
        return jnp.concatenate(
            [
                ref[pl.ds(start, 8, stride=PITCH), :],
                ref[pl.ds(start + 8 * PITCH, 8, stride=PITCH), :],
            ],
            axis=0,
        )

    return one(0), one(1)


def put_fine_slab(ref, comp, i, value):
    for half in range(2):
        start = comp * 32 + 2 * i + half
        ref[pl.ds(start, 8, stride=PITCH), :] = value[half][0:8]
        ref[pl.ds(start + 8 * PITCH, 8, stride=PITCH), :] = value[half][8:16]


def fetch_fine(source, target, sem):
    return [
        pltpu.make_async_copy(source.at[b], target.at[pl.ds(b * PITCH, 96)], sem)
        for b in range(FB)
    ]


def face_row_wise(load):
    out = [jnp.zeros((CB, 128), F32)] * 2
    group = lax.broadcasted_iota(jnp.int32, (CB, 128), 1) // 16
    for i in range(EDGE):
        turned = pltpu.roll(load(i), i % 8 * 16, 1)
        out[i // 8] = jnp.where(group == i % 8, turned, out[i // 8])
    return tuple(out)


def face_column_wise(load):
    out = (jnp.zeros((CB, 128), F32),) * 2
    column = lax.broadcasted_iota(jnp.int32, (CB, 128), 1) & 15
    for i in range(EDGE):
        out = each(lambda x, h: jnp.where(column == i, pltpu.roll(x, i, 1), h), load(i), out)
    return out


def routes(pairs_ref):
    slot, face, owner = pairs_ref[0], pairs_ref[1], pairs_ref[2]
    peer = lax.broadcasted_iota(jnp.int32, (PEERS, PAIRS), 0)
    named = (owner == peer).astype(F32)
    before = (
        lax.broadcasted_iota(jnp.int32, (PAIRS, PAIRS), 0)
        < lax.broadcasted_iota(jnp.int32, (PAIRS, PAIRS), 1)
    ).astype(F32)
    earlier = mm(named.astype(BF16), before.astype(BF16))
    rank = jnp.sum(named * earlier, axis=0, keepdims=True)
    first = jnp.where(rank < 0.5, named, 0.0)
    second = jnp.where(rank < 0.5, 0.0, named)
    at_row = lax.broadcasted_iota(jnp.int32, (3 * CB, PAIRS), 0)
    source = (face * CB + slot == at_row).astype(F32)
    return first, second, source


def edges(cell, emf):
    last = [slab(cell, c, EDGE - 1, 0, CB) for c in range(3)]
    now = last
    add = lambda a, b: a + b
    quarter = lambda a, b: 0.25 * (a + b)
    for i in reversed(range(EDGE)):
        prior = [slab(cell, c, i - 1, 0, CB) for c in range(3)] if i else last
        sum_x = each(add, now[0], y_prev(now[0]))
        sum_y = each(add, now[1], prior[1])
        sum_z = each(add, now[2], prior[2])
        put_slab(emf, 0, i, 0, CB, each(quarter, sum_x, z_prev(sum_x)))
        put_slab(emf, 1, i, 0, CB, each(quarter, sum_y, z_prev(sum_y)))
        put_slab(emf, 2, i, 0, CB, each(quarter, sum_z, y_prev(sum_z)))
        now = prior


def face_of(ref, along, d):
    if d == 0:
        return slab(ref, along, 0, 0, CB)
    if d == 1:
        return face_row_wise(lambda i: slab(ref, along, i, 0, CB)[0])
    return face_column_wise(lambda i: slab(ref, along, i, 0, CB))


def coarse_parts(cb, cv, b_c, v_c, sems):
    return [
        [
            pltpu.make_async_copy(far.at[:, :, part], near.at[:, :, part], sems.at[q])
            for far, near in ((cb, b_c), (cv, v_c))
        ]
        for q, part in enumerate(pl.ds(q * 4 * WIDE, 4 * WIDE) for q in range(4))
    ]


def wait_part(copies, i):
    for q in range(4):
        if i == max(4 * q - 1, 0):
            for copy in copies[q]:
                copy.wait()


def centres(load_b, i):
    bx, by, bz = (load_b(c, i) for c in range(3))
    mean = lambda a, b: 0.5 * (a + b)
    return (
        each(mean, bx, load_b(0, (i + 1) % EDGE)),
        each(mean, by, y_next(by)),
        each(mean, bz, z_next(bz)),
    )


def speeds(centre, velocity):
    size = lambda a, b, c: jnp.sqrt(a * a + b * b + c * c)
    fast = each(lambda a, b: a + b, each(size, *velocity), each(size, *centre))
    return jnp.maximum(fast[0], fast[1])


def put_cell(cell, i, centre, velocity):
    cross = lambda a, b, c, d: a * b - c * d
    (cx, cy, cz), (vx, vy, vz) = centre, velocity
    put_slab(cell, 0, i, 0, CB, each(cross, vz, cy, vy, cz))
    put_slab(cell, 1, i, 0, CB, each(cross, vx, cz, vz, cx))
    put_slab(cell, 2, i, 0, CB, each(cross, vy, cx, vx, cy))


def first_kernel(
    cb, cv, fb, fv, far_pairs,
    send, emf_f, b_f,
    b_c, v_c, pitched_b, v_f, pairs, out, sems,
):
    fine_copies = fetch_fine(fb, pitched_b, sems.at[0]) + fetch_fine(fv, v_f, sems.at[1])
    coarse_copies = coarse_parts(cb, cv, b_c, v_c, sems.at[pl.ds(2, 4)])
    pairs_copy = pltpu.make_async_copy(far_pairs, pairs, sems.at[6])
    for copy in [pairs_copy, *fine_copies, *sum(coarse_copies, [])]:
        copy.start()
    idle = pl.ds(FB * PITCH, (CB - FB) * PITCH)
    pitched_b[idle, :] = jnp.zeros(((CB - FB) * PITCH, 128), F32)
    v_f[idle, :] = jnp.zeros(((CB - FB) * PITCH, 128), F32)
    pairs_copy.wait()
    first, second, source = routes(pairs)
    nt = ((1,), (1,))
    key = (pairs[1] * 64 + (pairs[4] * 2 + pairs[5]) * CB + pairs[3] + 1).astype(F32)
    lane = lax.broadcasted_iota(jnp.int32, (PEERS, 128), 1)
    meta = jnp.zeros((PEERS, 128), F32)
    picks = []
    for k, chosen in enumerate((first, second)):
        picks.append(mm(chosen.astype(BF16), source.astype(BF16), nt).astype(BF16))
        meta = jnp.where(lane == k, jnp.sum(chosen * key, axis=1, keepdims=True), meta)

    for copy in fine_copies:
        copy.wait()
    held = {}

    def fine_b(c, i):
        if (c, i) not in held:
            held[c, i] = fine_slab(pitched_b, c, i)
            put_slab(b_f, c, i, 0, CB, held[c, i])
        return held[c, i]

    top_fine = top_coarse = jnp.zeros((CB, 128), F32)
    for i in range(EDGE):
        centre, velocity = centres(fine_b, i), [fine_slab(v_f, c, i) for c in range(3)]
        put_cell(emf_f, i, centre, velocity)
        top_fine = jnp.maximum(top_fine, speeds(centre, velocity))
    edges(emf_f, emf_f)
    restrict = [restrict_matrix(False), restrict_matrix(True)]
    rows = []
    for d in range(3):
        planes = [face_of(emf_f, along, d) for along in TANGENT[d]]
        both = jnp.concatenate([*planes[0], *planes[1]], axis=1)
        rows.append(mm_left(both, restrict[1 if d == 2 else 0]))
    rows = jnp.concatenate(rows, axis=0)
    for k in range(2):
        out[:, 0, k * 128 : (k + 1) * 128] = mm_right(picks[k], rows)
    rows_copy = pltpu.make_async_copy(
        out.at[:, :, pl.ds(0, 256)], send.at[:, :, pl.ds(0, 256)], sems.at[7]
    )
    rows_copy.start()

    for i in range(EDGE):
        wait_part(coarse_copies, i)
        centre = centres(lambda c, k: slab(b_c, c, k, 0, CB), i)
        top_coarse = jnp.maximum(top_coarse, speeds(centre, [slab(v_c, c, i, 0, CB) for c in range(3)]))
    top = jnp.max(jnp.maximum(top_fine, top_coarse), axis=0, keepdims=True)
    top = jnp.broadcast_to(jnp.max(top, axis=1, keepdims=True), (PEERS, 128))
    out[:, 0, 256:384] = jnp.where(lane < 2, meta, top)
    meta_copy = pltpu.make_async_copy(
        out.at[:, :, pl.ds(256, 128)], send.at[:, :, pl.ds(256, 128)], sems.at[8]
    )
    meta_copy.start()
    rows_copy.wait()
    meta_copy.wait()


def coarse_kernel(cb, cv, emf, planes, quads, b_c, v_c, sems):
    copies = coarse_parts(cb, cv, b_c, v_c, sems)
    for copy in sum(copies, []):
        copy.start()
    load_b, load_v = (lambda c, i, ref=ref: slab(ref, c, i, 0, CB) for ref in (b_c, v_c))
    for i in range(EDGE):
        wait_part(copies, i)
        centre = centres(load_b, i)
        put_cell(emf, i, centre, [load_v(c, i) for c in range(3)])
    edges(emf, emf)
    for d in range(3):
        for t in range(2):
            at = (d * 2 + t) * CB
            face = face_of(emf, TANGENT[d][t], d)
            planes[at : at + CB, 0:128] = face[0]
            planes[at : at + CB, 128:256] = face[1]
    quadrant = [quadrant_matrix(False), quadrant_matrix(True)]
    for d in range(3):
        normal = jnp.concatenate(face_of(b_c, d, d), axis=1)
        quads[d * CB : (d + 1) * CB, :] = mm_left(normal, quadrant[1 if d == 2 else 0])


def answer_kernel(
    got, planes, quads_b, back, far_patch, masks, top, patch, out, sems
):
    expand = [expand_matrix(False), expand_matrix(True)]
    quadrant = [quadrant_matrix(False), quadrant_matrix(True)]
    meta = got[:, 0, 256:384]
    top[...] = jnp.max(meta, axis=0, keepdims=True)
    keys = [meta[:, k : k + 1].astype(jnp.int32) - 1 for k in range(2)]
    target = lax.broadcasted_iota(jnp.int32, (PEERS, 256), 1)
    hit = jnp.concatenate([(k == target).astype(F32) for k in keys], axis=0).astype(BF16)
    rows = jnp.concatenate([got[:, 0, 0:128], got[:, 0, 128:256]], axis=0)
    tn = ((0,), (0,))
    replaced = mm_right(hit, rows, tn)[0:192]
    counted = mm(hit, jnp.ones((2 * PEERS, 128), BF16), tn)[0:192]
    spread = (mm_left(replaced, expand[0]), mm_left(replaced, expand[1]))
    lane = lax.broadcasted_iota(jnp.int32, (CB, 128), 1)

    def at(d, quad):
        return slice(d * 64 + quad * CB, d * 64 + (quad + 1) * CB)

    def value(d, t, flip):
        part = slice(t * 128, (t + 1) * 128)
        out = []
        for h in range(2):
            near, far = (h, h + 2) if flip else (2 * h, 2 * h + 1)
            x = spread[flip]
            out.append(x[at(d, near), part] + pltpu.roll(x[at(d, far), part], 8, 1))
        return tuple(out)

    def mask(d, flip):
        out = []
        for h in range(2):
            near, far = (h, h + 2) if flip else (2 * h, 2 * h + 1)
            out.append(jnp.where((lane & 15) < 8, counted[at(d, near)], counted[at(d, far)]) > 0.5)
        return tuple(out)

    value = {
        (d, t): value(d, t, int(d == 2)) for d in range(3) for t in range(2)
    } | {"1x": value(1, 0, 1), "2x": value(2, 0, 0)}
    hits = {d: mask(d, int(d == 2)) for d in range(3)} | {"1x": mask(1, 1), "2x": mask(2, 0)}
    for h in range(2):
        side = slice(h * 128, (h + 1) * 128)
        masks[:, side] = sum(hits[d][h].astype(F32) * 2.0**d for d in range(3))
        for d in range(3):
            for t in range(2):
                first = (d * 2 + t) * CB
                patch[first : first + CB, side] = value[d, t][h]

    store = pltpu.make_async_copy(patch, far_patch, sems.at[0])
    store.start()

    def face(d, t):
        first = (d * 2 + t) * CB
        return planes[first : first + CB, 0:128], planes[first : first + CB, 128:256]

    both = lambda a, b: a & b
    column = ((lane & 15) == 0,) * 2
    row = (lane < 16, lane < 0)
    put = lambda m, new, old: each(jnp.where, m, new, old)
    ey_0 = put(hits[0], value[0, 0], face(0, 0))
    ez_0 = put(hits[0], value[0, 1], face(0, 1))
    ez_1 = put(each(both, row, hits[0]), value[0, 1], face(1, 1))
    ey_2 = put(each(both, column, hits[0]), value[0, 0], face(2, 1))
    ex_1 = put(hits[1], value[1, 0], face(1, 0))
    ez_1 = put(hits[1], value[1, 1], ez_1)
    ez_0 = put(each(both, row, hits[1]), value[1, 1], ez_0)
    ex_2 = put(each(both, row, hits["1x"]), value["1x"], face(2, 0))
    ex_2 = put(hits[2], value[2, 0], ex_2)
    ey_2 = put(hits[2], value[2, 1], ey_2)
    ex_1 = put(each(both, column, hits["2x"]), value["2x"], ex_1)
    ey_0 = put(each(both, column, hits[2]), value[2, 1], ey_0)
    curl = lambda p, q, r, s: (p - q) - (r - s)
    curls = (
        each(curl, y_next(ez_0), ez_0, z_next(ey_0), ey_0),
        each(curl, z_next(ex_1), ex_1, y_next(ez_1), ez_1),
        each(curl, z_next(ey_2), ey_2, y_next(ex_2), ex_2),
    )
    straight = jnp.concatenate(
        [jnp.concatenate(curls[0], axis=1), jnp.concatenate(curls[1], axis=1)], axis=0
    )
    quads_c = jnp.concatenate(
        [
            mm_left(straight, quadrant[0]),
            mm_left(jnp.concatenate(curls[2], axis=1), quadrant[1]),
        ],
        axis=0,
    )
    wide_lane = lax.broadcasted_iota(jnp.int32, (PEERS, 3 * CB), 1)
    out_lane = lax.broadcasted_iota(jnp.int32, (PEERS, 128), 1)
    for part, quads in enumerate((quads_b[...], quads_c)):
        answers = []
        for k in range(2):
            key = keys[k]
            place = jnp.where(key >= 0, (key >> 6) * CB + (key & 15), -1)
            pick = (place == wide_lane).astype(F32).astype(BF16)
            found = mm_right(pick, quads)
            quad = (key >> 4) & 3
            side = jnp.where(quad >= 2, found[:, 128:256], found[:, 0:128])
            answers.append(jnp.where((quad & 1) == k, side, pltpu.roll(side, 64, 1)))
        side = slice(part * 128, (part + 1) * 128)
        out[:, 0, side] = jnp.where(out_lane < 64, answers[0], answers[1])
    send = pltpu.make_async_copy(out, back, sems.at[1])
    send.start()
    for copy in (store, send):
        copy.wait()


def update_kernel(
    top, emf_c, far_patch, masks, emf_f, b_c, b_f, far_pairs,
    new_c, new_f, picked, chosen,
    emf, out_c, out_f, pairs, patch, sems,
):
    load = pltpu.make_async_copy(far_pairs, pairs, sems.at[2])
    load_patch = pltpu.make_async_copy(far_patch, patch, sems.at[3])
    load_patch.start()
    load.start()
    time_step = 0.2 / top[0:1, 2:3]
    lane = lax.broadcasted_iota(jnp.int32, (CB, 128), 1)

    def pair(ref, first):
        return ref[first : first + CB, 0:128], ref[first : first + CB, 128:256]

    def update(emf, factor, load_b, store, done):
        for i in range(EDGE):
            following = (i + 1) % EDGE
            ex, ey, ez = (slab(emf, c, i, 0, CB) for c in range(3))
            ey_far, ez_far = (slab(emf, c, following, 0, CB) for c in (1, 2))
            curl = lambda b, p, q, r, s: b - factor * ((p - q) - (r - s))
            store(0, i, each(curl, load_b(0, i), y_next(ez), ez, z_next(ey), ey))
            store(1, i, each(curl, load_b(1, i), z_next(ex), ex, ez_far, ez))
            store(2, i, each(curl, load_b(2, i), ey_far, ey, y_next(ex), ex))
            done(i)

    update(
        emf_f,
        time_step / 0.5,
        lambda c, i: slab(b_f, c, i, 0, CB),
        lambda c, i, value: put_fine_slab(out_f, c, i, value),
        lambda i: None,
    )
    results = [
        pltpu.make_async_copy(out_f.at[pl.ds(b * PITCH, 96)], new_f.at[b], sems.at[0])
        for b in range(FB)
    ]
    for copy in results:
        copy.start()

    load_patch.wait()
    planes = {(d, t): pair(patch, (d * 2 + t) * CB) for d in range(3) for t in range(2)}
    bits = [m.astype(jnp.int32) for m in pair(masks, 0)]
    hits = [[((m >> d) & 1).astype(F32) for m in bits] for d in range(3)]
    for i in range(EDGE):
        now = {c: slab(emf_c, c, i, 0, CB) for c in range(3)}
        if i == 0:
            for t, c in enumerate(TANGENT[0]):
                now[c] = each(lambda m, p, e: jnp.where(m > 0.5, p, e), hits[0], planes[0, t], now[c])
        turn, h = (8 - i % 8) % 8 * 16, i // 8
        there = (lane < 16) & (pltpu.roll(hits[1][h], turn, 1) > 0.5)
        for t, c in enumerate(TANGENT[1]):
            now[c] = (jnp.where(there, pltpu.roll(planes[1, t][h], turn, 1), now[c][0]), now[c][1])
        turn = (128 - i) % 128
        there = [((lane & 15) == 0) & (pltpu.roll(m, turn, 1) > 0.5) for m in hits[2]]
        for t, c in enumerate(TANGENT[2]):
            value = [pltpu.roll(p, turn, 1) for p in planes[2, t]]
            now[c] = each(jnp.where, there, value, now[c])
        for c in range(3):
            put_slab(emf, c, i, 0, CB, now[c])

    def send_chunk(i):
        if i % 4 == 3:
            part = pl.ds((i - 3) * WIDE, 4 * WIDE)
            copy = pltpu.make_async_copy(out_c.at[:, :, part], new_c.at[:, :, part], sems.at[1])
            copy.start()
            results.append(copy)

    update(
        emf,
        time_step,
        lambda c, i: slab(b_c, c, i, 0, CB),
        lambda c, i, value: put_slab(out_c, c, i, 0, CB, value),
        send_chunk,
    )
    faces = (
        fine_slab(out_f, 0, 0),
        face_row_wise(lambda i: fine_slab(out_f, 1, i)[0]),
        face_column_wise(lambda i: fine_slab(out_f, 2, i)),
    )
    load.wait()
    first, second, source = routes(pairs)
    tn = ((0,), (0,))
    same = (
        lax.broadcasted_iota(jnp.int32, (PEERS, PEERS), 0)
        == lax.broadcasted_iota(jnp.int32, (PEERS, PEERS), 1)
    ).astype(F32).astype(BF16)
    chosen[...] = jnp.concatenate(
        [mm(first.astype(BF16), same, tn), mm(second.astype(BF16), same, tn)], axis=1
    )
    source = source.astype(BF16)
    flip = flip_matrix()
    normals = [jnp.concatenate(face, axis=1) for face in faces]
    straight = mm_right(source[0 : 2 * CB], jnp.concatenate(normals[0:2], axis=0), tn)
    flipped = mm_left(mm_right(source[2 * CB :], normals[2], tn), flip)
    picked[...] = straight + flipped
    for copy in results:
        copy.wait()


def third_kernel(got, top, picked, chosen, jump, held, sems):
    rows = got[:, 0, 0:128] - (0.2 / top[0:1, 2:3]) * got[:, 0, 128:256]
    lane = lax.broadcasted_iota(jnp.int32, (PAIRS, 128), 1)
    picks = chosen[...].astype(BF16)
    sides = [mm_right(picks[:, k * PEERS : (k + 1) * PEERS], rows) for k in range(2)]
    own = jnp.where(lane < 64, sides[0], sides[1])
    held[...] = picked[...] - mm_left(own, prolong_matrix())
    copy = pltpu.make_async_copy(held, jump, sems.at[0])
    copy.start()
    copy.wait()


VMEM = pl.BlockSpec(memory_space=pltpu.VMEM)
HBM = pl.BlockSpec(memory_space=pltpu.HBM)
FIELD = (3, CB, CELLS)
PITCHED = (CB * PITCH, 128)
FACES = (6 * CB, WIDE)


def call(kernel, outs, args, scratch=(), aliases=None):
    far = [isinstance(out, tuple) and out[0] == "hbm" for out in outs]
    return pl.pallas_call(
        kernel,
        out_shape=[
            pltpu.HBM(out[1], F32) if is_far else pltpu.VMEM(out, F32)
            for out, is_far in zip(outs, far)
        ],
        in_specs=[HBM if is_far else VMEM for _, is_far in args],
        out_specs=[HBM if is_far else VMEM for is_far in far],
        scratch_shapes=list(scratch),
        input_output_aliases=aliases or {},
        compiler_params=pltpu.CompilerParams(vmem_limit_bytes=24 * 1024 * 1024),
    )(
        *(
            pltpu.with_memory_space_constraint(a, pltpu.HBM if is_far else pltpu.VMEM)
            for a, is_far in args
        )
    )


def on_device(coarse_field, coarse_velocity, fine_field, fine_velocity, pairs):
    cb = coarse_field[0].transpose(1, 0, 2)
    cv = coarse_velocity[0].transpose(1, 0, 2)
    fb = fine_field[0].reshape(FB, 96, 128)
    fv = fine_velocity[0].reshape(FB, 96, 128)
    rows = pairs.transpose(2, 0, 1)
    near = lambda *arrays: [(a, False) for a in arrays]
    far = lambda *arrays: [(a, True) for a in arrays]
    count = lax.axis_size("gz")

    field = pltpu.VMEM(FIELD, F32)
    pitched = pltpu.VMEM(PITCHED, F32)
    small = pltpu.VMEM((6, 1, PAIRS), jnp.int32)
    sems = pltpu.SemaphoreType.DMA
    send, emf_f, b_f = call(
        first_kernel,
        [("hbm", (PEERS, 1, 384)), FIELD, FIELD],
        far(cb, cv, fb, fv, rows),
        [field, field, pitched, pitched, small, pltpu.VMEM((PEERS, 1, 384), F32), sems((9,))],
    )
    got = lax.all_to_all(send, BLOCKS, 0, 0, tiled=True)
    emf_c, planes, quads, b_c = call(
        coarse_kernel, [FIELD, FACES, (3 * CB, WIDE), FIELD], far(cb, cv), [field, sems((4,))]
    )
    got, emf_c, planes, quads, b_c = lax.optimization_barrier((got, emf_c, planes, quads, b_c))
    back, patch, masks, top = call(
        answer_kernel,
        [("hbm", (PEERS, 1, 256)), ("hbm", FACES), (CB, WIDE), (1, 128)],
        near(got, planes, quads),
        [pltpu.VMEM(FACES, F32), pltpu.VMEM((PEERS, 1, 256), F32), sems((2,))],
    )
    others = []
    for k in range(1, count):
        others.append(lax.ppermute(top, "gz", [(i, (i + k) % count) for i in range(count)]))
    for other in others:
        top = jnp.maximum(top, other)
    returned = lax.all_to_all(back, BLOCKS, 0, 0, tiled=True)
    new_c, new_f, picked, chosen = call(
        update_kernel,
        [("hbm", FIELD), ("hbm", (FB, 96, 128)), (PAIRS, WIDE), (PAIRS, 128)],
        near(top, emf_c) + far(patch) + near(masks, emf_f, b_c, b_f) + far(rows),
        [field, field, pitched, small, pltpu.VMEM(FACES, F32), sems((4,))],
    )
    (jump,) = call(
        third_kernel,
        [("hbm", (PAIRS, WIDE))],
        near(returned, top, picked, chosen),
        [pltpu.VMEM((PAIRS, WIDE), F32), sems((1,))],
    )
    return (
        new_c.transpose(1, 0, 2)[None],
        new_f.reshape(1, FB, 3, CELLS),
        jump[None],
    )


def solution(mesh):
    split = Mesh(
        mesh.devices.reshape(4, 8, 2, mesh.shape["gz"]), ("blocks_0", "blocks_1", "blocks_2", "gz")
    )
    in_specs = (
        P("gz", BLOCKS, None, None),
        P("gz", BLOCKS, None, None),
        P("gz", BLOCKS, None, None),
        P("gz", BLOCKS, None, None),
        P("gz", BLOCKS, None),
    )
    out_specs = (P("gz", BLOCKS, None, None), P("gz", BLOCKS, None, None), P("gz", BLOCKS, None))

    return jax.shard_map(on_device, mesh=split, in_specs=in_specs, out_specs=out_specs, check_vma=False)
```

```python
import jax
import jax.numpy as jnp
from jax import lax
from jax.experimental import pallas as pl
from jax.experimental.pallas import tpu as pltpu
from jax.sharding import Mesh
from jax.sharding import PartitionSpec as P

EDGE = 16
HALF = 8
CB = 16
FB = 12
PAIRS = 32
PEERS = 64
WIDE = EDGE * EDGE
CELLS = EDGE**3
PITCH = 104
BLOCKS = ("blocks_0", "blocks_1", "blocks_2")
F32 = jnp.float32
BF16 = jnp.bfloat16
TANGENT = ((1, 2), (0, 2), (0, 1))


def grid_of(rows, cols):
    return (
        lax.broadcasted_iota(jnp.int32, (rows, cols), 0),
        lax.broadcasted_iota(jnp.int32, (1, cols), 1),
    )


def face_lane(row, col, flip):
    return col * EDGE + row if flip else row * EDGE + col


def as_matrix(where, value=1.0):
    return jnp.where(where, value, 0.0).astype(BF16)


def restrict_matrix(flip):
    at, to = grid_of(WIDE, 128)
    m, n = (to >> 3) & 7, to & 7
    base = face_lane(2 * m, 2 * n, flip)
    firsts = (to < 64) & ((at == base) | (at == base + face_lane(1, 0, flip)))
    seconds = (to >= 64) & ((at == base) | (at == base + face_lane(0, 1, flip)))
    return jnp.concatenate([as_matrix(firsts, 0.5), as_matrix(seconds, 0.5)], axis=0)


def expand_matrix(flip):
    at, _ = grid_of(128, 256)
    to = lax.broadcasted_iota(jnp.int32, (128, 256), 1)
    place = face_lane((at >> 3) & 7, at & 7, flip)
    return as_matrix(((at >> 6) == (to >> 7)) & (place == (to & 127)))


def quadrant_matrix(flip):
    at, to = grid_of(WIDE, WIDE)
    row, col = (to >> 7) * HALF + ((to >> 3) & 7), ((to >> 6) & 1) * HALF + (to & 7)
    return as_matrix(at == face_lane(row, col, flip))


def flip_matrix():
    at, to = grid_of(WIDE, WIDE)
    return as_matrix(at == (to & 15) * EDGE + (to >> 4))


def prolong_matrix():
    at, to = grid_of(128, WIDE)
    return as_matrix((at & 63) == (to >> 5) * HALF + ((to & 15) >> 1))


def halves(value):
    high = value.astype(BF16)
    return high, (value - high.astype(F32)).astype(BF16)


def mm(a, b, dims=((1,), (0,))):
    return lax.dot_general(a, b, (dims, ((), ())), preferred_element_type=F32)


def mm_left(value, matrix, dims=((1,), (0,))):
    high, low = halves(value)
    return mm(high, matrix, dims) + mm(low, matrix, dims)


def mm_right(matrix, value, dims=((1,), (0,))):
    high, low = halves(value)
    return mm(matrix, high, dims) + mm(matrix, low, dims)


def lanes_of(value):
    return lax.broadcasted_iota(jnp.int32, value.shape, 1)


def y_prev(p):
    a, b = pltpu.roll(p[0], 16, 1), pltpu.roll(p[1], 16, 1)
    edge = lanes_of(a) < 16
    return jnp.where(edge, b, a), jnp.where(edge, a, b)


def y_next(p):
    a, b = pltpu.roll(p[0], 112, 1), pltpu.roll(p[1], 112, 1)
    edge = lanes_of(a) >= 112
    return jnp.where(edge, b, a), jnp.where(edge, a, b)


def z_prev(p):
    edge = (lanes_of(p[0]) & 15) == 0
    return tuple(jnp.where(edge, pltpu.roll(x, 113, 1), pltpu.roll(x, 1, 1)) for x in p)


def z_next(p):
    edge = (lanes_of(p[0]) & 15) == 15
    return tuple(jnp.where(edge, pltpu.roll(x, 15, 1), pltpu.roll(x, 127, 1)) for x in p)


def each(fn, *pairs):
    return tuple(fn(*(p[h] for p in pairs)) for h in range(2))


def span(i, half):
    start = i * WIDE + half * 128
    return pl.ds(start if isinstance(start, int) else pl.multiple_of(start, 128), 128)


def slab(ref, comp, i, first, count):
    return tuple(ref[comp, first : first + count, span(i, half)] for half in range(2))


def put_slab(ref, comp, i, first, count, value):
    for half in range(2):
        ref[comp, first : first + count, span(i, half)] = value[half]


def fine_slab(ref, comp, i):
    def one(half):
        start = comp * 32 + 2 * i + half
        return jnp.concatenate(
            [
                ref[pl.ds(start, 8, stride=PITCH), :],
                ref[pl.ds(start + 8 * PITCH, 8, stride=PITCH), :],
            ],
            axis=0,
        )

    return one(0), one(1)


def put_fine_slab(ref, comp, i, value):
    for half in range(2):
        start = comp * 32 + 2 * i + half
        ref[pl.ds(start, 8, stride=PITCH), :] = value[half][0:8]
        ref[pl.ds(start + 8 * PITCH, 8, stride=PITCH), :] = value[half][8:16]


def fetch_fine(source, target, sem):
    return [
        pltpu.make_async_copy(source.at[b], target.at[pl.ds(b * PITCH, 96)], sem)
        for b in range(FB)
    ]


def face_row_wise(load):
    out = [jnp.zeros((CB, 128), F32)] * 2
    group = lax.broadcasted_iota(jnp.int32, (CB, 128), 1) // 16
    for i in range(EDGE):
        turned = pltpu.roll(load(i), i % 8 * 16, 1)
        out[i // 8] = jnp.where(group == i % 8, turned, out[i // 8])
    return tuple(out)


def face_column_wise(load):
    out = (jnp.zeros((CB, 128), F32),) * 2
    column = lax.broadcasted_iota(jnp.int32, (CB, 128), 1) & 15
    for i in range(EDGE):
        out = each(lambda x, h: jnp.where(column == i, pltpu.roll(x, i, 1), h), load(i), out)
    return out


def routes(pairs_ref):
    slot, face, owner = pairs_ref[0], pairs_ref[1], pairs_ref[2]
    peer = lax.broadcasted_iota(jnp.int32, (PEERS, PAIRS), 0)
    named = (owner == peer).astype(F32)
    before = (
        lax.broadcasted_iota(jnp.int32, (PAIRS, PAIRS), 0)
        < lax.broadcasted_iota(jnp.int32, (PAIRS, PAIRS), 1)
    ).astype(F32)
    earlier = mm(named.astype(BF16), before.astype(BF16))
    rank = jnp.sum(named * earlier, axis=0, keepdims=True)
    first = jnp.where(rank < 0.5, named, 0.0)
    second = jnp.where(rank < 0.5, 0.0, named)
    at_row = lax.broadcasted_iota(jnp.int32, (3 * CB, PAIRS), 0)
    source = (face * CB + slot == at_row).astype(F32)
    return first, second, source


def edges(cell, emf):
    last = [slab(cell, c, EDGE - 1, 0, CB) for c in range(3)]
    now = last
    add = lambda a, b: a + b
    quarter = lambda a, b: 0.25 * (a + b)
    for i in reversed(range(EDGE)):
        prior = [slab(cell, c, i - 1, 0, CB) for c in range(3)] if i else last
        sum_x = each(add, now[0], y_prev(now[0]))
        sum_y = each(add, now[1], prior[1])
        sum_z = each(add, now[2], prior[2])
        put_slab(emf, 0, i, 0, CB, each(quarter, sum_x, z_prev(sum_x)))
        put_slab(emf, 1, i, 0, CB, each(quarter, sum_y, z_prev(sum_y)))
        put_slab(emf, 2, i, 0, CB, each(quarter, sum_z, y_prev(sum_z)))
        now = prior


def face_of(ref, along, d):
    if d == 0:
        return slab(ref, along, 0, 0, CB)
    if d == 1:
        return face_row_wise(lambda i: slab(ref, along, i, 0, CB)[0])
    return face_column_wise(lambda i: slab(ref, along, i, 0, CB))


def coarse_parts(cb, cv, b_c, v_c, sems):
    return [
        [
            pltpu.make_async_copy(far.at[:, :, part], near.at[:, :, part], sems.at[q])
            for far, near in ((cb, b_c), (cv, v_c))
        ]
        for q, part in enumerate(pl.ds(q * 4 * WIDE, 4 * WIDE) for q in range(4))
    ]


def wait_part(copies, i):
    for q in range(4):
        if i == max(4 * q - 1, 0):
            for copy in copies[q]:
                copy.wait()


def centres(load_b, i):
    bx, by, bz = (load_b(c, i) for c in range(3))
    mean = lambda a, b: 0.5 * (a + b)
    return (
        each(mean, bx, load_b(0, (i + 1) % EDGE)),
        each(mean, by, y_next(by)),
        each(mean, bz, z_next(bz)),
    )


def speeds(centre, velocity):
    size = lambda a, b, c: jnp.sqrt(a * a + b * b + c * c)
    fast = each(lambda a, b: a + b, each(size, *velocity), each(size, *centre))
    return jnp.maximum(fast[0], fast[1])


def put_cell(cell, i, centre, velocity):
    cross = lambda a, b, c, d: a * b - c * d
    (cx, cy, cz), (vx, vy, vz) = centre, velocity
    put_slab(cell, 0, i, 0, CB, each(cross, vz, cy, vy, cz))
    put_slab(cell, 1, i, 0, CB, each(cross, vx, cz, vz, cx))
    put_slab(cell, 2, i, 0, CB, each(cross, vy, cx, vx, cy))


def first_kernel(
    cb, cv, fb, fv, far_pairs,
    send, emf_f, b_f,
    b_c, v_c, pitched_b, v_f, pairs, out, sems,
):
    fine_copies = fetch_fine(fb, pitched_b, sems.at[0]) + fetch_fine(fv, v_f, sems.at[1])
    coarse_copies = coarse_parts(cb, cv, b_c, v_c, sems.at[pl.ds(2, 4)])
    pairs_copy = pltpu.make_async_copy(far_pairs, pairs, sems.at[6])
    for copy in [pairs_copy, *fine_copies, *sum(coarse_copies, [])]:
        copy.start()
    idle = pl.ds(FB * PITCH, (CB - FB) * PITCH)
    pitched_b[idle, :] = jnp.zeros(((CB - FB) * PITCH, 128), F32)
    v_f[idle, :] = jnp.zeros(((CB - FB) * PITCH, 128), F32)
    pairs_copy.wait()
    first, second, source = routes(pairs)
    nt = ((1,), (1,))
    key = (pairs[1] * 64 + (pairs[4] * 2 + pairs[5]) * CB + pairs[3] + 1).astype(F32)
    lane = lax.broadcasted_iota(jnp.int32, (PEERS, 128), 1)
    meta = jnp.zeros((PEERS, 128), F32)
    picks = []
    for k, chosen in enumerate((first, second)):
        picks.append(mm(chosen.astype(BF16), source.astype(BF16), nt).astype(BF16))
        meta = jnp.where(lane == k, jnp.sum(chosen * key, axis=1, keepdims=True), meta)

    for copy in fine_copies:
        copy.wait()
    held = {}

    def fine_b(c, i):
        if (c, i) not in held:
            held[c, i] = fine_slab(pitched_b, c, i)
            put_slab(b_f, c, i, 0, CB, held[c, i])
        return held[c, i]

    top_fine = top_coarse = jnp.zeros((CB, 128), F32)
    for i in range(EDGE):
        centre, velocity = centres(fine_b, i), [fine_slab(v_f, c, i) for c in range(3)]
        put_cell(emf_f, i, centre, velocity)
        top_fine = jnp.maximum(top_fine, speeds(centre, velocity))
    edges(emf_f, emf_f)
    restrict = [restrict_matrix(False), restrict_matrix(True)]
    rows = []
    for d in range(3):
        planes = [face_of(emf_f, along, d) for along in TANGENT[d]]
        both = jnp.concatenate([*planes[0], *planes[1]], axis=1)
        rows.append(mm_left(both, restrict[1 if d == 2 else 0]))
    rows = jnp.concatenate(rows, axis=0)
    for k in range(2):
        out[:, 0, k * 128 : (k + 1) * 128] = mm_right(picks[k], rows)
    rows_copy = pltpu.make_async_copy(
        out.at[:, :, pl.ds(0, 256)], send.at[:, :, pl.ds(0, 256)], sems.at[7]
    )
    rows_copy.start()

    for i in range(EDGE):
        wait_part(coarse_copies, i)
        centre = centres(lambda c, k: slab(b_c, c, k, 0, CB), i)
        top_coarse = jnp.maximum(top_coarse, speeds(centre, [slab(v_c, c, i, 0, CB) for c in range(3)]))
    top = jnp.max(jnp.maximum(top_fine, top_coarse), axis=0, keepdims=True)
    top = jnp.broadcast_to(jnp.max(top, axis=1, keepdims=True), (PEERS, 128))
    out[:, 0, 256:384] = jnp.where(lane < 2, meta, top)
    meta_copy = pltpu.make_async_copy(
        out.at[:, :, pl.ds(256, 128)], send.at[:, :, pl.ds(256, 128)], sems.at[8]
    )
    meta_copy.start()
    rows_copy.wait()
    meta_copy.wait()


def coarse_kernel(cb, cv, emf, planes, quads, b_c, v_c, sems):
    copies = coarse_parts(cb, cv, b_c, v_c, sems)
    for copy in sum(copies, []):
        copy.start()
    load_b, load_v = (lambda c, i, ref=ref: slab(ref, c, i, 0, CB) for ref in (b_c, v_c))
    for i in range(EDGE):
        wait_part(copies, i)
        centre = centres(load_b, i)
        put_cell(emf, i, centre, [load_v(c, i) for c in range(3)])
    edges(emf, emf)
    for d in range(3):
        for t in range(2):
            at = (d * 2 + t) * CB
            face = face_of(emf, TANGENT[d][t], d)
            planes[at : at + CB, 0:128] = face[0]
            planes[at : at + CB, 128:256] = face[1]
    quadrant = [quadrant_matrix(False), quadrant_matrix(True)]
    for d in range(3):
        normal = jnp.concatenate(face_of(b_c, d, d), axis=1)
        quads[d * CB : (d + 1) * CB, :] = mm_left(normal, quadrant[1 if d == 2 else 0])


def answer_kernel(
    got, planes, quads_b, back, far_patch, masks, top, patch, out, sems
):
    expand = [expand_matrix(False), expand_matrix(True)]
    quadrant = [quadrant_matrix(False), quadrant_matrix(True)]
    meta = got[:, 0, 256:384]
    top[...] = jnp.max(meta, axis=0, keepdims=True)
    keys = [meta[:, k : k + 1].astype(jnp.int32) - 1 for k in range(2)]
    target = lax.broadcasted_iota(jnp.int32, (PEERS, 256), 1)
    hit = jnp.concatenate([(k == target).astype(F32) for k in keys], axis=0).astype(BF16)
    rows = jnp.concatenate([got[:, 0, 0:128], got[:, 0, 128:256]], axis=0)
    tn = ((0,), (0,))
    replaced = mm_right(hit, rows, tn)[0:192]
    counted = mm(hit, jnp.ones((2 * PEERS, 128), BF16), tn)[0:192]
    spread = (mm_left(replaced, expand[0]), mm_left(replaced, expand[1]))
    lane = lax.broadcasted_iota(jnp.int32, (CB, 128), 1)

    def at(d, quad):
        return slice(d * 64 + quad * CB, d * 64 + (quad + 1) * CB)

    def value(d, t, flip):
        part = slice(t * 128, (t + 1) * 128)
        out = []
        for h in range(2):
            near, far = (h, h + 2) if flip else (2 * h, 2 * h + 1)
            x = spread[flip]
            out.append(x[at(d, near), part] + pltpu.roll(x[at(d, far), part], 8, 1))
        return tuple(out)

    def mask(d, flip):
        out = []
        for h in range(2):
            near, far = (h, h + 2) if flip else (2 * h, 2 * h + 1)
            out.append(jnp.where((lane & 15) < 8, counted[at(d, near)], counted[at(d, far)]) > 0.5)
        return tuple(out)

    value = {
        (d, t): value(d, t, int(d == 2)) for d in range(3) for t in range(2)
    } | {"1x": value(1, 0, 1), "2x": value(2, 0, 0)}
    hits = {d: mask(d, int(d == 2)) for d in range(3)} | {"1x": mask(1, 1), "2x": mask(2, 0)}
    for h in range(2):
        side = slice(h * 128, (h + 1) * 128)
        masks[:, side] = sum(hits[d][h].astype(F32) * 2.0**d for d in range(3))
        for d in range(3):
            for t in range(2):
                first = (d * 2 + t) * CB
                patch[first : first + CB, side] = value[d, t][h]

    store = pltpu.make_async_copy(patch, far_patch, sems.at[0])
    store.start()

    def face(d, t):
        first = (d * 2 + t) * CB
        return planes[first : first + CB, 0:128], planes[first : first + CB, 128:256]

    both = lambda a, b: a & b
    column = ((lane & 15) == 0,) * 2
    row = (lane < 16, lane < 0)
    put = lambda m, new, old: each(jnp.where, m, new, old)
    ey_0 = put(hits[0], value[0, 0], face(0, 0))
    ez_0 = put(hits[0], value[0, 1], face(0, 1))
    ez_1 = put(each(both, row, hits[0]), value[0, 1], face(1, 1))
    ey_2 = put(each(both, column, hits[0]), value[0, 0], face(2, 1))
    ex_1 = put(hits[1], value[1, 0], face(1, 0))
    ez_1 = put(hits[1], value[1, 1], ez_1)
    ez_0 = put(each(both, row, hits[1]), value[1, 1], ez_0)
    ex_2 = put(each(both, row, hits["1x"]), value["1x"], face(2, 0))
    ex_2 = put(hits[2], value[2, 0], ex_2)
    ey_2 = put(hits[2], value[2, 1], ey_2)
    ex_1 = put(each(both, column, hits["2x"]), value["2x"], ex_1)
    ey_0 = put(each(both, column, hits[2]), value[2, 1], ey_0)
    curl = lambda p, q, r, s: (p - q) - (r - s)
    curls = (
        each(curl, y_next(ez_0), ez_0, z_next(ey_0), ey_0),
        each(curl, z_next(ex_1), ex_1, y_next(ez_1), ez_1),
        each(curl, z_next(ey_2), ey_2, y_next(ex_2), ex_2),
    )
    straight = jnp.concatenate(
        [jnp.concatenate(curls[0], axis=1), jnp.concatenate(curls[1], axis=1)], axis=0
    )
    quads_c = jnp.concatenate(
        [
            mm_left(straight, quadrant[0]),
            mm_left(jnp.concatenate(curls[2], axis=1), quadrant[1]),
        ],
        axis=0,
    )
    wide_lane = lax.broadcasted_iota(jnp.int32, (PEERS, 3 * CB), 1)
    out_lane = lax.broadcasted_iota(jnp.int32, (PEERS, 128), 1)
    for part, quads in enumerate((quads_b[...], quads_c)):
        answers = []
        for k in range(2):
            key = keys[k]
            place = jnp.where(key >= 0, (key >> 6) * CB + (key & 15), -1)
            pick = (place == wide_lane).astype(F32).astype(BF16)
            found = mm_right(pick, quads)
            quad = (key >> 4) & 3
            side = jnp.where(quad >= 2, found[:, 128:256], found[:, 0:128])
            answers.append(jnp.where((quad & 1) == k, side, pltpu.roll(side, 64, 1)))
        side = slice(part * 128, (part + 1) * 128)
        out[:, 0, side] = jnp.where(out_lane < 64, answers[0], answers[1])
    send = pltpu.make_async_copy(out, back, sems.at[1])
    send.start()
    for copy in (store, send):
        copy.wait()


def curls(load, curl):
    first = [load(c, 0) for c in range(3)]
    now = first
    turn = lambda p, q, r, s: (p - q) - (r - s)
    for i in range(EDGE):
        far = [load(c, i + 1) for c in range(3)] if i + 1 < EDGE else first
        ex, ey, ez = now
        put_slab(curl, 0, i, 0, CB, each(turn, y_next(ez), ez, z_next(ey), ey))
        put_slab(curl, 1, i, 0, CB, each(turn, z_next(ex), ex, far[2], ez))
        put_slab(curl, 2, i, 0, CB, each(turn, far[1], ey, y_next(ex), ex))
        now = far


def curl_kernel(emf_c, far_patch, masks, emf_f, curl_c, curl_f, patch, sems):
    load_patch = pltpu.make_async_copy(far_patch, patch, sems.at[0])
    load_patch.start()
    curls(lambda c, i: slab(emf_f, c, i, 0, CB), curl_f)
    lane = lax.broadcasted_iota(jnp.int32, (CB, 128), 1)

    def pair(ref, first):
        return ref[first : first + CB, 0:128], ref[first : first + CB, 128:256]

    load_patch.wait()
    planes = {(d, t): pair(patch, (d * 2 + t) * CB) for d in range(3) for t in range(2)}
    bits = [m.astype(jnp.int32) for m in pair(masks, 0)]
    hits = [[((m >> d) & 1).astype(F32) for m in bits] for d in range(3)]
    ready = {}

    def corrected(i):
        now = {c: slab(emf_c, c, i, 0, CB) for c in range(3)}
        if i == 0:
            for t, c in enumerate(TANGENT[0]):
                now[c] = each(lambda m, p, e: jnp.where(m > 0.5, p, e), hits[0], planes[0, t], now[c])
        turn, h = (8 - i % 8) % 8 * 16, i // 8
        there = (lane < 16) & (pltpu.roll(hits[1][h], turn, 1) > 0.5)
        for t, c in enumerate(TANGENT[1]):
            now[c] = (jnp.where(there, pltpu.roll(planes[1, t][h], turn, 1), now[c][0]), now[c][1])
        turn = (128 - i) % 128
        there = [((lane & 15) == 0) & (pltpu.roll(m, turn, 1) > 0.5) for m in hits[2]]
        for t, c in enumerate(TANGENT[2]):
            value = [pltpu.roll(p, turn, 1) for p in planes[2, t]]
            now[c] = each(jnp.where, there, value, now[c])
        return now

    def load(c, i):
        if i not in ready:
            ready[i] = corrected(i)
        return ready[i][c]

    curls(load, curl_c)


def update_kernel(
    top, curl_c, curl_f, b_c, b_f, far_pairs,
    new_c, new_f, picked, chosen,
    out_c, out_f, pairs, sems,
):
    load = pltpu.make_async_copy(far_pairs, pairs, sems.at[2])
    load.start()
    time_step = 0.2 / top[0:1, 2:3]
    results = []
    step = lambda factor: lambda b, c: b - factor * c
    for i in range(EDGE):
        for c in range(3):
            value = each(step(time_step), slab(b_c, c, i, 0, CB), slab(curl_c, c, i, 0, CB))
            put_slab(out_c, c, i, 0, CB, value)
        if i % 4 == 3:
            part = pl.ds((i - 3) * WIDE, 4 * WIDE)
            copy = pltpu.make_async_copy(out_c.at[:, :, part], new_c.at[:, :, part], sems.at[1])
            copy.start()
            results.append(copy)
    for i in range(EDGE):
        for c in range(3):
            value = each(step(time_step / 0.5), slab(b_f, c, i, 0, CB), slab(curl_f, c, i, 0, CB))
            put_fine_slab(out_f, c, i, value)
    for b in range(FB):
        copy = pltpu.make_async_copy(out_f.at[pl.ds(b * PITCH, 96)], new_f.at[b], sems.at[0])
        copy.start()
        results.append(copy)
    faces = (
        fine_slab(out_f, 0, 0),
        face_row_wise(lambda i: fine_slab(out_f, 1, i)[0]),
        face_column_wise(lambda i: fine_slab(out_f, 2, i)),
    )
    load.wait()
    first, second, source = routes(pairs)
    tn = ((0,), (0,))
    same = (
        lax.broadcasted_iota(jnp.int32, (PEERS, PEERS), 0)
        == lax.broadcasted_iota(jnp.int32, (PEERS, PEERS), 1)
    ).astype(F32).astype(BF16)
    chosen[...] = jnp.concatenate(
        [mm(first.astype(BF16), same, tn), mm(second.astype(BF16), same, tn)], axis=1
    )
    source = source.astype(BF16)
    flip = flip_matrix()
    normals = [jnp.concatenate(face, axis=1) for face in faces]
    straight = mm_right(source[0 : 2 * CB], jnp.concatenate(normals[0:2], axis=0), tn)
    flipped = mm_left(mm_right(source[2 * CB :], normals[2], tn), flip)
    picked[...] = straight + flipped
    for copy in results:
        copy.wait()


def third_kernel(got, top, picked, chosen, jump, held, sems):
    rows = got[:, 0, 0:128] - (0.2 / top[0:1, 2:3]) * got[:, 0, 128:256]
    lane = lax.broadcasted_iota(jnp.int32, (PAIRS, 128), 1)
    picks = chosen[...].astype(BF16)
    sides = [mm_right(picks[:, k * PEERS : (k + 1) * PEERS], rows) for k in range(2)]
    own = jnp.where(lane < 64, sides[0], sides[1])
    held[...] = picked[...] - mm_left(own, prolong_matrix())
    copy = pltpu.make_async_copy(held, jump, sems.at[0])
    copy.start()
    copy.wait()


VMEM = pl.BlockSpec(memory_space=pltpu.VMEM)
HBM = pl.BlockSpec(memory_space=pltpu.HBM)
FIELD = (3, CB, CELLS)
PITCHED = (CB * PITCH, 128)
FACES = (6 * CB, WIDE)


def call(kernel, outs, args, scratch=(), aliases=None):
    far = [isinstance(out, tuple) and out[0] == "hbm" for out in outs]
    return pl.pallas_call(
        kernel,
        out_shape=[
            pltpu.HBM(out[1], F32) if is_far else pltpu.VMEM(out, F32)
            for out, is_far in zip(outs, far)
        ],
        in_specs=[HBM if is_far else VMEM for _, is_far in args],
        out_specs=[HBM if is_far else VMEM for is_far in far],
        scratch_shapes=list(scratch),
        input_output_aliases=aliases or {},
        compiler_params=pltpu.CompilerParams(vmem_limit_bytes=24 * 1024 * 1024),
    )(
        *(
            pltpu.with_memory_space_constraint(a, pltpu.HBM if is_far else pltpu.VMEM)
            for a, is_far in args
        )
    )


def on_device(coarse_field, coarse_velocity, fine_field, fine_velocity, pairs):
    cb = coarse_field[0].transpose(1, 0, 2)
    cv = coarse_velocity[0].transpose(1, 0, 2)
    fb = fine_field[0].reshape(FB, 96, 128)
    fv = fine_velocity[0].reshape(FB, 96, 128)
    rows = pairs.transpose(2, 0, 1)
    near = lambda *arrays: [(a, False) for a in arrays]
    far = lambda *arrays: [(a, True) for a in arrays]
    count = lax.axis_size("gz")

    field = pltpu.VMEM(FIELD, F32)
    pitched = pltpu.VMEM(PITCHED, F32)
    small = pltpu.VMEM((6, 1, PAIRS), jnp.int32)
    sems = pltpu.SemaphoreType.DMA
    send, emf_f, b_f = call(
        first_kernel,
        [("hbm", (PEERS, 1, 384)), FIELD, FIELD],
        far(cb, cv, fb, fv, rows),
        [field, field, pitched, pitched, small, pltpu.VMEM((PEERS, 1, 384), F32), sems((9,))],
    )
    got = lax.all_to_all(send, BLOCKS, 0, 0, tiled=True)
    emf_c, planes, quads, b_c = call(
        coarse_kernel, [FIELD, FACES, (3 * CB, WIDE), FIELD], far(cb, cv), [field, sems((4,))]
    )
    got, emf_c, planes, quads, b_c = lax.optimization_barrier((got, emf_c, planes, quads, b_c))
    back, patch, masks, top = call(
        answer_kernel,
        [("hbm", (PEERS, 1, 256)), ("hbm", FACES), (CB, WIDE), (1, 128)],
        near(got, planes, quads),
        [pltpu.VMEM(FACES, F32), pltpu.VMEM((PEERS, 1, 256), F32), sems((2,))],
    )
    others = []
    for k in range(1, count):
        others.append(lax.ppermute(top, "gz", [(i, (i + k) % count) for i in range(count)]))
    for other in others:
        top = jnp.maximum(top, other)
    returned = lax.all_to_all(back, BLOCKS, 0, 0, tiled=True)
    curl_c, curl_f = call(
        curl_kernel,
        [FIELD, FIELD],
        near(emf_c) + far(patch) + near(masks, emf_f),
        [pltpu.VMEM(FACES, F32), sems((1,))],
        {0: 0, 3: 1},
    )
    new_c, new_f, picked, chosen = call(
        update_kernel,
        [("hbm", FIELD), ("hbm", (FB, 96, 128)), (PAIRS, WIDE), (PAIRS, 128)],
        near(top, curl_c, curl_f, b_c, b_f) + far(rows),
        [field, pitched, small, sems((3,))],
    )
    (jump,) = call(
        third_kernel,
        [("hbm", (PAIRS, WIDE))],
        near(returned, top, picked, chosen),
        [pltpu.VMEM((PAIRS, WIDE), F32), sems((1,))],
    )
    return (
        new_c.transpose(1, 0, 2)[None],
        new_f.reshape(1, FB, 3, CELLS),
        jump[None],
    )


def solution(mesh):
    split = Mesh(
        mesh.devices.reshape(4, 8, 2, mesh.shape["gz"]), ("blocks_0", "blocks_1", "blocks_2", "gz")
    )
    in_specs = (
        P("gz", BLOCKS, None, None),
        P("gz", BLOCKS, None, None),
        P("gz", BLOCKS, None, None),
        P("gz", BLOCKS, None, None),
        P("gz", BLOCKS, None),
    )
    out_specs = (P("gz", BLOCKS, None, None), P("gz", BLOCKS, None, None), P("gz", BLOCKS, None))

    return jax.shard_map(on_device, mesh=split, in_specs=in_specs, out_specs=out_specs, check_vma=False)
```

```python
import jax
import jax.numpy as jnp
from jax import lax
from jax.experimental import pallas as pl
from jax.experimental.pallas import tpu as pltpu
from jax.sharding import Mesh
from jax.sharding import PartitionSpec as P

EDGE = 16
HALF = 8
CB = 16
FB = 12
PAIRS = 32
PEERS = 64
WIDE = EDGE * EDGE
CELLS = EDGE**3
PITCH = 104
BLOCKS = ("blocks_0", "blocks_1", "blocks_2")
F32 = jnp.float32
BF16 = jnp.bfloat16
TANGENT = ((1, 2), (0, 2), (0, 1))
CHUNK = 16


def grid_of(rows, cols):
    return (
        lax.broadcasted_iota(jnp.int32, (rows, cols), 0),
        lax.broadcasted_iota(jnp.int32, (1, cols), 1),
    )


def face_lane(row, col, flip):
    return col * EDGE + row if flip else row * EDGE + col


def as_matrix(where, value=1.0):
    return jnp.where(where, value, 0.0).astype(BF16)


def restrict_matrix(flip):
    at, to = grid_of(WIDE, 128)
    m, n = (to >> 3) & 7, to & 7
    base = face_lane(2 * m, 2 * n, flip)
    firsts = (to < 64) & ((at == base) | (at == base + face_lane(1, 0, flip)))
    seconds = (to >= 64) & ((at == base) | (at == base + face_lane(0, 1, flip)))
    return jnp.concatenate([as_matrix(firsts, 0.5), as_matrix(seconds, 0.5)], axis=0)


def expand_matrix(flip):
    at, _ = grid_of(128, 256)
    to = lax.broadcasted_iota(jnp.int32, (128, 256), 1)
    place = face_lane((at >> 3) & 7, at & 7, flip)
    return as_matrix(((at >> 6) == (to >> 7)) & (place == (to & 127)))


def quadrant_matrix(flip):
    at, to = grid_of(WIDE, WIDE)
    row, col = (to >> 7) * HALF + ((to >> 3) & 7), ((to >> 6) & 1) * HALF + (to & 7)
    return as_matrix(at == face_lane(row, col, flip))


def flip_matrix():
    at, to = grid_of(WIDE, WIDE)
    return as_matrix(at == (to & 15) * EDGE + (to >> 4))


def prolong_matrix():
    at, to = grid_of(128, WIDE)
    return as_matrix((at & 63) == (to >> 5) * HALF + ((to & 15) >> 1))


def halves(value):
    high = value.astype(BF16)
    return high, (value - high.astype(F32)).astype(BF16)


def mm(a, b, dims=((1,), (0,))):
    return lax.dot_general(a, b, (dims, ((), ())), preferred_element_type=F32)


def mm_left(value, matrix, dims=((1,), (0,))):
    high, low = halves(value)
    return mm(high, matrix, dims) + mm(low, matrix, dims)


def mm_right(matrix, value, dims=((1,), (0,))):
    high, low = halves(value)
    return mm(matrix, high, dims) + mm(matrix, low, dims)


def lanes_of(value):
    return lax.broadcasted_iota(jnp.int32, value.shape, 1)


def y_next(p):
    a, b = pltpu.roll(p[0], 112, 1), pltpu.roll(p[1], 112, 1)
    edge = lanes_of(a) >= 112
    return jnp.where(edge, b, a), jnp.where(edge, a, b)


def z_next(p):
    edge = (lanes_of(p[0]) & 15) == 15
    return tuple(jnp.where(edge, pltpu.roll(x, 15, 1), pltpu.roll(x, 127, 1)) for x in p)


def each(fn, *pairs):
    return tuple(fn(*(p[h] for p in pairs)) for h in range(2))


def span(i, half):
    start = i * WIDE + half * 128
    return pl.ds(start if isinstance(start, int) else pl.multiple_of(start, 128), 128)


def slab(ref, comp, i, first, count):
    return tuple(ref[comp, first : first + count, span(i, half)] for half in range(2))


def put_slab(ref, comp, i, first, count, value):
    for half in range(2):
        ref[comp, first : first + count, span(i, half)] = value[half]


def fine_slab(ref, comp, i):
    def one(half):
        start = comp * 32 + 2 * i + half
        return jnp.concatenate(
            [
                ref[pl.ds(start, 8, stride=PITCH), :],
                ref[pl.ds(start + 8 * PITCH, 8, stride=PITCH), :],
            ],
            axis=0,
        )

    return one(0), one(1)


def put_fine_slab(ref, comp, i, value):
    for half in range(2):
        start = comp * 32 + 2 * i + half
        ref[pl.ds(start, 8, stride=PITCH), :] = value[half][0:8]
        ref[pl.ds(start + 8 * PITCH, 8, stride=PITCH), :] = value[half][8:16]


def fetch_fine(source, target, sem):
    return [
        pltpu.make_async_copy(source.at[b], target.at[pl.ds(b * PITCH, 96)], sem)
        for b in range(FB)
    ]


def face_row_wise(load):
    out = [jnp.zeros((CB, 128), F32)] * 2
    group = lax.broadcasted_iota(jnp.int32, (CB, 128), 1) // 16
    for i in range(EDGE):
        turned = pltpu.roll(load(i), i % 8 * 16, 1)
        out[i // 8] = jnp.where(group == i % 8, turned, out[i // 8])
    return tuple(out)


def face_column_wise(load):
    out = (jnp.zeros((CB, 128), F32),) * 2
    column = lax.broadcasted_iota(jnp.int32, (CB, 128), 1) & 15
    for i in range(EDGE):
        out = each(lambda x, h: jnp.where(column == i, pltpu.roll(x, i, 1), h), load(i), out)
    return out


def routes(pairs_ref):
    slot, face, owner = pairs_ref[0], pairs_ref[1], pairs_ref[2]
    peer = lax.broadcasted_iota(jnp.int32, (PEERS, PAIRS), 0)
    named = (owner == peer).astype(F32)
    before = (
        lax.broadcasted_iota(jnp.int32, (PAIRS, PAIRS), 0)
        < lax.broadcasted_iota(jnp.int32, (PAIRS, PAIRS), 1)
    ).astype(F32)
    earlier = mm(named.astype(BF16), before.astype(BF16))
    rank = jnp.sum(named * earlier, axis=0, keepdims=True)
    first = jnp.where(rank < 0.5, named, 0.0)
    second = jnp.where(rank < 0.5, 0.0, named)
    at_row = lax.broadcasted_iota(jnp.int32, (3 * CB, PAIRS), 0)
    source = (face * CB + slot == at_row).astype(F32)
    return first, second, source


def lane_maps():
    at, to = grid_of(WIDE, WIDE)
    z_back = (to & ~15) | ((to - 1) & 15)
    z_on = (to & ~15) | ((to + 1) & 15)
    return at, to, (to - 16) & 255, (to + 16) & 255, z_back, z_on


def corner_matrices():
    at, to, y_back, _, z_back, _ = lane_maps()
    same, y, z = at == to, at == y_back, at == z_back
    both = at == ((z_back - 16) & 255)
    return as_matrix(same | y | z | both, 0.25), as_matrix(same | z, 0.25), as_matrix(same | y, 0.25)


def ahead_matrices():
    at, to, _, y_on, _, z_on = lane_maps()
    own = jnp.where(at == to, 1.0, 0.0)
    return tuple((jnp.where(at == on, 1.0, 0.0) - own).astype(BF16) for on in (y_on, z_on))


def stacked(load, c, slabs):
    return jnp.concatenate([jnp.concatenate(load(c, i % EDGE), axis=1) for i in slabs], axis=0)


def put_stacked(ref, c, slabs, value):
    for k, i in enumerate(slabs):
        part = value[k * CB : (k + 1) * CB]
        put_slab(ref, c, i, 0, CB, (part[:, 0:128], part[:, 128:256]))


def edges(cell, emf, corners):
    load = lambda c, i: slab(cell, c, i, 0, CB)
    for start in range(0, EDGE, CHUNK):
        here, prior = range(start, start + CHUNK), range(start - 1, start - 1 + CHUNK)
        put_stacked(emf, 0, here, mm_left(stacked(load, 0, here), corners[0]))
        for c in (1, 2):
            both = stacked(load, c, here) + stacked(load, c, prior)
            put_stacked(emf, c, here, mm_left(both, corners[c]))


def curls(emf, curl, aheads):
    load = lambda c, i: slab(emf, c, i, 0, CB)
    ahead_y, ahead_z = aheads
    for start in range(0, EDGE, CHUNK):
        here, far = range(start, start + CHUNK), range(start + 1, start + 1 + CHUNK)
        ex, ey, ez = (stacked(load, c, here) for c in range(3))
        put_stacked(curl, 0, here, mm_left(ez, ahead_y) - mm_left(ey, ahead_z))
        put_stacked(curl, 1, here, mm_left(ex, ahead_z) - (stacked(load, 2, far) - ez))
        put_stacked(curl, 2, here, (stacked(load, 1, far) - ey) - mm_left(ex, ahead_y))


def face_of(ref, along, d):
    if d == 0:
        return slab(ref, along, 0, 0, CB)
    if d == 1:
        return face_row_wise(lambda i: slab(ref, along, i, 0, CB)[0])
    return face_column_wise(lambda i: slab(ref, along, i, 0, CB))


def coarse_parts(cb, cv, b_c, v_c, sems):
    return [
        [
            pltpu.make_async_copy(far.at[:, :, part], near.at[:, :, part], sems.at[q])
            for far, near in ((cb, b_c), (cv, v_c))
        ]
        for q, part in enumerate(pl.ds(q * 4 * WIDE, 4 * WIDE) for q in range(4))
    ]


def wait_part(copies, i):
    for q in range(4):
        if i == max(4 * q - 1, 0):
            for copy in copies[q]:
                copy.wait()


def centres(load_b, i):
    bx, by, bz = (load_b(c, i) for c in range(3))
    mean = lambda a, b: 0.5 * (a + b)
    return (
        each(mean, bx, load_b(0, (i + 1) % EDGE)),
        each(mean, by, y_next(by)),
        each(mean, bz, z_next(bz)),
    )


def speeds(centre, velocity):
    size = lambda a, b, c: jnp.sqrt(a * a + b * b + c * c)
    fast = each(lambda a, b: a + b, each(size, *velocity), each(size, *centre))
    return jnp.maximum(fast[0], fast[1])


def put_cell(cell, i, centre, velocity):
    cross = lambda a, b, c, d: a * b - c * d
    (cx, cy, cz), (vx, vy, vz) = centre, velocity
    put_slab(cell, 0, i, 0, CB, each(cross, vz, cy, vy, cz))
    put_slab(cell, 1, i, 0, CB, each(cross, vx, cz, vz, cx))
    put_slab(cell, 2, i, 0, CB, each(cross, vy, cx, vx, cy))


def first_kernel(
    cb, cv, fb, fv, far_pairs,
    send, emf_f, b_f,
    b_c, v_c, pitched_b, v_f, cell_f, pairs, out, held_corners, held_restrict, sems,
):
    fine_copies = fetch_fine(fb, pitched_b, sems.at[0]) + fetch_fine(fv, v_f, sems.at[1])
    coarse_copies = coarse_parts(cb, cv, b_c, v_c, sems.at[pl.ds(2, 4)])
    pairs_copy = pltpu.make_async_copy(far_pairs, pairs, sems.at[6])
    for copy in [pairs_copy, *fine_copies, *sum(coarse_copies, [])]:
        copy.start()
    idle = pl.ds(FB * PITCH, (CB - FB) * PITCH)
    pitched_b[idle, :] = jnp.zeros(((CB - FB) * PITCH, 128), F32)
    v_f[idle, :] = jnp.zeros(((CB - FB) * PITCH, 128), F32)
    pairs_copy.wait()
    first, second, source = routes(pairs)
    nt = ((1,), (1,))
    key = (pairs[1] * 64 + (pairs[4] * 2 + pairs[5]) * CB + pairs[3] + 1).astype(F32)
    lane = lax.broadcasted_iota(jnp.int32, (PEERS, 128), 1)
    meta = jnp.zeros((PEERS, 128), F32)
    picks = []
    for k, chosen in enumerate((first, second)):
        picks.append(mm(chosen.astype(BF16), source.astype(BF16), nt).astype(BF16))
        meta = jnp.where(lane == k, jnp.sum(chosen * key, axis=1, keepdims=True), meta)

    corners = corner_matrices()
    for k in range(3):
        held_corners[k] = corners[k]
    restrict = [restrict_matrix(False), restrict_matrix(True)]
    for k in range(2):
        held_restrict[k] = restrict[k]
    for copy in fine_copies:
        copy.wait()
    held = {}

    def fine_b(c, i):
        if (c, i) not in held:
            held[c, i] = fine_slab(pitched_b, c, i)
            put_slab(b_f, c, i, 0, CB, held[c, i])
        return held[c, i]

    top_fine = top_coarse = jnp.zeros((CB, 128), F32)
    for i in range(EDGE):
        centre, velocity = centres(fine_b, i), [fine_slab(v_f, c, i) for c in range(3)]
        put_cell(cell_f, i, centre, velocity)
        top_fine = jnp.maximum(top_fine, speeds(centre, velocity))
    edges(cell_f, emf_f, held_corners)
    restrict = held_restrict
    rows = []
    for d in range(3):
        planes = [face_of(emf_f, along, d) for along in TANGENT[d]]
        both = jnp.concatenate([*planes[0], *planes[1]], axis=1)
        rows.append(mm_left(both, restrict[1 if d == 2 else 0]))
    rows = jnp.concatenate(rows, axis=0)
    for k in range(2):
        out[:, 0, k * 128 : (k + 1) * 128] = mm_right(picks[k], rows)
    rows_copy = pltpu.make_async_copy(
        out.at[:, :, pl.ds(0, 256)], send.at[:, :, pl.ds(0, 256)], sems.at[7]
    )
    rows_copy.start()

    for i in range(EDGE):
        wait_part(coarse_copies, i)
        centre = centres(lambda c, k: slab(b_c, c, k, 0, CB), i)
        top_coarse = jnp.maximum(top_coarse, speeds(centre, [slab(v_c, c, i, 0, CB) for c in range(3)]))
    top = jnp.max(jnp.maximum(top_fine, top_coarse), axis=0, keepdims=True)
    top = jnp.broadcast_to(jnp.max(top, axis=1, keepdims=True), (PEERS, 128))
    out[:, 0, 256:384] = jnp.where(lane < 2, meta, top)
    meta_copy = pltpu.make_async_copy(
        out.at[:, :, pl.ds(256, 128)], send.at[:, :, pl.ds(256, 128)], sems.at[8]
    )
    meta_copy.start()
    rows_copy.wait()
    meta_copy.wait()


def coarse_kernel(cb, cv, emf_f, emf, planes, quads, b_c, curl_f, v_c, cell, held, sems):
    copies = coarse_parts(cb, cv, b_c, v_c, sems)
    for copy in sum(copies, []):
        copy.start()
    corners, aheads = corner_matrices(), ahead_matrices()
    curls(emf_f, held, aheads)
    for c in range(3):
        curl_f[c] = held[c]
    load_b, load_v = (lambda c, i, ref=ref: slab(ref, c, i, 0, CB) for ref in (b_c, v_c))
    for i in range(EDGE):
        wait_part(copies, i)
        centre = centres(load_b, i)
        put_cell(cell, i, centre, [load_v(c, i) for c in range(3)])
    edges(cell, emf, corners)
    for d in range(3):
        for t in range(2):
            at = (d * 2 + t) * CB
            face = face_of(emf, TANGENT[d][t], d)
            planes[at : at + CB, 0:128] = face[0]
            planes[at : at + CB, 128:256] = face[1]
    quadrant = [quadrant_matrix(False), quadrant_matrix(True)]
    for d in range(3):
        normal = jnp.concatenate(face_of(b_c, d, d), axis=1)
        quads[d * CB : (d + 1) * CB, :] = mm_left(normal, quadrant[1 if d == 2 else 0])


def answer_kernel(
    got, planes, quads_b, back, far_patch, masks, top, patch, out, sems
):
    expand = [expand_matrix(False), expand_matrix(True)]
    quadrant = [quadrant_matrix(False), quadrant_matrix(True)]
    meta = got[:, 0, 256:384]
    top[...] = jnp.max(meta, axis=0, keepdims=True)
    keys = [meta[:, k : k + 1].astype(jnp.int32) - 1 for k in range(2)]
    target = lax.broadcasted_iota(jnp.int32, (PEERS, 256), 1)
    hit = jnp.concatenate([(k == target).astype(F32) for k in keys], axis=0).astype(BF16)
    rows = jnp.concatenate([got[:, 0, 0:128], got[:, 0, 128:256]], axis=0)
    tn = ((0,), (0,))
    replaced = mm_right(hit, rows, tn)[0:192]
    counted = mm(hit, jnp.ones((2 * PEERS, 128), BF16), tn)[0:192]
    spread = (mm_left(replaced, expand[0]), mm_left(replaced, expand[1]))
    lane = lax.broadcasted_iota(jnp.int32, (CB, 128), 1)

    def at(d, quad):
        return slice(d * 64 + quad * CB, d * 64 + (quad + 1) * CB)

    def value(d, t, flip):
        part = slice(t * 128, (t + 1) * 128)
        out = []
        for h in range(2):
            near, far = (h, h + 2) if flip else (2 * h, 2 * h + 1)
            x = spread[flip]
            out.append(x[at(d, near), part] + pltpu.roll(x[at(d, far), part], 8, 1))
        return tuple(out)

    def mask(d, flip):
        out = []
        for h in range(2):
            near, far = (h, h + 2) if flip else (2 * h, 2 * h + 1)
            out.append(jnp.where((lane & 15) < 8, counted[at(d, near)], counted[at(d, far)]) > 0.5)
        return tuple(out)

    value = {
        (d, t): value(d, t, int(d == 2)) for d in range(3) for t in range(2)
    } | {"1x": value(1, 0, 1), "2x": value(2, 0, 0)}
    hits = {d: mask(d, int(d == 2)) for d in range(3)} | {"1x": mask(1, 1), "2x": mask(2, 0)}
    for h in range(2):
        side = slice(h * 128, (h + 1) * 128)
        masks[:, side] = sum(hits[d][h].astype(F32) * 2.0**d for d in range(3))
        for d in range(3):
            for t in range(2):
                first = (d * 2 + t) * CB
                patch[first : first + CB, side] = value[d, t][h]

    store = pltpu.make_async_copy(patch, far_patch, sems.at[0])
    store.start()

    def face(d, t):
        first = (d * 2 + t) * CB
        return planes[first : first + CB, 0:128], planes[first : first + CB, 128:256]

    both = lambda a, b: a & b
    column = ((lane & 15) == 0,) * 2
    row = (lane < 16, lane < 0)
    put = lambda m, new, old: each(jnp.where, m, new, old)
    ey_0 = put(hits[0], value[0, 0], face(0, 0))
    ez_0 = put(hits[0], value[0, 1], face(0, 1))
    ez_1 = put(each(both, row, hits[0]), value[0, 1], face(1, 1))
    ey_2 = put(each(both, column, hits[0]), value[0, 0], face(2, 1))
    ex_1 = put(hits[1], value[1, 0], face(1, 0))
    ez_1 = put(hits[1], value[1, 1], ez_1)
    ez_0 = put(each(both, row, hits[1]), value[1, 1], ez_0)
    ex_2 = put(each(both, row, hits["1x"]), value["1x"], face(2, 0))
    ex_2 = put(hits[2], value[2, 0], ex_2)
    ey_2 = put(hits[2], value[2, 1], ey_2)
    ex_1 = put(each(both, column, hits["2x"]), value["2x"], ex_1)
    ey_0 = put(each(both, column, hits[2]), value[2, 1], ey_0)
    curl = lambda p, q, r, s: (p - q) - (r - s)
    curls = (
        each(curl, y_next(ez_0), ez_0, z_next(ey_0), ey_0),
        each(curl, z_next(ex_1), ex_1, y_next(ez_1), ez_1),
        each(curl, z_next(ey_2), ey_2, y_next(ex_2), ex_2),
    )
    straight = jnp.concatenate(
        [jnp.concatenate(curls[0], axis=1), jnp.concatenate(curls[1], axis=1)], axis=0
    )
    quads_c = jnp.concatenate(
        [
            mm_left(straight, quadrant[0]),
            mm_left(jnp.concatenate(curls[2], axis=1), quadrant[1]),
        ],
        axis=0,
    )
    wide_lane = lax.broadcasted_iota(jnp.int32, (PEERS, 3 * CB), 1)
    out_lane = lax.broadcasted_iota(jnp.int32, (PEERS, 128), 1)
    for part, quads in enumerate((quads_b[...], quads_c)):
        answers = []
        for k in range(2):
            key = keys[k]
            place = jnp.where(key >= 0, (key >> 6) * CB + (key & 15), -1)
            pick = (place == wide_lane).astype(F32).astype(BF16)
            found = mm_right(pick, quads)
            quad = (key >> 4) & 3
            side = jnp.where(quad >= 2, found[:, 128:256], found[:, 0:128])
            answers.append(jnp.where((quad & 1) == k, side, pltpu.roll(side, 64, 1)))
        side = slice(part * 128, (part + 1) * 128)
        out[:, 0, side] = jnp.where(out_lane < 64, answers[0], answers[1])
    send = pltpu.make_async_copy(out, back, sems.at[1])
    send.start()
    for copy in (store, send):
        copy.wait()


def curl_kernel(emf_c, far_patch, masks, curl_c, patch, held, sems):
    load_patch = pltpu.make_async_copy(far_patch, patch, sems.at[0])
    load_patch.start()
    lane = lax.broadcasted_iota(jnp.int32, (CB, 128), 1)

    def pair(ref, first):
        return ref[first : first + CB, 0:128], ref[first : first + CB, 128:256]

    load_patch.wait()
    planes = {(d, t): pair(patch, (d * 2 + t) * CB) for d in range(3) for t in range(2)}
    bits = [m.astype(jnp.int32) for m in pair(masks, 0)]
    hits = [[((m >> d) & 1).astype(F32) for m in bits] for d in range(3)]
    for i in range(EDGE):
        now = {c: slab(emf_c, c, i, 0, CB) for c in range(3)}
        if i == 0:
            for t, c in enumerate(TANGENT[0]):
                now[c] = each(lambda m, p, e: jnp.where(m > 0.5, p, e), hits[0], planes[0, t], now[c])
        turn, h = (8 - i % 8) % 8 * 16, i // 8
        there = (lane < 16) & (pltpu.roll(hits[1][h], turn, 1) > 0.5)
        for t, c in enumerate(TANGENT[1]):
            now[c] = (jnp.where(there, pltpu.roll(planes[1, t][h], turn, 1), now[c][0]), now[c][1])
        turn = (128 - i) % 128
        there = [((lane & 15) == 0) & (pltpu.roll(m, turn, 1) > 0.5) for m in hits[2]]
        for t, c in enumerate(TANGENT[2]):
            value = [pltpu.roll(p, turn, 1) for p in planes[2, t]]
            now[c] = each(jnp.where, there, value, now[c])
        for c in range(3):
            put_slab(held, c, i, 0, CB, now[c])
    curls(held, curl_c, ahead_matrices())


def update_kernel(
    top, curl_c, curl_f, b_c, b_f, far_pairs,
    new_c, new_f, picked, chosen,
    out_c, out_f, pairs, sems,
):
    load = pltpu.make_async_copy(far_pairs, pairs, sems.at[2])
    load.start()
    time_step = 0.2 / top[0:1, 2:3]
    results = []
    step = lambda factor: lambda b, c: b - factor * c
    for i in range(EDGE):
        for c in range(3):
            value = each(step(time_step), slab(b_c, c, i, 0, CB), slab(curl_c, c, i, 0, CB))
            put_slab(out_c, c, i, 0, CB, value)
        if i % 4 == 3:
            part = pl.ds((i - 3) * WIDE, 4 * WIDE)
            copy = pltpu.make_async_copy(out_c.at[:, :, part], new_c.at[:, :, part], sems.at[1])
            copy.start()
            results.append(copy)
    for i in range(EDGE):
        for c in range(3):
            value = each(step(time_step / 0.5), slab(b_f, c, i, 0, CB), slab(curl_f, c, i, 0, CB))
            put_fine_slab(out_f, c, i, value)
    for b in range(FB):
        copy = pltpu.make_async_copy(out_f.at[pl.ds(b * PITCH, 96)], new_f.at[b], sems.at[0])
        copy.start()
        results.append(copy)
    faces = (
        fine_slab(out_f, 0, 0),
        face_row_wise(lambda i: fine_slab(out_f, 1, i)[0]),
        face_column_wise(lambda i: fine_slab(out_f, 2, i)),
    )
    load.wait()
    first, second, source = routes(pairs)
    tn = ((0,), (0,))
    same = (
        lax.broadcasted_iota(jnp.int32, (PEERS, PEERS), 0)
        == lax.broadcasted_iota(jnp.int32, (PEERS, PEERS), 1)
    ).astype(F32).astype(BF16)
    chosen[...] = jnp.concatenate(
        [mm(first.astype(BF16), same, tn), mm(second.astype(BF16), same, tn)], axis=1
    )
    source = source.astype(BF16)
    flip = flip_matrix()
    normals = [jnp.concatenate(face, axis=1) for face in faces]
    straight = mm_right(source[0 : 2 * CB], jnp.concatenate(normals[0:2], axis=0), tn)
    flipped = mm_left(mm_right(source[2 * CB :], normals[2], tn), flip)
    picked[...] = straight + flipped
    for copy in results:
        copy.wait()


def third_kernel(got, top, picked, chosen, jump, held, sems):
    rows = got[:, 0, 0:128] - (0.2 / top[0:1, 2:3]) * got[:, 0, 128:256]
    lane = lax.broadcasted_iota(jnp.int32, (PAIRS, 128), 1)
    picks = chosen[...].astype(BF16)
    sides = [mm_right(picks[:, k * PEERS : (k + 1) * PEERS], rows) for k in range(2)]
    own = jnp.where(lane < 64, sides[0], sides[1])
    held[...] = picked[...] - mm_left(own, prolong_matrix())
    copy = pltpu.make_async_copy(held, jump, sems.at[0])
    copy.start()
    copy.wait()


VMEM = pl.BlockSpec(memory_space=pltpu.VMEM)
HBM = pl.BlockSpec(memory_space=pltpu.HBM)
FIELD = (3, CB, CELLS)
PITCHED = (CB * PITCH, 128)
FACES = (6 * CB, WIDE)


def call(kernel, outs, args, scratch=(), aliases=None):
    far = [isinstance(out, tuple) and out[0] == "hbm" for out in outs]
    return pl.pallas_call(
        kernel,
        out_shape=[
            pltpu.HBM(out[1], F32) if is_far else pltpu.VMEM(out, F32)
            for out, is_far in zip(outs, far)
        ],
        in_specs=[HBM if is_far else VMEM for _, is_far in args],
        out_specs=[HBM if is_far else VMEM for is_far in far],
        scratch_shapes=list(scratch),
        input_output_aliases=aliases or {},
        compiler_params=pltpu.CompilerParams(vmem_limit_bytes=24 * 1024 * 1024),
    )(
        *(
            pltpu.with_memory_space_constraint(a, pltpu.HBM if is_far else pltpu.VMEM)
            for a, is_far in args
        )
    )


def on_device(coarse_field, coarse_velocity, fine_field, fine_velocity, pairs):
    cb = coarse_field[0].transpose(1, 0, 2)
    cv = coarse_velocity[0].transpose(1, 0, 2)
    fb = fine_field[0].reshape(FB, 96, 128)
    fv = fine_velocity[0].reshape(FB, 96, 128)
    rows = pairs.transpose(2, 0, 1)
    near = lambda *arrays: [(a, False) for a in arrays]
    far = lambda *arrays: [(a, True) for a in arrays]
    count = lax.axis_size("gz")

    field = pltpu.VMEM(FIELD, F32)
    pitched = pltpu.VMEM(PITCHED, F32)
    small = pltpu.VMEM((6, 1, PAIRS), jnp.int32)
    sems = pltpu.SemaphoreType.DMA
    send, emf_f, b_f = call(
        first_kernel,
        [("hbm", (PEERS, 1, 384)), FIELD, FIELD],
        far(cb, cv, fb, fv, rows),
        [
            field,
            field,
            pitched,
            pitched,
            field,
            small,
            pltpu.VMEM((PEERS, 1, 384), F32),
            pltpu.VMEM((3, WIDE, WIDE), BF16),
            pltpu.VMEM((2, 2 * WIDE, 128), BF16),
            sems((9,)),
        ],
    )
    got = lax.all_to_all(send, BLOCKS, 0, 0, tiled=True)
    emf_c, planes, quads, b_c, curl_f = call(
        coarse_kernel,
        [FIELD, FACES, (3 * CB, WIDE), FIELD, FIELD],
        far(cb, cv) + near(emf_f),
        [field, field, field, sems((4,))],
        {2: 4},
    )
    got, emf_c, planes, quads, b_c, curl_f = lax.optimization_barrier(
        (got, emf_c, planes, quads, b_c, curl_f)
    )
    back, patch, masks, top = call(
        answer_kernel,
        [("hbm", (PEERS, 1, 256)), ("hbm", FACES), (CB, WIDE), (1, 128)],
        near(got, planes, quads),
        [pltpu.VMEM(FACES, F32), pltpu.VMEM((PEERS, 1, 256), F32), sems((2,))],
    )
    others = []
    for k in range(1, count):
        others.append(lax.ppermute(top, "gz", [(i, (i + k) % count) for i in range(count)]))
    for other in others:
        top = jnp.maximum(top, other)
    returned = lax.all_to_all(back, BLOCKS, 0, 0, tiled=True)
    (curl_c,) = call(
        curl_kernel,
        [FIELD],
        near(emf_c) + far(patch) + near(masks),
        [pltpu.VMEM(FACES, F32), field, sems((1,))],
        {0: 0},
    )
    new_c, new_f, picked, chosen = call(
        update_kernel,
        [("hbm", FIELD), ("hbm", (FB, 96, 128)), (PAIRS, WIDE), (PAIRS, 128)],
        near(top, curl_c, curl_f, b_c, b_f) + far(rows),
        [field, pitched, small, sems((3,))],
    )
    (jump,) = call(
        third_kernel,
        [("hbm", (PAIRS, WIDE))],
        near(returned, top, picked, chosen),
        [pltpu.VMEM((PAIRS, WIDE), F32), sems((1,))],
    )
    return (
        new_c.transpose(1, 0, 2)[None],
        new_f.reshape(1, FB, 3, CELLS),
        jump[None],
    )


def solution(mesh):
    split = Mesh(
        mesh.devices.reshape(4, 8, 2, mesh.shape["gz"]), ("blocks_0", "blocks_1", "blocks_2", "gz")
    )
    in_specs = (
        P("gz", BLOCKS, None, None),
        P("gz", BLOCKS, None, None),
        P("gz", BLOCKS, None, None),
        P("gz", BLOCKS, None, None),
        P("gz", BLOCKS, None),
    )
    out_specs = (P("gz", BLOCKS, None, None), P("gz", BLOCKS, None, None), P("gz", BLOCKS, None))

    return jax.shard_map(on_device, mesh=split, in_specs=in_specs, out_specs=out_specs, check_vma=False)
```

```python
import jax
import jax.numpy as jnp
from jax import lax
from jax.experimental import pallas as pl
from jax.experimental.pallas import tpu as pltpu
from jax.sharding import Mesh
from jax.sharding import PartitionSpec as P

EDGE = 16
HALF = 8
CB = 16
FB = 12
PAIRS = 32
PEERS = 64
WIDE = EDGE * EDGE
CELLS = EDGE**3
PITCH = 104
BLOCKS = ("blocks_0", "blocks_1", "blocks_2")
F32 = jnp.float32
BF16 = jnp.bfloat16
TANGENT = ((1, 2), (0, 2), (0, 1))
CHUNK = 16


def grid_of(rows, cols):
    return (
        lax.broadcasted_iota(jnp.int32, (rows, cols), 0),
        lax.broadcasted_iota(jnp.int32, (1, cols), 1),
    )


def face_lane(row, col, flip):
    return col * EDGE + row if flip else row * EDGE + col


def as_matrix(where, value=1.0):
    return jnp.where(where, value, 0.0).astype(BF16)


def restrict_matrix(flip):
    at, to = grid_of(WIDE, 128)
    m, n = (to >> 3) & 7, to & 7
    base = face_lane(2 * m, 2 * n, flip)
    firsts = (to < 64) & ((at == base) | (at == base + face_lane(1, 0, flip)))
    seconds = (to >= 64) & ((at == base) | (at == base + face_lane(0, 1, flip)))
    return jnp.concatenate([as_matrix(firsts, 0.5), as_matrix(seconds, 0.5)], axis=0)


def expand_matrix(flip):
    at, _ = grid_of(128, 256)
    to = lax.broadcasted_iota(jnp.int32, (128, 256), 1)
    place = face_lane((at >> 3) & 7, at & 7, flip)
    return as_matrix(((at >> 6) == (to >> 7)) & (place == (to & 127)))


def quadrant_matrix(flip):
    at, to = grid_of(WIDE, WIDE)
    row, col = (to >> 7) * HALF + ((to >> 3) & 7), ((to >> 6) & 1) * HALF + (to & 7)
    return as_matrix(at == face_lane(row, col, flip))


def flip_matrix():
    at, to = grid_of(WIDE, WIDE)
    return as_matrix(at == (to & 15) * EDGE + (to >> 4))


def prolong_matrix():
    at, to = grid_of(128, WIDE)
    return as_matrix((at & 63) == (to >> 5) * HALF + ((to & 15) >> 1))


def halves(value):
    high = value.astype(BF16)
    return high, (value - high.astype(F32)).astype(BF16)


def mm(a, b, dims=((1,), (0,))):
    return lax.dot_general(a, b, (dims, ((), ())), preferred_element_type=F32)


def mm_left(value, matrix, dims=((1,), (0,))):
    high, low = halves(value)
    return mm(high, matrix, dims) + mm(low, matrix, dims)


def mm_right(matrix, value, dims=((1,), (0,))):
    high, low = halves(value)
    return mm(matrix, high, dims) + mm(matrix, low, dims)


def lanes_of(value):
    return lax.broadcasted_iota(jnp.int32, value.shape, 1)


def y_next(p):
    a, b = pltpu.roll(p[0], 112, 1), pltpu.roll(p[1], 112, 1)
    edge = lanes_of(a) >= 112
    return jnp.where(edge, b, a), jnp.where(edge, a, b)


def z_next(p):
    edge = (lanes_of(p[0]) & 15) == 15
    return tuple(jnp.where(edge, pltpu.roll(x, 15, 1), pltpu.roll(x, 127, 1)) for x in p)


def each(fn, *pairs):
    return tuple(fn(*(p[h] for p in pairs)) for h in range(2))


def span(i, half):
    start = i * WIDE + half * 128
    return pl.ds(start if isinstance(start, int) else pl.multiple_of(start, 128), 128)


def slab(ref, comp, i, first, count):
    return tuple(ref[comp, first : first + count, span(i, half)] for half in range(2))


def put_slab(ref, comp, i, first, count, value):
    for half in range(2):
        ref[comp, first : first + count, span(i, half)] = value[half]


def fine_slab(ref, comp, i):
    def one(half):
        start = comp * 32 + 2 * i + half
        return jnp.concatenate(
            [
                ref[pl.ds(start, 8, stride=PITCH), :],
                ref[pl.ds(start + 8 * PITCH, 8, stride=PITCH), :],
            ],
            axis=0,
        )

    return one(0), one(1)


def put_fine_slab(ref, comp, i, value):
    for half in range(2):
        start = comp * 32 + 2 * i + half
        ref[pl.ds(start, 8, stride=PITCH), :] = value[half][0:8]
        ref[pl.ds(start + 8 * PITCH, 8, stride=PITCH), :] = value[half][8:16]


def fetch_fine(source, target, sem):
    return [
        pltpu.make_async_copy(source.at[b], target.at[pl.ds(b * PITCH, 96)], sem)
        for b in range(FB)
    ]


def face_row_wise(load):
    out = [jnp.zeros((CB, 128), F32)] * 2
    group = lax.broadcasted_iota(jnp.int32, (CB, 128), 1) // 16
    for i in range(EDGE):
        turned = pltpu.roll(load(i), i % 8 * 16, 1)
        out[i // 8] = jnp.where(group == i % 8, turned, out[i // 8])
    return tuple(out)


def face_column_wise(load):
    out = (jnp.zeros((CB, 128), F32),) * 2
    column = lax.broadcasted_iota(jnp.int32, (CB, 128), 1) & 15
    for i in range(EDGE):
        out = each(lambda x, h: jnp.where(column == i, pltpu.roll(x, i, 1), h), load(i), out)
    return out


def routes(pairs_ref):
    slot, face, owner = pairs_ref[0], pairs_ref[1], pairs_ref[2]
    peer = lax.broadcasted_iota(jnp.int32, (PEERS, PAIRS), 0)
    named = (owner == peer).astype(F32)
    before = (
        lax.broadcasted_iota(jnp.int32, (PAIRS, PAIRS), 0)
        < lax.broadcasted_iota(jnp.int32, (PAIRS, PAIRS), 1)
    ).astype(F32)
    earlier = mm(named.astype(BF16), before.astype(BF16))
    rank = jnp.sum(named * earlier, axis=0, keepdims=True)
    first = jnp.where(rank < 0.5, named, 0.0)
    second = jnp.where(rank < 0.5, 0.0, named)
    at_row = lax.broadcasted_iota(jnp.int32, (3 * CB, PAIRS), 0)
    source = (face * CB + slot == at_row).astype(F32)
    return first, second, source


def lane_maps():
    at, to = grid_of(WIDE, WIDE)
    z_back = (to & ~15) | ((to - 1) & 15)
    z_on = (to & ~15) | ((to + 1) & 15)
    return at, to, (to - 16) & 255, (to + 16) & 255, z_back, z_on


def corner_matrices():
    at, to, y_back, _, z_back, _ = lane_maps()
    same, y, z = at == to, at == y_back, at == z_back
    both = at == ((z_back - 16) & 255)
    return as_matrix(same | y | z | both, 0.25), as_matrix(same | z, 0.25), as_matrix(same | y, 0.25)


def ahead_matrices():
    at, to, _, y_on, _, z_on = lane_maps()
    own = jnp.where(at == to, 1.0, 0.0)
    return tuple((jnp.where(at == on, 1.0, 0.0) - own).astype(BF16) for on in (y_on, z_on))


def stacked(load, c, slabs):
    return jnp.concatenate([jnp.concatenate(load(c, i % EDGE), axis=1) for i in slabs], axis=0)


def put_stacked(ref, c, slabs, value):
    for k, i in enumerate(slabs):
        part = value[k * CB : (k + 1) * CB]
        put_slab(ref, c, i, 0, CB, (part[:, 0:128], part[:, 128:256]))


def edges(cell, emf, corners):
    load = lambda c, i: slab(cell, c, i, 0, CB)
    for start in range(0, EDGE, CHUNK):
        here, prior = range(start, start + CHUNK), range(start - 1, start - 1 + CHUNK)
        put_stacked(emf, 0, here, mm_left(stacked(load, 0, here), corners[0]))
        for c in (1, 2):
            both = stacked(load, c, here) + stacked(load, c, prior)
            put_stacked(emf, c, here, mm_left(both, corners[c]))


def curls(emf, curl, aheads):
    load = lambda c, i: slab(emf, c, i, 0, CB)
    ahead_y, ahead_z = aheads
    for start in range(0, EDGE, CHUNK):
        here, far = range(start, start + CHUNK), range(start + 1, start + 1 + CHUNK)
        ex, ey, ez = (stacked(load, c, here) for c in range(3))
        put_stacked(curl, 0, here, mm_left(ez, ahead_y) - mm_left(ey, ahead_z))
        put_stacked(curl, 1, here, mm_left(ex, ahead_z) - (stacked(load, 2, far) - ez))
        put_stacked(curl, 2, here, (stacked(load, 1, far) - ey) - mm_left(ex, ahead_y))


def face_of(ref, along, d):
    if d == 0:
        return slab(ref, along, 0, 0, CB)
    if d == 1:
        return face_row_wise(lambda i: slab(ref, along, i, 0, CB)[0])
    return face_column_wise(lambda i: slab(ref, along, i, 0, CB))


def coarse_parts(cb, cv, b_c, v_c, sems):
    return [
        [
            pltpu.make_async_copy(far.at[:, :, part], near.at[:, :, part], sems.at[q])
            for far, near in ((cb, b_c), (cv, v_c))
        ]
        for q, part in enumerate(pl.ds(q * 4 * WIDE, 4 * WIDE) for q in range(4))
    ]


def wait_part(copies, i):
    for q in range(4):
        if i == max(4 * q - 1, 0):
            for copy in copies[q]:
                copy.wait()


def centres(load_b, i):
    bx, by, bz = (load_b(c, i) for c in range(3))
    mean = lambda a, b: 0.5 * (a + b)
    return (
        each(mean, bx, load_b(0, (i + 1) % EDGE)),
        each(mean, by, y_next(by)),
        each(mean, bz, z_next(bz)),
    )


def speeds(centre, velocity):
    size = lambda a, b, c: jnp.sqrt(a * a + b * b + c * c)
    fast = each(lambda a, b: a + b, each(size, *velocity), each(size, *centre))
    return jnp.maximum(fast[0], fast[1])


def put_cell(cell, i, centre, velocity):
    cross = lambda a, b, c, d: a * b - c * d
    (cx, cy, cz), (vx, vy, vz) = centre, velocity
    put_slab(cell, 0, i, 0, CB, each(cross, vz, cy, vy, cz))
    put_slab(cell, 1, i, 0, CB, each(cross, vx, cz, vz, cx))
    put_slab(cell, 2, i, 0, CB, each(cross, vy, cx, vx, cy))


def first_kernel(
    cb, cv, fb, fv, far_pairs,
    send, emf_f, b_f,
    b_c, v_c, pitched_b, v_f, cell_f, pairs, out, held_corners, held_restrict, sems,
):
    fine_copies = fetch_fine(fb, pitched_b, sems.at[0]) + fetch_fine(fv, v_f, sems.at[1])
    coarse_copies = coarse_parts(cb, cv, b_c, v_c, sems.at[pl.ds(2, 4)])
    pairs_copy = pltpu.make_async_copy(far_pairs, pairs, sems.at[6])
    for copy in [pairs_copy, *fine_copies]:
        copy.start()
    idle = pl.ds(FB * PITCH, (CB - FB) * PITCH)
    pitched_b[idle, :] = jnp.zeros(((CB - FB) * PITCH, 128), F32)
    v_f[idle, :] = jnp.zeros(((CB - FB) * PITCH, 128), F32)
    pairs_copy.wait()
    first, second, source = routes(pairs)
    nt = ((1,), (1,))
    key = (pairs[1] * 64 + (pairs[4] * 2 + pairs[5]) * CB + pairs[3] + 1).astype(F32)
    lane = lax.broadcasted_iota(jnp.int32, (PEERS, 128), 1)
    meta = jnp.zeros((PEERS, 128), F32)
    picks = []
    for k, chosen in enumerate((first, second)):
        picks.append(mm(chosen.astype(BF16), source.astype(BF16), nt).astype(BF16))
        meta = jnp.where(lane == k, jnp.sum(chosen * key, axis=1, keepdims=True), meta)

    for copy in sum(coarse_copies, []):
        copy.start()
    corners = corner_matrices()
    for k in range(3):
        held_corners[k] = corners[k]
    restrict = [restrict_matrix(False), restrict_matrix(True)]
    for k in range(2):
        held_restrict[k] = restrict[k]
    for copy in fine_copies:
        copy.wait()
    held = {}

    def fine_b(c, i):
        if (c, i) not in held:
            held[c, i] = fine_slab(pitched_b, c, i)
            put_slab(b_f, c, i, 0, CB, held[c, i])
        return held[c, i]

    top_fine = top_coarse = jnp.zeros((CB, 128), F32)
    for i in range(EDGE):
        centre, velocity = centres(fine_b, i), [fine_slab(v_f, c, i) for c in range(3)]
        put_cell(cell_f, i, centre, velocity)
        top_fine = jnp.maximum(top_fine, speeds(centre, velocity))
    for copy in sum(coarse_copies, []):
        copy.wait()
    edges(cell_f, emf_f, held_corners)
    restrict = held_restrict
    rows = []
    for d in range(3):
        planes = [face_of(emf_f, along, d) for along in TANGENT[d]]
        both = jnp.concatenate([*planes[0], *planes[1]], axis=1)
        rows.append(mm_left(both, restrict[1 if d == 2 else 0]))
    rows = jnp.concatenate(rows, axis=0)
    for k in range(2):
        out[:, 0, k * 128 : (k + 1) * 128] = mm_right(picks[k], rows)
    for i in range(EDGE):
        centre = centres(lambda c, k: slab(b_c, c, k, 0, CB), i)
        top_coarse = jnp.maximum(top_coarse, speeds(centre, [slab(v_c, c, i, 0, CB) for c in range(3)]))
    top = jnp.max(jnp.maximum(top_fine, top_coarse), axis=0, keepdims=True)
    top = jnp.broadcast_to(jnp.max(top, axis=1, keepdims=True), (PEERS, 128))
    out[:, 0, 256:384] = jnp.where(lane < 2, meta, top)
    send_copy = pltpu.make_async_copy(out, send, sems.at[7])
    send_copy.start()
    send_copy.wait()


def coarse_kernel(cb, cv, emf_f, emf, planes, quads, b_c, curl_f, v_c, cell, held, sems):
    copies = coarse_parts(cb, cv, b_c, v_c, sems)
    for copy in sum(copies, []):
        copy.start()
    corners, aheads = corner_matrices(), ahead_matrices()
    curls(emf_f, held, aheads)
    for c in range(3):
        curl_f[c] = held[c]
    load_b, load_v = (lambda c, i, ref=ref: slab(ref, c, i, 0, CB) for ref in (b_c, v_c))
    for i in range(EDGE):
        wait_part(copies, i)
        centre = centres(load_b, i)
        put_cell(cell, i, centre, [load_v(c, i) for c in range(3)])
    edges(cell, emf, corners)
    for d in range(3):
        for t in range(2):
            at = (d * 2 + t) * CB
            face = face_of(emf, TANGENT[d][t], d)
            planes[at : at + CB, 0:128] = face[0]
            planes[at : at + CB, 128:256] = face[1]
    quadrant = [quadrant_matrix(False), quadrant_matrix(True)]
    for d in range(3):
        normal = jnp.concatenate(face_of(b_c, d, d), axis=1)
        quads[d * CB : (d + 1) * CB, :] = mm_left(normal, quadrant[1 if d == 2 else 0])


def answer_kernel(
    got, planes, quads_b, back, far_patch, masks, top, patch, out, sems
):
    expand = [expand_matrix(False), expand_matrix(True)]
    quadrant = [quadrant_matrix(False), quadrant_matrix(True)]
    meta = got[:, 0, 256:384]
    top[...] = jnp.max(meta, axis=0, keepdims=True)
    keys = [meta[:, k : k + 1].astype(jnp.int32) - 1 for k in range(2)]
    target = lax.broadcasted_iota(jnp.int32, (PEERS, 256), 1)
    hit = jnp.concatenate([(k == target).astype(F32) for k in keys], axis=0).astype(BF16)
    rows = jnp.concatenate([got[:, 0, 0:128], got[:, 0, 128:256]], axis=0)
    tn = ((0,), (0,))
    replaced = mm_right(hit, rows, tn)[0:192]
    counted = mm(hit, jnp.ones((2 * PEERS, 128), BF16), tn)[0:192]
    spread = (mm_left(replaced, expand[0]), mm_left(replaced, expand[1]))
    lane = lax.broadcasted_iota(jnp.int32, (CB, 128), 1)

    def at(d, quad):
        return slice(d * 64 + quad * CB, d * 64 + (quad + 1) * CB)

    def value(d, t, flip):
        part = slice(t * 128, (t + 1) * 128)
        out = []
        for h in range(2):
            near, far = (h, h + 2) if flip else (2 * h, 2 * h + 1)
            x = spread[flip]
            out.append(x[at(d, near), part] + pltpu.roll(x[at(d, far), part], 8, 1))
        return tuple(out)

    def mask(d, flip):
        out = []
        for h in range(2):
            near, far = (h, h + 2) if flip else (2 * h, 2 * h + 1)
            out.append(jnp.where((lane & 15) < 8, counted[at(d, near)], counted[at(d, far)]) > 0.5)
        return tuple(out)

    value = {
        (d, t): value(d, t, int(d == 2)) for d in range(3) for t in range(2)
    } | {"1x": value(1, 0, 1), "2x": value(2, 0, 0)}
    hits = {d: mask(d, int(d == 2)) for d in range(3)} | {"1x": mask(1, 1), "2x": mask(2, 0)}
    for h in range(2):
        side = slice(h * 128, (h + 1) * 128)
        masks[:, side] = sum(hits[d][h].astype(F32) * 2.0**d for d in range(3))
        for d in range(3):
            for t in range(2):
                first = (d * 2 + t) * CB
                patch[first : first + CB, side] = value[d, t][h]

    store = pltpu.make_async_copy(patch, far_patch, sems.at[0])
    store.start()

    def face(d, t):
        first = (d * 2 + t) * CB
        return planes[first : first + CB, 0:128], planes[first : first + CB, 128:256]

    both = lambda a, b: a & b
    column = ((lane & 15) == 0,) * 2
    row = (lane < 16, lane < 0)
    put = lambda m, new, old: each(jnp.where, m, new, old)
    ey_0 = put(hits[0], value[0, 0], face(0, 0))
    ez_0 = put(hits[0], value[0, 1], face(0, 1))
    ez_1 = put(each(both, row, hits[0]), value[0, 1], face(1, 1))
    ey_2 = put(each(both, column, hits[0]), value[0, 0], face(2, 1))
    ex_1 = put(hits[1], value[1, 0], face(1, 0))
    ez_1 = put(hits[1], value[1, 1], ez_1)
    ez_0 = put(each(both, row, hits[1]), value[1, 1], ez_0)
    ex_2 = put(each(both, row, hits["1x"]), value["1x"], face(2, 0))
    ex_2 = put(hits[2], value[2, 0], ex_2)
    ey_2 = put(hits[2], value[2, 1], ey_2)
    ex_1 = put(each(both, column, hits["2x"]), value["2x"], ex_1)
    ey_0 = put(each(both, column, hits[2]), value[2, 1], ey_0)
    curl = lambda p, q, r, s: (p - q) - (r - s)
    curls = (
        each(curl, y_next(ez_0), ez_0, z_next(ey_0), ey_0),
        each(curl, z_next(ex_1), ex_1, y_next(ez_1), ez_1),
        each(curl, z_next(ey_2), ey_2, y_next(ex_2), ex_2),
    )
    straight = jnp.concatenate(
        [jnp.concatenate(curls[0], axis=1), jnp.concatenate(curls[1], axis=1)], axis=0
    )
    quads_c = jnp.concatenate(
        [
            mm_left(straight, quadrant[0]),
            mm_left(jnp.concatenate(curls[2], axis=1), quadrant[1]),
        ],
        axis=0,
    )
    wide_lane = lax.broadcasted_iota(jnp.int32, (PEERS, 3 * CB), 1)
    out_lane = lax.broadcasted_iota(jnp.int32, (PEERS, 128), 1)
    for part, quads in enumerate((quads_b[...], quads_c)):
        answers = []
        for k in range(2):
            key = keys[k]
            place = jnp.where(key >= 0, (key >> 6) * CB + (key & 15), -1)
            pick = (place == wide_lane).astype(F32).astype(BF16)
            found = mm_right(pick, quads)
            quad = (key >> 4) & 3
            side = jnp.where(quad >= 2, found[:, 128:256], found[:, 0:128])
            answers.append(jnp.where((quad & 1) == k, side, pltpu.roll(side, 64, 1)))
        side = slice(part * 128, (part + 1) * 128)
        out[:, 0, side] = jnp.where(out_lane < 64, answers[0], answers[1])
    send = pltpu.make_async_copy(out, back, sems.at[1])
    send.start()
    for copy in (store, send):
        copy.wait()


def curl_kernel(emf_c, far_patch, masks, curl_c, patch, held, sems):
    load_patch = pltpu.make_async_copy(far_patch, patch, sems.at[0])
    load_patch.start()
    lane = lax.broadcasted_iota(jnp.int32, (CB, 128), 1)

    def pair(ref, first):
        return ref[first : first + CB, 0:128], ref[first : first + CB, 128:256]

    load_patch.wait()
    planes = {(d, t): pair(patch, (d * 2 + t) * CB) for d in range(3) for t in range(2)}
    bits = [m.astype(jnp.int32) for m in pair(masks, 0)]
    hits = [[((m >> d) & 1).astype(F32) for m in bits] for d in range(3)]
    for i in range(EDGE):
        now = {c: slab(emf_c, c, i, 0, CB) for c in range(3)}
        if i == 0:
            for t, c in enumerate(TANGENT[0]):
                now[c] = each(lambda m, p, e: jnp.where(m > 0.5, p, e), hits[0], planes[0, t], now[c])
        turn, h = (8 - i % 8) % 8 * 16, i // 8
        there = (lane < 16) & (pltpu.roll(hits[1][h], turn, 1) > 0.5)
        for t, c in enumerate(TANGENT[1]):
            now[c] = (jnp.where(there, pltpu.roll(planes[1, t][h], turn, 1), now[c][0]), now[c][1])
        turn = (128 - i) % 128
        there = [((lane & 15) == 0) & (pltpu.roll(m, turn, 1) > 0.5) for m in hits[2]]
        for t, c in enumerate(TANGENT[2]):
            value = [pltpu.roll(p, turn, 1) for p in planes[2, t]]
            now[c] = each(jnp.where, there, value, now[c])
        for c in range(3):
            put_slab(held, c, i, 0, CB, now[c])
    curls(held, curl_c, ahead_matrices())


def update_kernel(
    top, curl_c, curl_f, b_c, b_f, far_pairs,
    new_c, new_f, picked, chosen,
    out_c, out_f, pairs, sems,
):
    load = pltpu.make_async_copy(far_pairs, pairs, sems.at[2])
    load.start()
    time_step = 0.2 / top[0:1, 2:3]
    results = []
    step = lambda factor: lambda b, c: b - factor * c
    for i in range(EDGE):
        for c in range(3):
            value = each(step(time_step), slab(b_c, c, i, 0, CB), slab(curl_c, c, i, 0, CB))
            put_slab(out_c, c, i, 0, CB, value)
        if i % 4 == 3:
            part = pl.ds((i - 3) * WIDE, 4 * WIDE)
            copy = pltpu.make_async_copy(out_c.at[:, :, part], new_c.at[:, :, part], sems.at[1])
            copy.start()
            results.append(copy)
    for i in range(EDGE):
        for c in range(3):
            value = each(step(time_step / 0.5), slab(b_f, c, i, 0, CB), slab(curl_f, c, i, 0, CB))
            put_fine_slab(out_f, c, i, value)
    for b in range(FB):
        copy = pltpu.make_async_copy(out_f.at[pl.ds(b * PITCH, 96)], new_f.at[b], sems.at[0])
        copy.start()
        results.append(copy)
    faces = (
        fine_slab(out_f, 0, 0),
        face_row_wise(lambda i: fine_slab(out_f, 1, i)[0]),
        face_column_wise(lambda i: fine_slab(out_f, 2, i)),
    )
    load.wait()
    first, second, source = routes(pairs)
    tn = ((0,), (0,))
    same = (
        lax.broadcasted_iota(jnp.int32, (PEERS, PEERS), 0)
        == lax.broadcasted_iota(jnp.int32, (PEERS, PEERS), 1)
    ).astype(F32).astype(BF16)
    chosen[...] = jnp.concatenate(
        [mm(first.astype(BF16), same, tn), mm(second.astype(BF16), same, tn)], axis=1
    )
    source = source.astype(BF16)
    flip = flip_matrix()
    normals = [jnp.concatenate(face, axis=1) for face in faces]
    straight = mm_right(source[0 : 2 * CB], jnp.concatenate(normals[0:2], axis=0), tn)
    flipped = mm_left(mm_right(source[2 * CB :], normals[2], tn), flip)
    picked[...] = straight + flipped
    for copy in results:
        copy.wait()


def third_kernel(got, top, picked, chosen, jump, held, sems):
    rows = got[:, 0, 0:128] - (0.2 / top[0:1, 2:3]) * got[:, 0, 128:256]
    lane = lax.broadcasted_iota(jnp.int32, (PAIRS, 128), 1)
    picks = chosen[...].astype(BF16)
    sides = [mm_right(picks[:, k * PEERS : (k + 1) * PEERS], rows) for k in range(2)]
    own = jnp.where(lane < 64, sides[0], sides[1])
    held[...] = picked[...] - mm_left(own, prolong_matrix())
    copy = pltpu.make_async_copy(held, jump, sems.at[0])
    copy.start()
    copy.wait()


VMEM = pl.BlockSpec(memory_space=pltpu.VMEM)
HBM = pl.BlockSpec(memory_space=pltpu.HBM)
FIELD = (3, CB, CELLS)
PITCHED = (CB * PITCH, 128)
FACES = (6 * CB, WIDE)


def call(kernel, outs, args, scratch=(), aliases=None):
    far = [isinstance(out, tuple) and out[0] == "hbm" for out in outs]
    return pl.pallas_call(
        kernel,
        out_shape=[
            pltpu.HBM(out[1], F32) if is_far else pltpu.VMEM(out, F32)
            for out, is_far in zip(outs, far)
        ],
        in_specs=[HBM if is_far else VMEM for _, is_far in args],
        out_specs=[HBM if is_far else VMEM for is_far in far],
        scratch_shapes=list(scratch),
        input_output_aliases=aliases or {},
        compiler_params=pltpu.CompilerParams(vmem_limit_bytes=24 * 1024 * 1024),
    )(
        *(
            pltpu.with_memory_space_constraint(a, pltpu.HBM if is_far else pltpu.VMEM)
            for a, is_far in args
        )
    )


def on_device(coarse_field, coarse_velocity, fine_field, fine_velocity, pairs):
    cb = coarse_field[0].transpose(1, 0, 2)
    cv = coarse_velocity[0].transpose(1, 0, 2)
    fb = fine_field[0].reshape(FB, 96, 128)
    fv = fine_velocity[0].reshape(FB, 96, 128)
    rows = pairs.transpose(2, 0, 1)
    near = lambda *arrays: [(a, False) for a in arrays]
    far = lambda *arrays: [(a, True) for a in arrays]
    count = lax.axis_size("gz")

    field = pltpu.VMEM(FIELD, F32)
    pitched = pltpu.VMEM(PITCHED, F32)
    small = pltpu.VMEM((6, 1, PAIRS), jnp.int32)
    sems = pltpu.SemaphoreType.DMA
    send, emf_f, b_f = call(
        first_kernel,
        [("hbm", (PEERS, 1, 384)), FIELD, FIELD],
        far(cb, cv, fb, fv, rows),
        [
            field,
            field,
            pitched,
            pitched,
            field,
            small,
            pltpu.VMEM((PEERS, 1, 384), F32),
            pltpu.VMEM((3, WIDE, WIDE), BF16),
            pltpu.VMEM((2, 2 * WIDE, 128), BF16),
            sems((9,)),
        ],
    )
    got = lax.all_to_all(send, BLOCKS, 0, 0, tiled=True)
    emf_c, planes, quads, b_c, curl_f = call(
        coarse_kernel,
        [FIELD, FACES, (3 * CB, WIDE), FIELD, FIELD],
        far(cb, cv) + near(emf_f),
        [field, field, field, sems((4,))],
        {2: 4},
    )
    got, emf_c, planes, quads, b_c, curl_f = lax.optimization_barrier(
        (got, emf_c, planes, quads, b_c, curl_f)
    )
    back, patch, masks, top = call(
        answer_kernel,
        [("hbm", (PEERS, 1, 256)), ("hbm", FACES), (CB, WIDE), (1, 128)],
        near(got, planes, quads),
        [pltpu.VMEM(FACES, F32), pltpu.VMEM((PEERS, 1, 256), F32), sems((2,))],
    )
    others = []
    for k in range(1, count):
        others.append(lax.ppermute(top, "gz", [(i, (i + k) % count) for i in range(count)]))
    for other in others:
        top = jnp.maximum(top, other)
    returned = lax.all_to_all(back, BLOCKS, 0, 0, tiled=True)
    (curl_c,) = call(
        curl_kernel,
        [FIELD],
        near(emf_c) + far(patch) + near(masks),
        [pltpu.VMEM(FACES, F32), field, sems((1,))],
        {0: 0},
    )
    new_c, new_f, picked, chosen = call(
        update_kernel,
        [("hbm", FIELD), ("hbm", (FB, 96, 128)), (PAIRS, WIDE), (PAIRS, 128)],
        near(top, curl_c, curl_f, b_c, b_f) + far(rows),
        [field, pitched, small, sems((3,))],
    )
    (jump,) = call(
        third_kernel,
        [("hbm", (PAIRS, WIDE))],
        near(returned, top, picked, chosen),
        [pltpu.VMEM((PAIRS, WIDE), F32), sems((1,))],
    )
    return (
        new_c.transpose(1, 0, 2)[None],
        new_f.reshape(1, FB, 3, CELLS),
        jump[None],
    )


def solution(mesh):
    split = Mesh(
        mesh.devices.reshape(4, 8, 2, mesh.shape["gz"]), ("blocks_0", "blocks_1", "blocks_2", "gz")
    )
    in_specs = (
        P("gz", BLOCKS, None, None),
        P("gz", BLOCKS, None, None),
        P("gz", BLOCKS, None, None),
        P("gz", BLOCKS, None, None),
        P("gz", BLOCKS, None),
    )
    out_specs = (P("gz", BLOCKS, None, None), P("gz", BLOCKS, None, None), P("gz", BLOCKS, None))

    return jax.shard_map(on_device, mesh=split, in_specs=in_specs, out_specs=out_specs, check_vma=False)
```
